128 devices in a mesh: gx: 4 (over y), gy: 16 (over x_lo, z, core), gz: 2 (over x_hi).
Axes of the slice: x: 4 (x_hi: 2, x_lo: 2; x = x_hi * 2 + x_lo), y: 4, z: 4, core: 2. Of those that a mesh axis runs over, the one named last changes fastest.
Arguments:
- heat_source: float32 [64, 512, 2048], P('gz', 'gx', 'gy'), may hold values from -18 to 18
- conductance: float32 [64, 512, 2048], P('gz', 'gx', 'gy'), may hold values from 0.5 to 4
- projection: float32 [2, 4, 16, 3, 128, 128], P('gz', 'gx', 'gy'), may hold values from -1 to 2, as said below
- segment_map: int32 [2, 4, 16, 3, 128], P('gz', 'gx', 'gy'), may hold values from 0 to 127, each once within a row
Outputs:
- thermal_state: float32 [64, 512, 2048], P('gz', 'gx', 'gy')
- multiplier_x: float32 [2, 4, 16, 32, 128], P('gz', 'gx', 'gy')
- multiplier_y: float32 [2, 4, 16, 32, 128], P('gz', 'gx', 'gy')
- multiplier_z: float32 [2, 4, 16, 128, 128], P('gz', 'gx', 'gy')
The draws below stay inside these ranges and needn't reach their ends.
Inputs may be any that keep to these rules, and one draw needn't show every extreme that they name: projection entries are finite.
All inputs are finite; a program needn't handle non-finite values.
Results may differ from the reference program's by a relative error of at most 0.0001.
Values sent between devices are 32-bit elements; how exact they have to be, the bound alone decides.
No kernel may reach another device: no remote copies, remote signals or barrier semaphores. Data moves between devices by JAX's collectives and lax.ppermute only.
A program may use at most 128 MiB of HBM per device.

```python
import math
import jax
import jax.numpy as jnp
from jax import lax

C = 128
CZ = 32
ITERS = 4
SWEEPS = 2
NX = 512
NY = 2048
NZ = 64
N_GX = 4
N_GY = 16
N_GZ = 2


def draw_projection(key, part):
    lattice_dimensions = (N_GZ, N_GX, N_GY, 3, C, C)
    spread = 0.5 / jnp.sqrt(jnp.float32(C))
    noise = jax.random.normal(key, lattice_dimensions, jnp.float32) * spread
    noise = jnp.clip(noise, -4.0 * spread, 4.0 * spread)
    return jnp.eye(C, dtype=jnp.float32) + noise


def level_of(key, dims, shards, low, top_value):
    loudness = 1.0
    for position, blocks in shards:
        draws = jax.random.uniform(jax.random.fold_in(jax.random.fold_in(key, 6), position), (blocks,), jnp.float32, low / len(shards), top_value / len(shards))
        loudness = loudness * jnp.repeat(jnp.exp(draws), dims[position] // blocks).reshape((-1,) + (1,) * (len(dims) - 1 - position))
    return loudness


def bell_draw(stream_key, shape, scale, bound, cuts=(), kind=jnp.bfloat16):
    factor_of = level_of(stream_key, shape, cuts, -0.22, 0.18) if cuts else 1.0
    drawn = jax.random.normal(stream_key, shape, jnp.float32) * scale * factor_of
    return jnp.minimum(jnp.maximum(drawn, -bound), bound).astype(kind)


def setup_inputs(seed: int = 0) -> dict:
    streams_of = jax.random.split(jax.random.key(seed), 5)
    return {
        "heat_source": bell_draw(streams_of[0], (NZ, NX, NY), 3.0, 18.0, ((0, 2), (1, 4), (2, 16)), jnp.float32),
        "conductance": jnp.clip(jnp.exp(math.log(4.0) - 2.0794415 * jax.random.uniform(streams_of[1], (NZ, NX, NY), jnp.float32) ** level_of(streams_of[1], (NZ, NX, NY), ((0, 2), (1, 4), (2, 16)), -0.2, 0.2)), 0.5, 4.0),
        "projection": draw_projection(jax.random.fold_in(streams_of[4], 71), 0),
        "segment_map": jax.vmap(lambda own: jax.random.permutation(own, C))(jax.random.split(streams_of[3], N_GZ * N_GX * N_GY * 3)).reshape((N_GZ, N_GX, N_GY, 3, C)).astype(jnp.int32),
    }


HIGH = lax.Precision.HIGHEST
DAMPING_WEIGHT = 0.8
EPSILON = 1e-6


def to_patches(field):
    return field.reshape(N_GZ, CZ, N_GX, C, N_GY, C).transpose(0, 2, 4, 1, 3, 5)


def collect_block_traces(blocks):
    return blocks.transpose(0, 3, 1, 4, 2, 5).reshape(N_GZ * CZ, N_GX * C, N_GY * C)


def laplacian_operate(field, main_coefficients):
    padded = jnp.pad(field, ((0, 0), (0, 0), (0, 0), (1, 1), (1, 1), (1, 1)))
    nearby = padded[..., 2:, 1:-1, 1:-1] + padded[..., :-2, 1:-1, 1:-1]
    nearby = nearby + padded[..., 1:-1, 2:, 1:-1] + padded[..., 1:-1, :-2, 1:-1]
    nearby = nearby + padded[..., 1:-1, 1:-1, 2:] + padded[..., 1:-1, 1:-1, :-2]
    return main_coefficients * field - nearby


def mortar(projection, segment_map):
    width = projection.shape[-1]
    onehot = (segment_map[..., :, None] == jnp.arange(width, dtype=jnp.int32)).astype(jnp.float32)
    return jnp.einsum("...se,...rs->...er", onehot, projection, precision=HIGH)


FACES = ((0, 1, "x"), (1, 2, "y"), (2, 0, "z"))


def coupling_mismatch_amounts(field, coupling_bases):
    uppers = (field[..., :, -1, :], field[..., :, :, -1], field[..., -1, :, :])
    firsts = (field[..., :, 0, :], field[..., :, :, 0], field[..., 0, :, :])
    counts = (N_GX, N_GY, N_GZ)
    result = []
    for face, patch_axis, label in FACES:
        beyond = jnp.roll(firsts[face], -1, axis=patch_axis)
        projected = jnp.einsum("...ke,...er->...kr", beyond, coupling_bases[..., face, :, :], precision=HIGH)
        count = counts[face]
        lattice_dimensions = [1, 1, 1, 1, 1]
        lattice_dimensions[patch_axis] = count
        final = (jnp.arange(count) == count - 1).reshape(lattice_dimensions)
        result.append(jnp.where(final, jnp.float32(0.0), uppers[face] - projected))
    return result


def lift_faces(mismatch_arrays, coupling_bases, lattice_dimensions):
    backs = []
    for face, patch_axis, label in FACES:
        back = -jnp.einsum("...kr,...er->...ke", mismatch_arrays[face], coupling_bases[..., face, :, :], precision=HIGH)
        backs.append(jnp.roll(back, 1, axis=patch_axis))
    total = jnp.zeros(lattice_dimensions, jnp.float32)
    total = total.at[..., :, -1, :].add(mismatch_arrays[0]).at[..., :, 0, :].add(backs[0])
    total = total.at[..., :, :, -1].add(mismatch_arrays[1]).at[..., :, :, 0].add(backs[1])
    total = total.at[..., -1, :, :].add(mismatch_arrays[2]).at[..., 0, :, :].add(backs[2])
    return total


def reference(heat_source, conductance, projection, segment_map):
    source = to_patches(heat_source)
    main_coefficients = 6.0 + to_patches(conductance)
    coupling_bases = mortar(projection, segment_map)
    lattice_dimensions = source.shape
    thermal_state = jnp.zeros(lattice_dimensions, jnp.float32)
    dual_flux_variables = [jnp.zeros(lattice_dimensions[:3] + (CZ, C), jnp.float32), jnp.zeros(lattice_dimensions[:3] + (CZ, C), jnp.float32), jnp.zeros(lattice_dimensions[:3] + (C, C), jnp.float32)]
    for iteration in range(ITERS):
        volumetric_supply = source - lift_faces(dual_flux_variables, coupling_bases, lattice_dimensions)
        for sweep_index in range(SWEEPS):
            thermal_state = thermal_state + DAMPING_WEIGHT * (volumetric_supply - laplacian_operate(thermal_state, main_coefficients)) / main_coefficients
        mismatch_arrays = coupling_mismatch_amounts(thermal_state, coupling_bases)
        lifted = lift_faces(mismatch_arrays, coupling_bases, lattice_dimensions)
        squares = sum(jnp.sum(jump * jump) for jump in mismatch_arrays)
        energy = jnp.sum(lifted * lifted / main_coefficients)
        alpha = squares / (energy + EPSILON)
        dual_flux_variables = [dual_flux_variables[face] + alpha * mismatch_arrays[face] for face in range(3)]
    return collect_block_traces(thermal_state), dual_flux_variables[0], dual_flux_variables[1], dual_flux_variables[2]
```

```python
import functools

import jax
import jax.numpy as jnp
from jax import lax
from jax.experimental import pallas as pl
from jax.experimental.pallas import tpu as pltpu
from jax.sharding import PartitionSpec as P

HIGH = lax.Precision.HIGHEST
DAMPING_WEIGHT = 0.8
EPSILON = 1e-06
AXES = ("gx", "gy", "gz")
CZ = 32
C = 128
F32 = jnp.float32
UNROLL = 4

VM = pl.BlockSpec(memory_space=pltpu.MemorySpace.VMEM)


def dot(a, b):
    return jnp.dot(a, b, precision=HIGH, preferred_element_type=F32)


def dot_t(a, b):
    return lax.dot_general(a, b, (((1,), (1,)), ((), ())), precision=HIGH, preferred_element_type=F32)


def lane_of(shape):
    return lax.broadcasted_iota(jnp.int32, shape, len(shape) - 1)


def row_of(shape):
    return lax.broadcasted_iota(jnp.int32, shape, len(shape) - 2)


def zero_ends(ref):
    ref[0] = jnp.zeros((C, C), F32)
    ref[CZ + 1] = jnp.zeros((C, C), F32)


def neighbours(src, z):
    centre = src[z + 1]
    rows = row_of((C, C))
    lanes = lane_of((C, C))
    near = src[z] + src[z + 2]
    near = near + jnp.where(rows == 0, 0.0, pltpu.roll(centre, 1, 0))
    near = near + jnp.where(rows == C - 1, 0.0, pltpu.roll(centre, C - 1, 0))
    near = near + jnp.where(lanes == 0, 0.0, pltpu.roll(centre, 1, 1))
    near = near + jnp.where(lanes == C - 1, 0.0, pltpu.roll(centre, C - 1, 1))
    return centre, near


def sweep(src, dst, weight, supply):
    def plane(z, carry):
        centre, near = neighbours(src, z)
        dst[z + 1] = (1.0 - DAMPING_WEIGHT) * centre + weight[z] * (supply[z] + near)
        return carry

    lax.fori_loop(0, CZ, plane, 0, unroll=UNROLL)


def row_faces(src, low, high):
    for z in range(CZ):
        low[z : z + 1, :] = src[z + 1, 0:1, :]
        high[z : z + 1, :] = src[z + 1, C - 1 : C, :]


def column_faces(src, turn, low, high):
    half = lane_of((C, C)) // 2

    def plane(z, packed):
        return jnp.where(half == z, pltpu.roll(src[z + 1], 2 * z + 1, 1), packed)

    packed = lax.fori_loop(0, CZ, plane, jnp.zeros((C, C), F32), unroll=UNROLL)
    turn[...] = packed.T
    high[...] = turn[pl.ds(0, CZ, stride=2), :]
    low[...] = turn[pl.ds(1, CZ, stride=2), :]


def pack_columns(turn, low, high):
    turn[...] = jnp.zeros((C, C), F32)
    turn[pl.ds(0, CZ, stride=2), :] = high
    turn[pl.ds(1, CZ, stride=2), :] = low
    return turn[...].T


def column_plane(packed, z):
    lanes = lane_of((C, C))
    edge = (lanes == 0) | (lanes == C - 1)
    return jnp.where(edge, pltpu.roll(packed, C - 1 - 2 * z, 1), 0.0)


def lift_dense(dst, cols, faces, base, sign):
    def plane(z, carry):
        col = column_plane(cols[...], z)
        if base is None:
            dst[z] = sign * col
        else:
            dst[z] = base[z] + sign * col
        return carry

    lax.fori_loop(0, CZ, plane, 0, unroll=UNROLL)
    for z in range(CZ):
        dst[z, 0:1, :] = dst[z, 0:1, :] + sign * faces[0][z : z + 1, :]
        dst[z, C - 1 : C, :] = dst[z, C - 1 : C, :] + sign * faces[1][z : z + 1, :]
    dst[0] = dst[0] + sign * faces[4][...]
    dst[CZ - 1] = dst[CZ - 1] + sign * faces[5][...]


def places():
    x, y, z = (lax.axis_index(a) for a in AXES)
    more = [i < lax.axis_size(a) - 1 for a, i in zip(AXES, (x, y, z))]
    return x % 2 == 0, y % 2 == 0, z == 0, more


def pick(flag, a, b):
    return lax.select(jnp.broadcast_to(flag, a.shape), a, b)


def pack_sends(sends, own, index, extra):
    xeven, yeven, zlow, _ = places()
    xa, xb, ya, yb, zz = sends
    for even, a, b, low, high, n in (
        (xeven, xa, xb, own[0], own[1], CZ),
        (yeven, ya, yb, own[2], own[3], CZ),
    ):
        lo = low[...]
        hi = high[...]
        a[index * n : (index + 1) * n, :] = pick(even, hi, lo)
        b[index * n : (index + 1) * n, :] = pick(even, lo, hi)
    zz[index * C : (index + 1) * C, :] = pick(zlow, own[5][...], own[4][...])
    if extra is not None:
        for a in (xa, xb):
            a[CZ : CZ + C, :] = extra[0]
        for a in (ya, yb):
            a[CZ : CZ + C, :] = extra[1]
        zz[C : 2 * C, :] = extra[2]


def own_faces(src, own, turn):
    row_faces(src, own[0], own[1])
    column_faces(src, turn, own[2], own[3])
    own[4][...] = src[1]
    own[5][...] = src[CZ]


def first_kernel(heat, cond, proj, segs, weight, state, bases, x0, x1, y0, y1, z0, z1, xa, xb, ya, yb, zz, start, turn):
    own = (x0, x1, y0, y1, z0, z1)
    for d in range(3):
        onehot = jnp.where(row_of((C, C)) == segs[d : d + 1, :], 1.0, 0.0).astype(F32)
        bases[d] = dot_t(onehot, proj[d])
    zero_ends(start)
    zero_ends(state)

    def plane(z, carry):
        w = DAMPING_WEIGHT / (6.0 + cond[z])
        weight[z] = w
        start[z + 1] = w * heat[z]
        return carry

    lax.fori_loop(0, CZ, plane, 0, unroll=UNROLL)
    sweep(start, state, weight, heat)
    own_faces(state, own, turn)
    pack_sends((xa, xb, ya, yb, zz), own, 0, bases)


def free_kernel(state, weight, supply, out, mid):
    zero_ends(mid)
    zero_ends(out)
    sweep(state, mid, weight, supply)
    sweep(mid, out, weight, supply)


def jumps(own, got, bases, prev_bases, index, lifted):
    xeven, yeven, zlow, more = places()
    xa, xb, ya, yb, zz = got
    for d, (even, a, b, n) in enumerate(((xeven, xa, xb, CZ), (yeven, ya, yb, CZ), (zlow, zz, zz, C))):
        s = slice(index * n, (index + 1) * n)
        after = pick(even, a[s, :], b[s, :])
        before = pick(even, b[s, :], a[s, :])
        up = own[2 * d + 1][...] - dot(after, bases[d])
        lifted[2 * d + 1][...] = jnp.where(more[d], up, 0.0)
        down = before - dot(own[2 * d][...], prev_bases[d])
        back = -dot_t(down, prev_bases[d])
        if d == 2:
            back = jnp.where(zlow, 0.0, back)
        lifted[2 * d][...] = back


def square_sums(a, b):
    return sum(jnp.sum(a[i][...] * b[i][...]) for i in (1, 3, 5))


def row_of_sums(values):
    lanes = lane_of((1, C))
    row = jnp.zeros((1, C), F32)
    for i, v in enumerate(values):
        row = jnp.where(lanes == i, v, row)
    return row


def energy_sums(pairs, weight):
    def plane(z, carry):
        w = weight[z]
        out = []
        for (a, b), acc in zip(pairs, carry):
            t = a[z] * b[z] * w
            out.append(acc + jnp.sum(t.reshape(C // 8, 8, C), axis=0))
        return tuple(out)

    zero = jnp.zeros((8, C), F32)
    accs = lax.fori_loop(0, CZ, plane, (zero,) * len(pairs), unroll=UNROLL)
    return [jnp.sum(a) / DAMPING_WEIGHT for a in accs]


def second_kernel(first, *refs):
    it = iter(refs)
    take = lambda n: [next(it) for _ in range(n)]
    own = take(6)
    got = take(5)
    (bases,) = take(1)
    (prev,) = take(1) if not first else (None,)
    weight, free = take(2)
    lifted = take(6)
    (sums, resp) = take(2)
    own_u = take(6)
    own_v = take(6)
    sends = take(5)
    if first:
        (prev,) = take(1)
    lift, mid, turn, cols = take(4)
    xeven, yeven, zlow, _ = places()
    if first:
        xa, xb, ya, yb, zz = got
        prev[0] = pick(xeven, xb[CZ:, :], xa[CZ:, :])
        prev[1] = pick(yeven, yb[CZ:, :], ya[CZ:, :])
        prev[2] = zz[C:, :]
    jumps(own, got, bases, prev, 0, lifted)
    cols[...] = pack_columns(turn, lifted[2][...], lifted[3][...])
    lift_dense(lift, cols, lifted, None, 1.0)
    zero_ends(mid)
    zero_ends(resp)

    def plane(z, carry):
        mid[z + 1] = weight[z] * lift[z]
        return carry

    lax.fori_loop(0, CZ, plane, 0, unroll=UNROLL)
    sweep(mid, resp, weight, lift)
    own_faces(free, own_u, turn)
    own_faces(resp, own_v, turn)
    pack_sends(sends, own_u, 0, None)
    pack_sends(sends, own_v, 1, None)
    gg = square_sums(lifted, lifted)
    (gh,) = energy_sums([(lift, lift)], weight)
    sums[...] = row_of_sums([gg, gh])


def third_kernel(*refs):
    it = iter(refs)
    take = lambda n: [next(it) for _ in range(n)]
    own_u = take(6)
    own_v = take(6)
    got = take(5)
    bases, prev, weight, before = take(4)
    lift_u = take(6)
    lift_v = take(6)
    (rows,) = take(1)
    dense_u, dense_v, turn, cols = take(4)
    jumps(own_u, got, bases, prev, 0, lift_u)
    jumps(own_v, got, bases, prev, 1, lift_v)
    cols[...] = pack_columns(turn, lift_u[2][...], lift_u[3][...])
    lift_dense(dense_u, cols, lift_u, None, 1.0)
    cols[...] = pack_columns(turn, lift_v[2][...], lift_v[3][...])
    lift_dense(dense_v, cols, lift_v, None, 1.0)
    sums = [square_sums(lift_u, lift_u), square_sums(lift_u, lift_v), square_sums(lift_v, lift_v)]
    sums += energy_sums([(dense_u, dense_u), (dense_u, dense_v), (dense_v, dense_v)], weight)
    lanes = lane_of((1, C))
    row = row_of_sums([0.0, 0.0] + sums)
    row = jnp.where(lanes < 2, before[...], row)
    rows[...] = jnp.broadcast_to(row, (C, C))


def steps(totals):
    row = jnp.sum(totals[...], axis=0, keepdims=True)
    lanes = lane_of((1, C))
    gg, gh, guu, guv, gvv, huu, huv, hvv = [jnp.sum(jnp.where(lanes == i, row, 0.0), axis=1, keepdims=True) for i in range(8)]
    one = gg / (gh + EPSILON)
    two = (guu - 2.0 * one * guv + one * one * gvv) / (huu - 2.0 * one * huv + one * one * hvv + EPSILON)
    return one, two


def fourth_kernel(*refs):
    it = iter(refs)
    take = lambda n: [next(it) for _ in range(n)]
    totals, heat, weight, free, resp = take(5)
    lift_1 = take(6)
    lift_u = take(6)
    lift_v = take(6)
    supply, state = take(2)
    held = take(6)
    own = take(6)
    sends = take(5)
    mid, turn, cols = take(3)
    one, two = steps(totals)
    for i in range(6):
        held[i][...] = one * lift_1[i][...] + two * (lift_u[i][...] - one * lift_v[i][...])
    cols[...] = pack_columns(turn, held[2][...], held[3][...])
    lift_dense(supply, cols, held, heat, -1.0)
    zero_ends(mid)
    zero_ends(state)

    def plane(z, carry):
        state[z + 1] = free[z + 1] - one * resp[z + 1]
        return carry

    lax.fori_loop(0, CZ, plane, 0, unroll=UNROLL)
    sweep(state, mid, weight, supply)
    sweep(mid, state, weight, supply)
    own_faces(state, own, turn)
    pack_sends(sends, own, 0, None)


def last_kernel(*refs):
    it = iter(refs)
    take = lambda n: [next(it) for _ in range(n)]
    totals, free, resp = take(3)
    held = take(3)
    lift_3 = take(3)
    lift_u = take(3)
    lift_v = take(3)
    (state,) = take(1)
    outs = take(3)
    one, two = steps(totals)

    def plane(z, carry):
        state[z] = free[z + 1] - one * resp[z + 1]
        return carry

    lax.fori_loop(0, CZ, plane, 0, unroll=UNROLL)
    for i in range(3):
        outs[i][...] = held[i][...] + one * lift_3[i][...] + two * (lift_u[i][...] - one * lift_v[i][...])


FIELD = jax.ShapeDtypeStruct((CZ, C, C), F32)
PADDED = jax.ShapeDtypeStruct((CZ + 2, C, C), F32)
FACE = jax.ShapeDtypeStruct((CZ, C), F32)
SQUARE = jax.ShapeDtypeStruct((C, C), F32)
FACES = [FACE] * 4 + [SQUARE] * 2
BASES = jax.ShapeDtypeStruct((3, C, C), F32)
ROW = jax.ShapeDtypeStruct((1, C), F32)
S_FIELD = pltpu.VMEM((CZ, C, C), F32)
S_PADDED = pltpu.VMEM((CZ + 2, C, C), F32)
S_SQUARE = pltpu.VMEM((C, C), F32)


def sends_of(n, extra):
    small = jax.ShapeDtypeStruct((n * CZ + extra, C), F32)
    return [small] * 4 + [jax.ShapeDtypeStruct((n * C + extra, C), F32)]


def call(kernel, name, outs, scratch, args, us):
    return pl.pallas_call(
        kernel,
        out_shape=tuple(outs),
        in_specs=[VM] * len(args),
        out_specs=tuple([VM] * len(outs)),
        scratch_shapes=scratch,
        name=name,
        compiler_params=pltpu.CompilerParams(vmem_limit_bytes=40 * 1024 * 1024),
        cost_estimate=pl.CostEstimate(flops=us * 10**7, transcendentals=0, bytes_accessed=2**20),
    )(*args)


def swap_pairs(axis, start):
    n = lax.axis_size(axis)
    pairs = []
    for i in range(start, n - 1, 2):
        pairs += [(i, i + 1), (i + 1, i)]
    return pairs


def exchange(sends):
    xa, xb, ya, yb, zz = sends
    zz = lax.ppermute(zz, "gz", swap_pairs("gz", 0))
    yb = lax.ppermute(yb, "gy", swap_pairs("gy", 1))
    xb = lax.ppermute(xb, "gx", swap_pairs("gx", 1))
    xa = lax.ppermute(xa, "gx", swap_pairs("gx", 0))
    ya = lax.ppermute(ya, "gy", swap_pairs("gy", 0))
    return [xa, xb, ya, yb, zz]


def gather_rows(rows):
    rows = lax.all_to_all(rows.reshape(C, 1, C), AXES, 0, 0)
    return rows.reshape(C, C)


def body(heat, cond, projection, segment_map):
    proj = projection[0, 0, 0]
    segs = segment_map[0, 0, 0]
    out = call(first_kernel, "first", [FIELD, PADDED, BASES] + FACES + sends_of(1, C), [S_PADDED, S_SQUARE], (heat, cond, proj, segs), 4)
    weight, state, bases = out[:3]
    own, sends = list(out[3:9]), out[9:]
    supply = heat
    prev = None
    held = None
    for pair in range(2):
        got = exchange(sends)
        (free,) = call(free_kernel, "free", [PADDED], [S_PADDED], (state, weight, supply), 3)
        first = pair == 0
        args = own + got + [bases] + ([] if first else [prev]) + [weight, free]
        outs = FACES + [ROW, PADDED] + FACES + FACES + sends_of(2, 0) + ([BASES] if first else [])
        out = list(call(functools.partial(second_kernel, first), "second", outs, [S_FIELD, S_PADDED, S_SQUARE, S_SQUARE], args, 4))
        lift_1, (sums, resp), own_u, own_v, sends = out[:6], out[6:8], out[8:14], out[14:20], out[20:25]
        if first:
            prev = out[25]
        got = exchange(sends)
        args = own_u + own_v + got + [bases, prev, weight, sums]
        out = list(call(third_kernel, "third", FACES + FACES + [SQUARE], [S_FIELD, S_FIELD, S_SQUARE, S_SQUARE], args, 3))
        lift_u, lift_v, rows = out[:6], out[6:12], out[12]
        totals = gather_rows(rows)
        if first:
            args = [totals, heat, weight, free, resp] + lift_1 + lift_u + lift_v
            out = list(call(fourth_kernel, "fourth", [FIELD, PADDED] + FACES + FACES + sends_of(1, 0), [S_PADDED, S_SQUARE, S_SQUARE], args, 5))
            supply, state, held, own, sends = out[0], out[1], out[2:8], out[8:14], out[14:]
    upper = lambda faces: [faces[1], faces[3], faces[5]]
    args = [totals, free, resp] + upper(held) + upper(lift_1) + upper(lift_u) + upper(lift_v)
    state, mx, my, mz = call(last_kernel, "last", [FIELD, FACE, FACE, SQUARE], [], args, 2)
    return state, mx[None, None, None], my[None, None, None], mz[None, None, None]


def solution(mesh):
    field = P("gz", "gx", "gy")
    in_specs = (field, field, P("gz", "gx", "gy", None, None, None), P("gz", "gx", "gy", None, None))
    face = P("gz", "gx", "gy", None, None)
    return jax.shard_map(body, mesh=mesh, in_specs=in_specs, out_specs=(field, face, face, face), check_vma=False)
```

```python
import functools

import jax
import jax.numpy as jnp
from jax import lax
from jax.experimental import pallas as pl
from jax.experimental.pallas import tpu as pltpu
from jax.sharding import PartitionSpec as P

HIGH = lax.Precision.HIGHEST
DAMPING_WEIGHT = 0.8
EPSILON = 1e-06
AXES = ("gx", "gy", "gz")
CZ = 32
C = 128
F32 = jnp.float32
UNROLL = 4
WIDE = 16
PARTS = 4
KEPT = 1.0 - DAMPING_WEIGHT

VM = pl.BlockSpec(memory_space=pltpu.MemorySpace.VMEM)


def dot(a, b):
    return jnp.dot(a, b, precision=HIGH, preferred_element_type=F32)


def dot_t(a, b):
    return lax.dot_general(a, b, (((1,), (1,)), ((), ())), precision=HIGH, preferred_element_type=F32)


def lane_of(shape):
    return lax.broadcasted_iota(jnp.int32, shape, len(shape) - 1)


def row_of(shape):
    return lax.broadcasted_iota(jnp.int32, shape, len(shape) - 2)


def zero_ends(ref):
    ref[0] = jnp.zeros((C, C), F32)
    ref[CZ + 1] = jnp.zeros((C, C), F32)


def neighbours(src, z):
    centre = src[z + 1]
    return centre, src[z] + src[z + 2] + in_plane(centre)


def in_plane(centre):
    shape = centre.shape
    rows = row_of(shape)
    lanes = lane_of(shape)
    near = jnp.where(rows == 0, 0.0, pltpu.roll(centre, 1, 0))
    near = near + jnp.where(rows == shape[0] - 1, 0.0, pltpu.roll(centre, shape[0] - 1, 0))
    near = near + jnp.where(lanes == 0, 0.0, pltpu.roll(centre, 1, 1))
    return near + jnp.where(lanes == C - 1, 0.0, pltpu.roll(centre, C - 1, 1))


def sweep(src, dst, weight, supply):
    def plane(z, carry):
        centre, near = neighbours(src, z)
        dst[z + 1] = KEPT * centre + weight[z] * (supply[z] + near)
        return carry

    lax.fori_loop(0, CZ, plane, 0, unroll=UNROLL)


def row_layer(src, base, at, out):
    for z in range(CZ):
        out[z : z + 1, :] = src[z + base, at : at + 1, :]


def column_layers(src, base, turn):
    group = lane_of((C, C)) // 4

    def plane(z, packed):
        return jnp.where(group == z, pltpu.roll(src[z + base], 4 * z + 2, 1), packed)

    packed = lax.fori_loop(0, CZ, plane, jnp.zeros((C, C), F32), unroll=WIDE)
    turn[...] = packed.T


def layer_rows(i):
    return pl.ds(i, CZ, stride=4)


def pack_columns(turn, low, high):
    turn[...] = jnp.zeros((C, C), F32)
    turn[layer_rows(1), :] = high
    turn[layer_rows(2), :] = low
    return turn[...].T


def column_plane(packed, z):
    lanes = lane_of((C, C))
    edge = (lanes == 0) | (lanes == C - 1)
    return jnp.where(edge, pltpu.roll(packed, C - 2 - 4 * z, 1), 0.0)


def lift_dense(dst, cols, faces, base, sign):
    def plane(z, carry):
        col = column_plane(cols[...], z)
        if base is None:
            dst[z] = sign * col
        else:
            dst[z] = base[z] + sign * col
        return carry

    lax.fori_loop(0, CZ, plane, 0, unroll=WIDE)
    for z in range(CZ):
        dst[z, 0:1, :] = dst[z, 0:1, :] + sign * faces[0][z : z + 1, :]
        dst[z, C - 1 : C, :] = dst[z, C - 1 : C, :] + sign * faces[1][z : z + 1, :]
    dst[0] = dst[0] + sign * faces[4][...]
    dst[CZ - 1] = dst[CZ - 1] + sign * faces[5][...]


EDGES = (0, 1, C - 2, C - 1)


def rim(low, high, at):
    lanes = lane_of(low.shape)
    a = low if at == 0 else pltpu.roll(low, C - at, 1)
    b = high if at == C - 1 else pltpu.roll(high, C - 1 - at, 1)
    return jnp.where(lanes == 0, a, jnp.where(lanes == C - 1, b, 0.0))


def ends(low, high):
    rows = row_of((CZ, C))
    return jnp.where(rows == 0, low, jnp.where(rows == CZ - 1, high, 0.0))


def lift_layers(faces, turn, inner):
    bx, hx, by, hy, bz, hz = [f[...] for f in faces]
    lanes = lane_of((C, C))
    columns = jnp.where(lanes < 4, pltpu.roll(bz, 2, 1), pltpu.roll(hz, 6, 1)).T
    at = lambda i: columns[i : i + 1, :]
    column = {C - 2: (at(0), at(4)), C - 1: (at(1), at(5)), 0: (at(2), at(6)), 1: (at(3), at(7))}
    edges = EDGES if inner else (0, C - 1)
    on_x = {}
    on_y = {}
    for e in edges:
        on_x[e] = rim(by, hy, e) + ends(bz[e : e + 1, :], hz[e : e + 1, :])
        on_y[e] = rim(bx, hx, e) + ends(*column[e])
    on_x[0] = on_x[0] + bx
    on_x[C - 1] = on_x[C - 1] + hx
    on_y[0] = on_y[0] + by
    on_y[C - 1] = on_y[C - 1] + hy
    packed = pack_columns(turn, by, hy)
    rows = row_of((C, C))
    on_z = {}
    for z in (0, 1, CZ - 2, CZ - 1) if inner else (0, CZ - 1):
        p = column_plane(packed, z)
        p = p + jnp.where(rows == 0, bx[z : z + 1, :], jnp.where(rows == C - 1, hx[z : z + 1, :], 0.0))
        on_z[z] = p + bz if z == 0 else p + hz if z == CZ - 1 else p
    return on_x, on_y, on_z


def layer_weights(weight, wx, wy):
    return (
        {e: wx[i] for i, e in enumerate(EDGES)},
        {e: wy[i] for i, e in enumerate(EDGES)},
        {z: weight[z] for z in (0, 1, CZ - 2, CZ - 1)},
    )


def face_response(layers, weights):
    out = []
    for layer, w, last in zip(layers, weights, (C - 1, C - 1, CZ - 1)):
        for face, inside in ((0, 1), (last, last - 1)):
            once = w[face] * layer[face]
            near = in_plane(once) + w[inside] * layer[inside]
            out.append(KEPT * once + w[face] * (layer[face] + near))
    return out


def fold(t):
    return jnp.sum(t.reshape(t.shape[0] // 8, 8, C), axis=0)


def layer_energy(a, b, weights):
    rows = row_of((CZ, C))
    lanes = lane_of((CZ, C))
    inner = (rows > 0) & (rows < CZ - 1)
    both = inner & (lanes > 0) & (lanes < C - 1)
    acc = jnp.zeros((8, C), F32)
    for layers_a, layers_b, w, last, mask in zip(a, b, weights, (C - 1, C - 1, CZ - 1), (inner, both, None)):
        for e in (0, last):
            t = layers_a[e] * layers_b[e] * w[e]
            acc = acc + fold(t if mask is None else jnp.where(mask, t, 0.0))
    return jnp.sum(acc) / DAMPING_WEIGHT


def places():
    x, y, z = (lax.axis_index(a) for a in AXES)
    more = [i < lax.axis_size(a) - 1 for a, i in zip(AXES, (x, y, z))]
    return x % 2 == 0, y % 2 == 0, z == 0, more


def pick(flag, a, b):
    return lax.select(jnp.broadcast_to(flag, a.shape), a, b)


def pack_sends(sends, faces, index):
    xeven, yeven, zlow, _ = places()
    xa, xb, ya, yb, zz = sends
    for even, a, b, lo, hi in ((xeven, xa, xb, faces[0], faces[1]), (yeven, ya, yb, faces[2], faces[3])):
        s = slice(index * CZ, (index + 1) * CZ)
        a[s, :] = pick(even, hi, lo)
        b[s, :] = pick(even, lo, hi)
    zz[index * C : (index + 1) * C, :] = pick(zlow, faces[5], faces[4])


def own_faces(src, own, turn):
    row_layer(src, 1, 0, own[0])
    row_layer(src, 1, C - 1, own[1])
    column_layers(src, 1, turn)
    own[2][...] = turn[layer_rows(2), :]
    own[3][...] = turn[layer_rows(1), :]
    own[4][...] = src[1]
    own[5][...] = src[CZ]


def first_kernel(heat_in, cond_in, proj, segs, weight, state, bases, heat, *refs):
    own = refs[:6]
    sends = refs[6:11]
    cond, start, turn, sems = refs[11:]
    part = CZ // PARTS
    copies = []
    for i in range(PARTS):
        s = pl.ds(i * part, part)
        pair = (
            pltpu.make_async_copy(cond_in.at[s], cond.at[s], sems.at[0, i]),
            pltpu.make_async_copy(heat_in.at[s], heat.at[s], sems.at[1, i]),
        )
        for c in pair:
            c.start()
        copies.append(pair)
    for d in range(3):
        onehot = jnp.where(row_of((C, C)) == segs[d : d + 1, :], 1.0, 0.0).astype(F32)
        bases[d] = dot_t(onehot, proj[d])
    zero_ends(start)
    zero_ends(state)

    def plane(z, carry):
        w = DAMPING_WEIGHT / (6.0 + cond[z])
        weight[z] = w
        start[z + 1] = w * heat[z]
        return carry

    for i, pair in enumerate(copies):
        for c in pair:
            c.wait()
        lax.fori_loop(i * part, (i + 1) * part, plane, 0, unroll=UNROLL)
    sweep(start, state, weight, heat)
    own_faces(state, own, turn)
    pack_sends(sends, [f[...] for f in own], 0)
    for a in sends[:2]:
        a[CZ : CZ + C, :] = bases[0]
    for a in sends[2:4]:
        a[CZ : CZ + C, :] = bases[1]
    sends[4][C : 2 * C, :] = bases[2]


def free_kernel(first, state, weight, supply, *refs):
    out = refs[0]
    own = refs[1:7]
    mid, turn = refs[-2:]
    zero_ends(mid)
    zero_ends(out)
    sweep(state, mid, weight, supply)
    sweep(mid, out, weight, supply)
    own_faces(out, own, turn)
    if first:
        wx, wy = refs[7:9]
        for i, e in enumerate(EDGES):
            row_layer(weight, 0, e, wx.at[i])
        column_layers(weight, 0, turn)
        for i, e in enumerate((2, 3, 0, 1)):
            wy[i] = turn[layer_rows(e), :]


def jumps(own, got, bases, prev_bases, n, lifted):
    xeven, yeven, zlow, more = places()
    xa, xb, ya, yb, zz = got
    for d, (even, a, b, rows) in enumerate(((xeven, xa, xb, n * CZ), (yeven, ya, yb, n * CZ), (zlow, zz, zz, n * C))):
        a = a[0:rows, :]
        b = b[0:rows, :]
        up = own[2 * d + 1][...] - dot(pick(even, a, b), bases[d])
        up = jnp.where(more[d], up, 0.0)
        down = pick(even, b, a) - dot(own[2 * d][...], prev_bases[d])
        back = -dot_t(down, prev_bases[d])
        if d == 2:
            back = jnp.where(zlow, 0.0, back)
        size = rows // n
        for i in range(n):
            lifted[i][2 * d][...] = back[i * size : (i + 1) * size, :]
            lifted[i][2 * d + 1][...] = up[i * size : (i + 1) * size, :]


def square_sum(a, b):
    return jnp.sum(sum(fold(a[i][...] * b[i][...]) for i in (1, 3, 5)))


def row_of_sums(values):
    lanes = lane_of((1, C))
    row = jnp.zeros((1, C), F32)
    for i, v in enumerate(values):
        row = jnp.where(lanes == i, v, row)
    return row


def second_kernel(first, *refs):
    it = iter(refs)
    take = lambda n: [next(it) for _ in range(n)]
    own = take(6)
    got = take(5)
    (bases,) = take(1)
    (prev,) = take(1) if not first else (None,)
    weight, wx, wy = take(3)
    own_u = take(6)
    lifted = take(6)
    own_uv = take(6)
    sends = take(5)
    if first:
        (prev,) = take(1)
    (turn,) = take(1)
    xeven, yeven, zlow, _ = places()
    if first:
        xa, xb, ya, yb, zz = got
        prev[0] = pick(xeven, xb[CZ:, :], xa[CZ:, :])
        prev[1] = pick(yeven, yb[CZ:, :], ya[CZ:, :])
        prev[2] = zz[C:, :]
    jumps(own, got, bases, prev, 1, [lifted])
    response = face_response(lift_layers(lifted, turn, True), layer_weights(weight, wx, wy))
    free = [f[...] for f in own_u]
    for o, u, v in zip(own_uv, free, response):
        n = u.shape[0]
        o[0:n, :] = u
        o[n:, :] = v
    pack_sends(sends, free, 0)
    pack_sends(sends, response, 1)


def response_kernel(*refs):
    lifted = refs[:6]
    weight, resp, sums, lift, mid, turn, cols = refs[6:]
    cols[...] = pack_columns(turn, lifted[2][...], lifted[3][...])
    lift_dense(lift, cols, lifted, None, 1.0)
    zero_ends(mid)
    zero_ends(resp)

    def plane(z, acc):
        once = weight[z] * lift[z]
        mid[z + 1] = once
        return acc + fold(once * lift[z])

    acc = lax.fori_loop(0, CZ, plane, jnp.zeros((8, C), F32), unroll=UNROLL)
    sweep(mid, resp, weight, lift)
    sums[...] = row_of_sums([square_sum(lifted, lifted), jnp.sum(acc) / DAMPING_WEIGHT])


def third_kernel(*refs):
    it = iter(refs)
    take = lambda n: [next(it) for _ in range(n)]
    own_uv = take(6)
    got = take(5)
    bases, prev, weight, wx, wy, before = take(6)
    lift_u = take(6)
    lift_v = take(6)
    (rows,) = take(1)
    (turn,) = take(1)
    jumps(own_uv, got, bases, prev, 2, [lift_u, lift_v])
    weights = layer_weights(weight, wx, wy)
    u = lift_layers(lift_u, turn.at[0], False)
    v = lift_layers(lift_v, turn.at[1], False)
    sums = [square_sum(lift_u, lift_u), square_sum(lift_u, lift_v), square_sum(lift_v, lift_v)]
    sums += [layer_energy(u, u, weights), layer_energy(u, v, weights), layer_energy(v, v, weights)]
    lanes = lane_of((1, C))
    row = row_of_sums([0.0, 0.0] + sums)
    row = jnp.where(lanes < 2, before[...], row)
    rows[...] = jnp.broadcast_to(row, (C, C))


def steps(totals):
    row = jnp.sum(totals[...], axis=0, keepdims=True)
    lanes = lane_of((1, C))
    gg, gh, guu, guv, gvv, huu, huv, hvv = [jnp.sum(jnp.where(lanes == i, row, 0.0), axis=1, keepdims=True) for i in range(8)]
    one = gg / (gh + EPSILON)
    two = (guu - 2.0 * one * guv + one * one * gvv) / (huu - 2.0 * one * huv + one * one * hvv + EPSILON)
    return one, two


def fourth_kernel(*refs):
    it = iter(refs)
    take = lambda n: [next(it) for _ in range(n)]
    totals, heat, weight, free, resp = take(5)
    lift_1 = take(6)
    lift_u = take(6)
    lift_v = take(6)
    supply, state = take(2)
    held = take(6)
    own = take(6)
    sends = take(5)
    mid, turn, cols = take(3)
    one, two = steps(totals)
    for i in range(6):
        held[i][...] = one * lift_1[i][...] + two * (lift_u[i][...] - one * lift_v[i][...])
    cols[...] = pack_columns(turn, held[2][...], held[3][...])
    lift_dense(supply, cols, held, heat, -1.0)
    zero_ends(mid)
    zero_ends(state)

    def plane(z, carry):
        state[z + 1] = free[z + 1] - one * resp[z + 1]
        return carry

    lax.fori_loop(0, CZ, plane, 0, unroll=UNROLL)
    sweep(state, mid, weight, supply)
    sweep(mid, state, weight, supply)
    own_faces(state, own, turn)
    pack_sends(sends, [f[...] for f in own], 0)


def last_kernel(*refs):
    it = iter(refs)
    take = lambda n: [next(it) for _ in range(n)]
    totals, free, resp = take(3)
    held = take(3)
    lift_3 = take(3)
    lift_u = take(3)
    lift_v = take(3)
    (state,) = take(1)
    outs = take(3)
    one, two = steps(totals)

    def plane(z, carry):
        state[z] = free[z + 1] - one * resp[z + 1]
        return carry

    lax.fori_loop(0, CZ, plane, 0, unroll=UNROLL)
    for i in range(3):
        outs[i][...] = held[i][...] + one * lift_3[i][...] + two * (lift_u[i][...] - one * lift_v[i][...])


FIELD = jax.ShapeDtypeStruct((CZ, C, C), F32)
PADDED = jax.ShapeDtypeStruct((CZ + 2, C, C), F32)
FACE = jax.ShapeDtypeStruct((CZ, C), F32)
SQUARE = jax.ShapeDtypeStruct((C, C), F32)
FACES = [FACE] * 4 + [SQUARE] * 2
BASES = jax.ShapeDtypeStruct((3, C, C), F32)
LAYERS = jax.ShapeDtypeStruct((4, CZ, C), F32)
ROW = jax.ShapeDtypeStruct((1, C), F32)
S_FIELD = pltpu.VMEM((CZ, C, C), F32)
S_PADDED = pltpu.VMEM((CZ + 2, C, C), F32)
S_SQUARE = pltpu.VMEM((C, C), F32)


def sends_of(n, extra):
    small = jax.ShapeDtypeStruct((n * CZ + extra, C), F32)
    return [small] * 4 + [jax.ShapeDtypeStruct((n * C + extra, C), F32)]


def call(kernel, name, outs, scratch, args, us, in_specs=None):
    return list(
        pl.pallas_call(
            kernel,
            out_shape=tuple(outs),
            in_specs=in_specs or [VM] * len(args),
            out_specs=tuple([VM] * len(outs)),
            scratch_shapes=scratch,
            name=name,
            compiler_params=pltpu.CompilerParams(vmem_limit_bytes=40 * 1024 * 1024),
            cost_estimate=pl.CostEstimate(flops=us * 10**7, transcendentals=0, bytes_accessed=2**20),
        )(*args)
    )


def swap_pairs(axis, start):
    n = lax.axis_size(axis)
    pairs = []
    for i in range(start, n - 1, 2):
        pairs += [(i, i + 1), (i + 1, i)]
    return pairs


def exchange(sends):
    xa, xb, ya, yb, zz = sends
    zz = lax.ppermute(zz, "gz", swap_pairs("gz", 0))
    yb = lax.ppermute(yb, "gy", swap_pairs("gy", 1))
    xb = lax.ppermute(xb, "gx", swap_pairs("gx", 1))
    xa = lax.ppermute(xa, "gx", swap_pairs("gx", 0))
    ya = lax.ppermute(ya, "gy", swap_pairs("gy", 0))
    return [xa, xb, ya, yb, zz]


def gather_rows(rows):
    rows = lax.all_to_all(rows.reshape(C, 1, C), AXES, 0, 0)
    return rows.reshape(C, C)


def body(heat, cond, projection, segment_map):
    proj = projection[0, 0, 0]
    segs = segment_map[0, 0, 0]
    scratch = [S_FIELD, S_PADDED, S_SQUARE, pltpu.SemaphoreType.DMA((2, PARTS))]
    outs = [FIELD, PADDED, BASES, FIELD] + FACES + sends_of(1, C)
    away = pl.BlockSpec(memory_space=pl.ANY)
    out = call(first_kernel, "first", outs, scratch, (heat, cond, proj, segs), 4, [away, away, VM, VM])
    weight, state, bases, heat = out[:4]
    own, sends = out[4:10], out[10:]
    supply = heat
    prev = []
    held = None
    for pair in range(2):
        first = pair == 0
        got = exchange(sends)
        outs = [PADDED] + FACES + ([LAYERS, LAYERS] if first else [])
        out = call(functools.partial(free_kernel, first), "free", outs, [S_PADDED, S_SQUARE], (state, weight, supply), 3)
        free, own_u = out[0], out[1:7]
        if first:
            wx, wy = out[7:]
        args = own + got + [bases] + prev + [weight, wx, wy] + own_u
        stacked = [jax.ShapeDtypeStruct((2 * f.shape[0], C), F32) for f in FACES]
        outs = FACES + stacked + sends_of(2, 0) + ([BASES] if first else [])
        out = call(functools.partial(second_kernel, first), "second", outs, [S_SQUARE], args, 2)
        lift_1, own_uv, sends = out[:6], out[6:12], out[12:17]
        if first:
            prev = [out[17]]
        got = exchange(sends)
        resp, sums = call(response_kernel, "response", [PADDED, ROW], [S_FIELD, S_PADDED, S_SQUARE, S_SQUARE], lift_1 + [weight], 3)
        args = own_uv + got + [bases] + prev + [weight, wx, wy, sums]
        out = call(third_kernel, "third", FACES + FACES + [SQUARE], [pltpu.VMEM((2, C, C), F32)], args, 2)
        lift_u, lift_v, rows = out[:6], out[6:12], out[12]
        totals = gather_rows(rows)
        if first:
            args = [totals, heat, weight, free, resp] + lift_1 + lift_u + lift_v
            out = call(fourth_kernel, "fourth", [FIELD, PADDED] + FACES + FACES + sends_of(1, 0), [S_PADDED, S_SQUARE, S_SQUARE], args, 5)
            supply, state, held, own, sends = out[0], out[1], out[2:8], out[8:14], out[14:]
    upper = lambda faces: [faces[1], faces[3], faces[5]]
    args = [totals, free, resp] + upper(held) + upper(lift_1) + upper(lift_u) + upper(lift_v)
    state, mx, my, mz = call(last_kernel, "last", [FIELD, FACE, FACE, SQUARE], [], args, 2)
    return state, mx[None, None, None], my[None, None, None], mz[None, None, None]


def solution(mesh):
    field = P("gz", "gx", "gy")
    in_specs = (field, field, P("gz", "gx", "gy", None, None, None), P("gz", "gx", "gy", None, None))
    face = P("gz", "gx", "gy", None, None)
    return jax.shard_map(body, mesh=mesh, in_specs=in_specs, out_specs=(field, face, face, face), check_vma=False)
```

```python
import functools

import jax
import jax.numpy as jnp
from jax import lax
from jax.experimental import pallas as pl
from jax.experimental.pallas import tpu as pltpu
from jax.sharding import PartitionSpec as P

HIGH = lax.Precision.HIGHEST
DAMPING_WEIGHT = 0.8
EPSILON = 1e-06
AXES = ("gx", "gy", "gz")
CZ = 32
C = 128
F32 = jnp.float32
UNROLL = 4
WIDE = 16
PARTS = 4
BLOCK = 16
DEPTH = 8
KEPT = 1.0 - DAMPING_WEIGHT

VM = pl.BlockSpec(memory_space=pltpu.MemorySpace.VMEM)
AWAY = pl.BlockSpec(memory_space=pltpu.MemorySpace.HBM)
BF16 = jnp.bfloat16
PAD = 8


def dot_t(a, b):
    return lax.dot_general(a, b, (((1,), (1,)), ((), ())), precision=HIGH, preferred_element_type=F32)


def parts_of(a):
    first = a.astype(BF16)
    rest = a - first.astype(F32)
    second = rest.astype(BF16)
    third = (rest - second.astype(F32)).astype(BF16)
    return first, second, third


def dot(a, parts, d):
    n = a.shape[0]
    mul = functools.partial(jnp.dot, preferred_element_type=F32)
    a1, a2, a3 = parts_of(a)
    r = mul(jnp.concatenate([a1, a2, a3], axis=0), parts[3 * d])
    s = mul(jnp.concatenate([a1, a2], axis=0), parts[3 * d + 1])
    t = mul(a1, parts[3 * d + 2])
    return r[:n] + (r[n : 2 * n] + s[:n] + (r[2 * n :] + s[n:] + t))


def store_parts(ref, d, a):
    for i, p in enumerate(parts_of(a)):
        ref[3 * d + i] = p


def lane_of(shape):
    return lax.broadcasted_iota(jnp.int32, shape, len(shape) - 1)


def row_of(shape):
    return lax.broadcasted_iota(jnp.int32, shape, len(shape) - 2)


INNER = slice(PAD, PAD + C)


def zero_ends(ref):
    ref[0] = jnp.zeros((C + 2 * PAD, C), F32)
    ref[CZ + 1] = jnp.zeros((C + 2 * PAD, C), F32)
    for z in range(1, CZ + 1):
        ref[z, 0:PAD, :] = jnp.zeros((PAD, C), F32)
        ref[z, PAD + C :, :] = jnp.zeros((PAD, C), F32)


def in_plane(centre):
    shape = centre.shape
    rows = row_of(shape)
    lanes = lane_of(shape)
    near = jnp.where(rows == 0, 0.0, pltpu.roll(centre, 1, 0))
    near = near + jnp.where(rows == shape[0] - 1, 0.0, pltpu.roll(centre, shape[0] - 1, 0))
    near = near + jnp.where(lanes == 0, 0.0, pltpu.roll(centre, 1, 1))
    return near + jnp.where(lanes == C - 1, 0.0, pltpu.roll(centre, C - 1, 1))


def sweep(src, dst, weight, supply):
    lanes = lane_of((BLOCK, C))
    low = lanes == 0
    high = lanes == C - 1

    def planes(i, carry):
        z = i * DEPTH
        for x in range(0, C, BLOCK):
            r = PAD + x
            column = [src[z + j, r : r + BLOCK, :] for j in range(DEPTH + 2)]
            for j in range(DEPTH):
                centre = column[j + 1]
                near = column[j] + column[j + 2]
                near = near + src[z + j + 1, r - 1 : r - 1 + BLOCK, :] + src[z + j + 1, r + 1 : r + 1 + BLOCK, :]
                near = near + jnp.where(low, 0.0, pltpu.roll(centre, 1, 1)) + jnp.where(high, 0.0, pltpu.roll(centre, C - 1, 1))
                dst[z + j + 1, r : r + BLOCK, :] = KEPT * centre + weight[z + j, x : x + BLOCK, :] * (supply[z + j, x : x + BLOCK, :] + near)
        return carry

    lax.fori_loop(0, CZ // DEPTH, planes, 0)


def row_layer(src, base, at, out):
    for z in range(CZ):
        out[z : z + 1, :] = src[z + base, PAD * base + at : PAD * base + at + 1, :]


def column_layers(src, base, turn):
    group = lane_of((C, C)) // 4

    def plane(z, packed):
        return jnp.where(group == z, pltpu.roll(src[z + base, PAD * base : PAD * base + C, :], 4 * z + 2, 1), packed)

    packed = lax.fori_loop(0, CZ, plane, jnp.zeros((C, C), F32), unroll=WIDE)
    turn[...] = packed.T


def layer_rows(i):
    return pl.ds(i, CZ, stride=4)


def pack_columns(turn, low, high):
    turn[...] = jnp.zeros((C, C), F32)
    turn[layer_rows(1), :] = high
    turn[layer_rows(2), :] = low
    return turn[...].T


def column_plane(packed, z):
    lanes = lane_of((C, C))
    edge = (lanes == 0) | (lanes == C - 1)
    return jnp.where(edge, pltpu.roll(packed, C - 2 - 4 * z, 1), 0.0)


def add_rows(dst, faces, sign):
    for z in range(CZ):
        dst[z, 0:1, :] = dst[z, 0:1, :] + sign * faces[0][z : z + 1, :]
        dst[z, C - 1 : C, :] = dst[z, C - 1 : C, :] + sign * faces[1][z : z + 1, :]
    dst[0] = dst[0] + sign * faces[4][...]
    dst[CZ - 1] = dst[CZ - 1] + sign * faces[5][...]


EDGES = (0, 1, C - 2, C - 1)


def rim(low, high, at):
    lanes = lane_of(low.shape)
    a = low if at == 0 else pltpu.roll(low, C - at, 1)
    b = high if at == C - 1 else pltpu.roll(high, C - 1 - at, 1)
    return jnp.where(lanes == 0, a, jnp.where(lanes == C - 1, b, 0.0))


def ends(low, high):
    rows = row_of((CZ, C))
    return jnp.where(rows == 0, low, jnp.where(rows == CZ - 1, high, 0.0))


def lift_layers(faces, turn, inner):
    bx, hx, by, hy, bz, hz = [f[...] for f in faces]
    lanes = lane_of((C, C))
    columns = jnp.where(lanes < 4, pltpu.roll(bz, 2, 1), pltpu.roll(hz, 6, 1)).T
    at = lambda i: columns[i : i + 1, :]
    column = {C - 2: (at(0), at(4)), C - 1: (at(1), at(5)), 0: (at(2), at(6)), 1: (at(3), at(7))}
    edges = EDGES if inner else (0, C - 1)
    on_x = {}
    on_y = {}
    for e in edges:
        on_x[e] = rim(by, hy, e) + ends(bz[e : e + 1, :], hz[e : e + 1, :])
        on_y[e] = rim(bx, hx, e) + ends(*column[e])
    on_x[0] = on_x[0] + bx
    on_x[C - 1] = on_x[C - 1] + hx
    on_y[0] = on_y[0] + by
    on_y[C - 1] = on_y[C - 1] + hy
    packed = pack_columns(turn, by, hy)
    rows = row_of((C, C))
    on_z = {}
    for z in (0, 1, CZ - 2, CZ - 1) if inner else (0, CZ - 1):
        p = column_plane(packed, z)
        p = p + jnp.where(rows == 0, bx[z : z + 1, :], jnp.where(rows == C - 1, hx[z : z + 1, :], 0.0))
        on_z[z] = p + bz if z == 0 else p + hz if z == CZ - 1 else p
    return on_x, on_y, on_z


def layer_weights(weight, wx, wy):
    return (
        {e: wx[i] for i, e in enumerate(EDGES)},
        {e: wy[i] for i, e in enumerate(EDGES)},
        {z: weight[z] for z in (0, 1, CZ - 2, CZ - 1)},
    )


def face_response(layers, weights):
    out = []
    for layer, w, last in zip(layers, weights, (C - 1, C - 1, CZ - 1)):
        for face, inside in ((0, 1), (last, last - 1)):
            once = w[face] * layer[face]
            near = in_plane(once) + w[inside] * layer[inside]
            out.append(KEPT * once + w[face] * (layer[face] + near))
    return out


def fold(t):
    return jnp.sum(t.reshape(t.shape[0] // 8, 8, C), axis=0)


def layer_energy(a, b, weights):
    rows = row_of((CZ, C))
    lanes = lane_of((CZ, C))
    inner = (rows > 0) & (rows < CZ - 1)
    both = inner & (lanes > 0) & (lanes < C - 1)
    acc = jnp.zeros((8, C), F32)
    for layers_a, layers_b, w, last, mask in zip(a, b, weights, (C - 1, C - 1, CZ - 1), (inner, both, None)):
        for e in (0, last):
            t = layers_a[e] * layers_b[e] * w[e]
            acc = acc + fold(t if mask is None else jnp.where(mask, t, 0.0))
    return jnp.sum(acc) / DAMPING_WEIGHT


def places():
    x, y, z = (lax.axis_index(a) for a in AXES)
    more = [i < lax.axis_size(a) - 1 for a, i in zip(AXES, (x, y, z))]
    return x % 2 == 0, y % 2 == 0, z == 0, more


def pick(flag, a, b):
    return lax.select(jnp.broadcast_to(flag, a.shape), a, b)


def pack_sends(sends, faces, index):
    xeven, yeven, zlow, _ = places()
    xa, xb, ya, yb, zz = sends
    for even, a, b, lo, hi in ((xeven, xa, xb, faces[0], faces[1]), (yeven, ya, yb, faces[2], faces[3])):
        s = slice(index * CZ, (index + 1) * CZ)
        a[s, :] = pick(even, hi, lo)
        b[s, :] = pick(even, lo, hi)
    zz[index * C : (index + 1) * C, :] = pick(zlow, faces[5], faces[4])


def own_faces(src, own, turn):
    row_layer(src, 1, 0, own[0])
    row_layer(src, 1, C - 1, own[1])
    column_layers(src, 1, turn)
    own[2][...] = turn[layer_rows(2), :]
    own[3][...] = turn[layer_rows(1), :]
    own[4][...] = src[1, INNER, :]
    own[5][...] = src[CZ, INNER, :]


def first_kernel(heat_in, cond_in, proj_in, segs_in, weight, state, parts, heat, *refs):
    own = refs[:6]
    sends = refs[6:11]
    cond, proj, segs, start, turn, sems, small = refs[11:]
    tables = (pltpu.make_async_copy(proj_in, proj, small.at[0]), pltpu.make_async_copy(segs_in, segs, small.at[1]))
    for c in tables:
        c.start()
    part = CZ // PARTS
    copies = []
    for i in range(PARTS):
        s = pl.ds(i * part, part)
        pair = (
            pltpu.make_async_copy(cond_in.at[s], cond.at[s], sems.at[0, i]),
            pltpu.make_async_copy(heat_in.at[s], heat.at[s], sems.at[1, i]),
        )
        for c in pair:
            c.start()
        copies.append(pair)
    zero_ends(start)
    zero_ends(state)
    for c in tables:
        c.wait()
    for d in range(3):
        onehot = jnp.where(row_of((C, C)) == segs[d : d + 1, :], 1.0, 0.0).astype(BF16)
        base = sum(lax.dot_general(onehot, p, (((1,), (1,)), ((), ())), preferred_element_type=F32) for p in reversed(parts_of(proj[d])))
        store_parts(parts, d, base)
        for a in (sends[:2], sends[2:4])[d] if d < 2 else ():
            a[CZ : CZ + C, :] = base
        if d == 2:
            sends[4][C : 2 * C, :] = base

    def plane(z, carry):
        w = DAMPING_WEIGHT / (6.0 + cond[z])
        weight[z] = w
        start[z + 1, INNER, :] = w * heat[z]
        return carry

    for i, pair in enumerate(copies):
        for c in pair:
            c.wait()
        lax.fori_loop(i * part, (i + 1) * part, plane, 0, unroll=UNROLL)
    sweep(start, state, weight, heat)
    own_faces(state, own, turn)
    pack_sends(sends, [f[...] for f in own], 0)


def free_kernel(first, state, weight, supply, *refs):
    out = refs[0]
    own = refs[1:7]
    mid, turn = refs[-2:]
    zero_ends(mid)
    zero_ends(out)
    sweep(state, mid, weight, supply)
    sweep(mid, out, weight, supply)
    own_faces(out, own, turn)
    if first:
        wx, wy = refs[7:9]
        for i, e in enumerate(EDGES):
            row_layer(weight, 0, e, wx.at[i])
        column_layers(weight, 0, turn)
        for i, e in enumerate((2, 3, 0, 1)):
            wy[i] = turn[layer_rows(e), :]


def jumps(own, got, bases, prev_bases, back_bases, n, lifted):
    xeven, yeven, zlow, more = places()
    xa, xb, ya, yb, zz = got
    for d, (even, a, b, rows) in enumerate(((xeven, xa, xb, n * CZ), (yeven, ya, yb, n * CZ), (zlow, zz, zz, n * C))):
        a = a[0:rows, :]
        b = b[0:rows, :]
        up = own[2 * d + 1][...] - dot(pick(even, a, b), bases, d)
        up = jnp.where(more[d], up, 0.0)
        down = pick(even, b, a) - dot(own[2 * d][...], prev_bases, d)
        back = -dot(down, back_bases, d)
        if d == 2:
            back = jnp.where(zlow, 0.0, back)
        size = rows // n
        for i in range(n):
            lifted[i][2 * d][...] = back[i * size : (i + 1) * size, :]
            lifted[i][2 * d + 1][...] = up[i * size : (i + 1) * size, :]


def square_sum(a, b):
    return jnp.sum(sum(fold(a[i][...] * b[i][...]) for i in (1, 3, 5)))


def row_of_sums(values):
    lanes = lane_of((1, C))
    row = jnp.zeros((1, C), F32)
    for i, v in enumerate(values):
        row = jnp.where(lanes == i, v, row)
    return row


def second_kernel(first, *refs):
    it = iter(refs)
    take = lambda n: [next(it) for _ in range(n)]
    own = take(6)
    got = take(5)
    (bases,) = take(1)
    prev, back = take(2) if not first else (None, None)
    weight, wx, wy = take(3)
    own_u = take(6)
    lifted = take(6)
    own_uv = take(6)
    sends = take(5)
    if first:
        prev, back = take(2)
    (turn,) = take(1)
    xeven, yeven, zlow, _ = places()
    if first:
        xa, xb, ya, yb, zz = got
        for d, base in enumerate((pick(xeven, xb[CZ:, :], xa[CZ:, :]), pick(yeven, yb[CZ:, :], ya[CZ:, :]), zz[C:, :])):
            store_parts(prev, d, base)
            store_parts(back, d, base.T)
    jumps(own, got, bases, prev, back, 1, [lifted])
    response = face_response(lift_layers(lifted, turn, True), layer_weights(weight, wx, wy))
    free = [f[...] for f in own_u]
    for o, u, v in zip(own_uv, free, response):
        n = u.shape[0]
        o[0:n, :] = u
        o[n:, :] = v
    pack_sends(sends, free, 0)
    pack_sends(sends, response, 1)


def response_kernel(*refs):
    lifted = refs[:6]
    weight, resp, sums, lift, mid, turn, cols = refs[6:]
    cols[...] = pack_columns(turn, lifted[2][...], lifted[3][...])

    def plane(z, carry):
        lift[z] = column_plane(cols[...], z)
        return carry

    lax.fori_loop(0, CZ, plane, 0, unroll=WIDE)
    add_rows(lift, lifted, 1.0)
    zero_ends(mid)
    zero_ends(resp)

    def scale(z, acc):
        once = weight[z] * lift[z]
        mid[z + 1, INNER, :] = once
        return acc + fold(once * lift[z])

    acc = lax.fori_loop(0, CZ, scale, jnp.zeros((8, C), F32), unroll=UNROLL)
    sweep(mid, resp, weight, lift)
    sums[...] = row_of_sums([square_sum(lifted, lifted), jnp.sum(acc) / DAMPING_WEIGHT])


def third_kernel(*refs):
    it = iter(refs)
    take = lambda n: [next(it) for _ in range(n)]
    own_uv = take(6)
    got = take(5)
    bases, prev, back, weight, wx, wy, before = take(7)
    lift_u = take(6)
    lift_v = take(6)
    (rows,) = take(1)
    (turn,) = take(1)
    jumps(own_uv, got, bases, prev, back, 2, [lift_u, lift_v])
    weights = layer_weights(weight, wx, wy)
    u = lift_layers(lift_u, turn.at[0], False)
    v = lift_layers(lift_v, turn.at[1], False)
    sums = [square_sum(lift_u, lift_u), square_sum(lift_u, lift_v), square_sum(lift_v, lift_v)]
    sums += [layer_energy(u, u, weights), layer_energy(u, v, weights), layer_energy(v, v, weights)]
    lanes = lane_of((1, C))
    row = row_of_sums([0.0, 0.0] + sums)
    row = jnp.where(lanes < 2, before[...], row)
    rows[...] = jnp.broadcast_to(row, (C, C))


def steps(totals):
    row = jnp.sum(totals[...], axis=0, keepdims=True)
    lanes = lane_of((1, C))
    gg, gh, guu, guv, gvv, huu, huv, hvv = [jnp.sum(jnp.where(lanes == i, row, 0.0), axis=1, keepdims=True) for i in range(8)]
    one = gg / (gh + EPSILON)
    two = (guu - 2.0 * one * guv + one * one * gvv) / (huu - 2.0 * one * huv + one * one * hvv + EPSILON)
    return one, two


def fourth_kernel(*refs):
    it = iter(refs)
    take = lambda n: [next(it) for _ in range(n)]
    totals, heat, weight, free, resp = take(5)
    lift_1 = take(6)
    lift_u = take(6)
    lift_v = take(6)
    supply, state = take(2)
    held = take(6)
    own = take(6)
    sends = take(5)
    mid, turn, cols = take(3)
    one, two = steps(totals)
    for i in range(6):
        held[i][...] = one * lift_1[i][...] + two * (lift_u[i][...] - one * lift_v[i][...])
    cols[...] = pack_columns(turn, held[2][...], held[3][...])
    zero_ends(mid)
    zero_ends(state)

    def plane(z, carry):
        supply[z] = heat[z] - column_plane(cols[...], z)
        state[z + 1, INNER, :] = free[z + 1, INNER, :] - one * resp[z + 1, INNER, :]
        return carry

    lax.fori_loop(0, CZ, plane, 0, unroll=2 * UNROLL)
    add_rows(supply, held, -1.0)
    sweep(state, mid, weight, supply)
    sweep(mid, state, weight, supply)
    own_faces(state, own, turn)
    pack_sends(sends, [f[...] for f in own], 0)


def last_kernel(*refs):
    it = iter(refs)
    take = lambda n: [next(it) for _ in range(n)]
    totals, free, resp = take(3)
    held = take(3)
    lift_3 = take(3)
    lift_u = take(3)
    lift_v = take(3)
    (out,) = take(1)
    outs = take(3)
    state, sems = take(2)
    one, two = steps(totals)

    def plane(z, carry):
        state[z] = free[z + 1, INNER, :] - one * resp[z + 1, INNER, :]
        return carry

    part = CZ // PARTS
    copies = []
    for i in range(PARTS):
        lax.fori_loop(i * part, (i + 1) * part, plane, 0, unroll=UNROLL)
        s = pl.ds(i * part, part)
        copies.append(pltpu.make_async_copy(state.at[s], out.at[s], sems.at[i]))
        copies[-1].start()
    for i in range(3):
        outs[i][...] = held[i][...] + one * lift_3[i][...] + two * (lift_u[i][...] - one * lift_v[i][...])
    for c in copies:
        c.wait()


FIELD = jax.ShapeDtypeStruct((CZ, C, C), F32)
PADDED = jax.ShapeDtypeStruct((CZ + 2, C + 2 * PAD, C), F32)
FACE = jax.ShapeDtypeStruct((CZ, C), F32)
SQUARE = jax.ShapeDtypeStruct((C, C), F32)
FACES = [FACE] * 4 + [SQUARE] * 2
LAYERS = jax.ShapeDtypeStruct((4, CZ, C), F32)
ROW = jax.ShapeDtypeStruct((1, C), F32)
S_FIELD = pltpu.VMEM((CZ, C, C), F32)
S_PADDED = pltpu.VMEM((CZ + 2, C + 2 * PAD, C), F32)
PIECES = jax.ShapeDtypeStruct((9, C, C), BF16)
S_SQUARE = pltpu.VMEM((C, C), F32)


def sends_of(n, extra):
    small = jax.ShapeDtypeStruct((n * CZ + extra, C), F32)
    return [small] * 4 + [jax.ShapeDtypeStruct((n * C + extra, C), F32)]


def call(kernel, name, outs, scratch, args, us, in_specs=None, out_specs=None):
    return list(
        pl.pallas_call(
            kernel,
            out_shape=tuple(outs),
            in_specs=in_specs or [VM] * len(args),
            out_specs=tuple(out_specs or [VM] * len(outs)),
            scratch_shapes=scratch,
            name=name,
            compiler_params=pltpu.CompilerParams(vmem_limit_bytes=40 * 1024 * 1024),
            cost_estimate=pl.CostEstimate(flops=us * 10**7, transcendentals=0, bytes_accessed=2**20),
        )(*args)
    )


def swap_pairs(axis, start):
    n = lax.axis_size(axis)
    pairs = []
    for i in range(start, n - 1, 2):
        pairs += [(i, i + 1), (i + 1, i)]
    return pairs


def exchange(sends):
    xa, xb, ya, yb, zz = sends
    zz = lax.ppermute(zz, "gz", swap_pairs("gz", 0))
    yb = lax.ppermute(yb, "gy", swap_pairs("gy", 1))
    xb = lax.ppermute(xb, "gx", swap_pairs("gx", 1))
    xa = lax.ppermute(xa, "gx", swap_pairs("gx", 0))
    ya = lax.ppermute(ya, "gy", swap_pairs("gy", 0))
    return [xa, xb, ya, yb, zz]


def gather_rows(rows):
    rows = lax.all_to_all(rows.reshape(C, 1, C), AXES, 0, 0)
    return rows.reshape(C, C)


def body(heat, cond, projection, segment_map):
    proj = projection[0, 0, 0]
    segs = segment_map[0, 0, 0]
    dma = pltpu.SemaphoreType.DMA
    scratch = [S_FIELD, pltpu.VMEM(proj.shape, F32), pltpu.VMEM(segs.shape, jnp.int32), S_PADDED, S_SQUARE, dma((2, PARTS)), dma((2,))]
    outs = [FIELD, PADDED, PIECES, FIELD] + FACES + sends_of(1, C)
    out = call(first_kernel, "first", outs, scratch, (heat, cond, proj, segs), 4, [AWAY] * 4)
    weight, state, bases, heat = out[:4]
    own, sends = out[4:10], out[10:]
    supply = heat
    prev = []
    held = None
    for pair in range(2):
        first = pair == 0
        got = exchange(sends)
        outs = [PADDED] + FACES + ([LAYERS, LAYERS] if first else [])
        out = call(functools.partial(free_kernel, first), "free", outs, [S_PADDED, S_SQUARE], (state, weight, supply), 3)
        free, own_u = out[0], out[1:7]
        if first:
            wx, wy = out[7:]
        args = own + got + [bases] + prev + [weight, wx, wy] + own_u
        stacked = [jax.ShapeDtypeStruct((2 * f.shape[0], C), F32) for f in FACES]
        outs = FACES + stacked + sends_of(2, 0) + ([PIECES, PIECES] if first else [])
        out = call(functools.partial(second_kernel, first), "second", outs, [S_SQUARE], args, 2)
        lift_1, own_uv, sends = out[:6], out[6:12], out[12:17]
        if first:
            prev = out[17:]
        got = exchange(sends)
        resp, sums = call(response_kernel, "response", [PADDED, ROW], [S_FIELD, S_PADDED, S_SQUARE, S_SQUARE], lift_1 + [weight], 3)
        args = own_uv + got + [bases] + prev + [weight, wx, wy, sums]
        out = call(third_kernel, "third", FACES + FACES + [SQUARE], [pltpu.VMEM((2, C, C), F32)], args, 2)
        lift_u, lift_v, rows = out[:6], out[6:12], out[12]
        totals = gather_rows(rows)
        if first:
            args = [totals, heat, weight, free, resp] + lift_1 + lift_u + lift_v
            out = call(fourth_kernel, "fourth", [FIELD, PADDED] + FACES + FACES + sends_of(1, 0), [S_PADDED, S_SQUARE, S_SQUARE], args, 5)
            supply, state, held, own, sends = out[0], out[1], out[2:8], out[8:14], out[14:]
    upper = lambda faces: [faces[1], faces[3], faces[5]]
    args = [totals, free, resp] + upper(held) + upper(lift_1) + upper(lift_u) + upper(lift_v)
    state, mx, my, mz = call(last_kernel, "last", [FIELD, FACE, FACE, SQUARE], [S_FIELD, dma((PARTS,))], args, 2, None, [AWAY, VM, VM, VM])
    return state, mx[None, None, None], my[None, None, None], mz[None, None, None]


def solution(mesh):
    field = P("gz", "gx", "gy")
    in_specs = (field, field, P("gz", "gx", "gy", None, None, None), P("gz", "gx", "gy", None, None))
    face = P("gz", "gx", "gy", None, None)
    return jax.shard_map(body, mesh=mesh, in_specs=in_specs, out_specs=(field, face, face, face), check_vma=False)
```

```python
import functools

import jax
import jax.numpy as jnp
from jax import lax
from jax.experimental import pallas as pl
from jax.experimental.pallas import tpu as pltpu
from jax.sharding import PartitionSpec as P

HIGH = lax.Precision.HIGHEST
DAMPING_WEIGHT = 0.8
EPSILON = 1e-06
AXES = ("gx", "gy", "gz")
CZ = 32
C = 128
F32 = jnp.float32
UNROLL = 4
WIDE = 16
PARTS = 4
BLOCK = 16
DEPTH = 8
KEPT = 1.0 - DAMPING_WEIGHT

VM = pl.BlockSpec(memory_space=pltpu.MemorySpace.VMEM)
AWAY = pl.BlockSpec(memory_space=pltpu.MemorySpace.HBM)
BF16 = jnp.bfloat16
PAD = 8


def dot_t(a, b):
    return lax.dot_general(a, b, (((1,), (1,)), ((), ())), precision=HIGH, preferred_element_type=F32)


def parts_of(a):
    first = a.astype(BF16)
    rest = a - first.astype(F32)
    second = rest.astype(BF16)
    third = (rest - second.astype(F32)).astype(BF16)
    return first, second, third


def dot(a, parts, d):
    n = a.shape[0]
    mul = functools.partial(jnp.dot, preferred_element_type=F32)
    a1, a2, a3 = parts_of(a)
    r = mul(jnp.concatenate([a1, a2, a3], axis=0), parts[3 * d])
    s = mul(jnp.concatenate([a1, a2], axis=0), parts[3 * d + 1])
    t = mul(a1, parts[3 * d + 2])
    return r[:n] + (r[n : 2 * n] + s[:n] + (r[2 * n :] + s[n:] + t))


def store_parts(ref, d, a):
    for i, p in enumerate(parts_of(a)):
        ref[3 * d + i] = p


def lane_of(shape):
    return lax.broadcasted_iota(jnp.int32, shape, len(shape) - 1)


def row_of(shape):
    return lax.broadcasted_iota(jnp.int32, shape, len(shape) - 2)


INNER = slice(PAD, PAD + C)


def zero_ends(ref):
    ref[0] = jnp.zeros((C + 2 * PAD, C), F32)
    ref[CZ + 1] = jnp.zeros((C + 2 * PAD, C), F32)
    for z in range(1, CZ + 1):
        ref[z, 0:PAD, :] = jnp.zeros((PAD, C), F32)
        ref[z, PAD + C :, :] = jnp.zeros((PAD, C), F32)


def in_plane(centre):
    shape = centre.shape
    rows = row_of(shape)
    lanes = lane_of(shape)
    near = jnp.where(rows == 0, 0.0, pltpu.roll(centre, 1, 0))
    near = near + jnp.where(rows == shape[0] - 1, 0.0, pltpu.roll(centre, shape[0] - 1, 0))
    near = near + jnp.where(lanes == 0, 0.0, pltpu.roll(centre, 1, 1))
    return near + jnp.where(lanes == C - 1, 0.0, pltpu.roll(centre, C - 1, 1))


def sweep(src, dst, weight, supply):
    lanes = lane_of((BLOCK, C))
    low = lanes == 0
    high = lanes == C - 1

    def planes(i, carry):
        z = i * DEPTH
        for x in range(0, C, BLOCK):
            r = PAD + x
            column = [src[z + j, r : r + BLOCK, :] for j in range(DEPTH + 2)]
            for j in range(DEPTH):
                centre = column[j + 1]
                near = column[j] + column[j + 2]
                near = near + src[z + j + 1, r - 1 : r - 1 + BLOCK, :] + src[z + j + 1, r + 1 : r + 1 + BLOCK, :]
                near = near + jnp.where(low, 0.0, pltpu.roll(centre, 1, 1)) + jnp.where(high, 0.0, pltpu.roll(centre, C - 1, 1))
                dst[z + j + 1, r : r + BLOCK, :] = KEPT * centre + weight[z + j, x : x + BLOCK, :] * (supply[z + j, x : x + BLOCK, :] + near)
        return carry

    lax.fori_loop(0, CZ // DEPTH, planes, 0)


def row_layer(src, base, at, out):
    for z in range(CZ):
        out[z : z + 1, :] = src[z + base, PAD * base + at : PAD * base + at + 1, :]


def column_layers(src, base, turn):
    group = lane_of((C, C)) // 4

    def plane(z, packed):
        return jnp.where(group == z, pltpu.roll(src[z + base, PAD * base : PAD * base + C, :], 4 * z + 2, 1), packed)

    packed = lax.fori_loop(0, CZ, plane, jnp.zeros((C, C), F32), unroll=WIDE)
    turn[...] = packed.T


def layer_rows(i):
    return pl.ds(i, CZ, stride=4)


def pack_columns(turn, low, high):
    turn[...] = jnp.zeros((C, C), F32)
    turn[layer_rows(1), :] = high
    turn[layer_rows(2), :] = low
    return turn[...].T


def column_plane(packed, z):
    lanes = lane_of((C, C))
    edge = (lanes == 0) | (lanes == C - 1)
    return jnp.where(edge, pltpu.roll(packed, C - 2 - 4 * z, 1), 0.0)


def add_rows(dst, faces, sign):
    for z in range(CZ):
        dst[z, 0:1, :] = dst[z, 0:1, :] + sign * faces[0][z : z + 1, :]
        dst[z, C - 1 : C, :] = dst[z, C - 1 : C, :] + sign * faces[1][z : z + 1, :]
    dst[0] = dst[0] + sign * faces[4][...]
    dst[CZ - 1] = dst[CZ - 1] + sign * faces[5][...]


EDGES = (0, 1, C - 2, C - 1)


def rim(low, high, at):
    lanes = lane_of(low.shape)
    a = low if at == 0 else pltpu.roll(low, C - at, 1)
    b = high if at == C - 1 else pltpu.roll(high, C - 1 - at, 1)
    return jnp.where(lanes == 0, a, jnp.where(lanes == C - 1, b, 0.0))


def ends(low, high):
    rows = row_of((CZ, C))
    return jnp.where(rows == 0, low, jnp.where(rows == CZ - 1, high, 0.0))


def lift_layers(faces, turn, inner):
    bx, hx, by, hy, bz, hz = [f[...] for f in faces]
    lanes = lane_of((C, C))
    columns = jnp.where(lanes < 4, pltpu.roll(bz, 2, 1), pltpu.roll(hz, 6, 1)).T
    at = lambda i: columns[i : i + 1, :]
    column = {C - 2: (at(0), at(4)), C - 1: (at(1), at(5)), 0: (at(2), at(6)), 1: (at(3), at(7))}
    edges = EDGES if inner else (0, C - 1)
    on_x = {}
    on_y = {}
    for e in edges:
        on_x[e] = rim(by, hy, e) + ends(bz[e : e + 1, :], hz[e : e + 1, :])
        on_y[e] = rim(bx, hx, e) + ends(*column[e])
    on_x[0] = on_x[0] + bx
    on_x[C - 1] = on_x[C - 1] + hx
    on_y[0] = on_y[0] + by
    on_y[C - 1] = on_y[C - 1] + hy
    packed = pack_columns(turn, by, hy)
    rows = row_of((C, C))
    on_z = {}
    for z in (0, 1, CZ - 2, CZ - 1) if inner else (0, CZ - 1):
        p = column_plane(packed, z)
        p = p + jnp.where(rows == 0, bx[z : z + 1, :], jnp.where(rows == C - 1, hx[z : z + 1, :], 0.0))
        on_z[z] = p + bz if z == 0 else p + hz if z == CZ - 1 else p
    return on_x, on_y, on_z


def layer_weights(weight, wx, wy):
    return (
        {e: wx[i] for i, e in enumerate(EDGES)},
        {e: wy[i] for i, e in enumerate(EDGES)},
        {z: weight[z] for z in (0, 1, CZ - 2, CZ - 1)},
    )


def face_response(layers, weights):
    out = []
    for layer, w, last in zip(layers, weights, (C - 1, C - 1, CZ - 1)):
        for face, inside in ((0, 1), (last, last - 1)):
            once = w[face] * layer[face]
            near = in_plane(once) + w[inside] * layer[inside]
            out.append(KEPT * once + w[face] * (layer[face] + near))
    return out


def fold(t):
    return jnp.sum(t.reshape(t.shape[0] // 8, 8, C), axis=0)


def layer_energy(a, b, weights):
    rows = row_of((CZ, C))
    lanes = lane_of((CZ, C))
    inner = (rows > 0) & (rows < CZ - 1)
    both = inner & (lanes > 0) & (lanes < C - 1)
    acc = jnp.zeros((8, C), F32)
    for layers_a, layers_b, w, last, mask in zip(a, b, weights, (C - 1, C - 1, CZ - 1), (inner, both, None)):
        for e in (0, last):
            t = layers_a[e] * layers_b[e] * w[e]
            acc = acc + fold(t if mask is None else jnp.where(mask, t, 0.0))
    return jnp.sum(acc) / DAMPING_WEIGHT


def places():
    x, y, z = (lax.axis_index(a) for a in AXES)
    more = [i < lax.axis_size(a) - 1 for a, i in zip(AXES, (x, y, z))]
    return x % 2 == 0, y % 2 == 0, z == 0, more


def pick(flag, a, b):
    return lax.select(jnp.broadcast_to(flag, a.shape), a, b)


def pack_sends(sends, faces, index):
    xeven, yeven, zlow, _ = places()
    xa, xb, ya, yb, zz = sends
    for even, a, b, lo, hi in ((xeven, xa, xb, faces[0], faces[1]), (yeven, ya, yb, faces[2], faces[3])):
        s = slice(index * CZ, (index + 1) * CZ)
        a[s, :] = pick(even, hi, lo)
        b[s, :] = pick(even, lo, hi)
    zz[index * C : (index + 1) * C, :] = pick(zlow, faces[5], faces[4])


def own_faces(src, own, turn):
    row_layer(src, 1, 0, own[0])
    row_layer(src, 1, C - 1, own[1])
    column_layers(src, 1, turn)
    own[2][...] = turn[layer_rows(2), :]
    own[3][...] = turn[layer_rows(1), :]
    own[4][...] = src[1, INNER, :]
    own[5][...] = src[CZ, INNER, :]


def first_kernel(heat_in, cond_in, proj_in, segs_in, weight, state, parts, heat, *refs):
    own = refs[:6]
    sends = refs[6:11]
    cond, proj, segs, start, turn, sems, small = refs[11:]
    tables = (pltpu.make_async_copy(proj_in, proj, small.at[0]), pltpu.make_async_copy(segs_in, segs, small.at[1]))
    for c in tables:
        c.start()
    part = CZ // PARTS
    copies = []
    for i in range(PARTS):
        s = pl.ds(i * part, part)
        pair = (
            pltpu.make_async_copy(cond_in.at[s], cond.at[s], sems.at[0, i]),
            pltpu.make_async_copy(heat_in.at[s], heat.at[s], sems.at[1, i]),
        )
        for c in pair:
            c.start()
        copies.append(pair)
    zero_ends(start)
    zero_ends(state)
    for c in tables:
        c.wait()
    for d in range(3):
        onehot = jnp.where(row_of((C, C)) == segs[d], 1.0, 0.0).astype(BF16)
        base = sum(lax.dot_general(onehot, p, (((1,), (1,)), ((), ())), preferred_element_type=F32) for p in reversed(parts_of(proj[d])))
        store_parts(parts, d, base)
        for a in (sends[:2], sends[2:4])[d] if d < 2 else ():
            a[CZ : CZ + C, :] = base
        if d == 2:
            sends[4][C : 2 * C, :] = base

    def plane(z, carry):
        w = DAMPING_WEIGHT / (6.0 + cond[z])
        weight[z] = w
        start[z + 1, INNER, :] = w * heat[z]
        return carry

    for i, pair in enumerate(copies):
        for c in pair:
            c.wait()
        lax.fori_loop(i * part, (i + 1) * part, plane, 0, unroll=UNROLL)
    sweep(start, state, weight, heat)
    own_faces(state, own, turn)
    pack_sends(sends, [f[...] for f in own], 0)


def free_kernel(first, state, weight, supply, *refs):
    out = refs[0]
    own = refs[1:7]
    mid, turn = refs[-2:]
    zero_ends(mid)
    zero_ends(out)
    sweep(state, mid, weight, supply)
    sweep(mid, out, weight, supply)
    own_faces(out, own, turn)
    if first:
        wx, wy = refs[7:9]
        for i, e in enumerate(EDGES):
            row_layer(weight, 0, e, wx.at[i])
        column_layers(weight, 0, turn)
        for i, e in enumerate((2, 3, 0, 1)):
            wy[i] = turn[layer_rows(e), :]


def jumps(own, got, bases, prev_bases, back_bases, n, lifted):
    xeven, yeven, zlow, more = places()
    xa, xb, ya, yb, zz = got
    for d, (even, a, b, rows) in enumerate(((xeven, xa, xb, n * CZ), (yeven, ya, yb, n * CZ), (zlow, zz, zz, n * C))):
        a = a[0:rows, :]
        b = b[0:rows, :]
        up = own[2 * d + 1][...] - dot(pick(even, a, b), bases, d)
        up = jnp.where(more[d], up, 0.0)
        down = pick(even, b, a) - dot(own[2 * d][...], prev_bases, d)
        back = -dot(down, back_bases, d)
        if d == 2:
            back = jnp.where(zlow, 0.0, back)
        size = rows // n
        for i in range(n):
            lifted[i][2 * d][...] = back[i * size : (i + 1) * size, :]
            lifted[i][2 * d + 1][...] = up[i * size : (i + 1) * size, :]


def square_sum(a, b):
    return jnp.sum(sum(fold(a[i][...] * b[i][...]) for i in (1, 3, 5)))


def row_of_sums(values):
    lanes = lane_of((1, C))
    row = jnp.zeros((1, C), F32)
    for i, v in enumerate(values):
        row = jnp.where(lanes == i, v, row)
    return row


def second_kernel(first, *refs):
    it = iter(refs)
    take = lambda n: [next(it) for _ in range(n)]
    own = take(6)
    got = take(5)
    (bases,) = take(1)
    prev, back = take(2) if not first else (None, None)
    weight, wx, wy = take(3)
    own_u = take(6)
    lifted = take(6)
    own_uv = take(6)
    sends = take(5)
    if first:
        prev, back = take(2)
    (turn,) = take(1)
    xeven, yeven, zlow, _ = places()
    if first:
        xa, xb, ya, yb, zz = got
        for d, base in enumerate((pick(xeven, xb[CZ:, :], xa[CZ:, :]), pick(yeven, yb[CZ:, :], ya[CZ:, :]), zz[C:, :])):
            store_parts(prev, d, base)
            store_parts(back, d, base.T)
    jumps(own, got, bases, prev, back, 1, [lifted])
    response = face_response(lift_layers(lifted, turn, True), layer_weights(weight, wx, wy))
    free = [f[...] for f in own_u]
    for o, u, v in zip(own_uv, free, response):
        n = u.shape[0]
        o[0:n, :] = u
        o[n:, :] = v
    pack_sends(sends, free, 0)
    pack_sends(sends, response, 1)


def response_kernel(*refs):
    lifted = refs[:6]
    weight, resp, sums, lift, mid, turn, cols = refs[6:]
    cols[...] = pack_columns(turn, lifted[2][...], lifted[3][...])

    def plane(z, carry):
        lift[z] = column_plane(cols[...], z)
        return carry

    lax.fori_loop(0, CZ, plane, 0, unroll=WIDE)
    add_rows(lift, lifted, 1.0)
    zero_ends(mid)
    zero_ends(resp)

    def scale(z, acc):
        once = weight[z] * lift[z]
        mid[z + 1, INNER, :] = once
        return acc + fold(once * lift[z])

    acc = lax.fori_loop(0, CZ, scale, jnp.zeros((8, C), F32), unroll=UNROLL)
    sweep(mid, resp, weight, lift)
    sums[...] = row_of_sums([square_sum(lifted, lifted), jnp.sum(acc) / DAMPING_WEIGHT])


def merge_sides(low, high):
    return [f for pair in zip(low, high) for f in pair]


def third_kernel(first, *refs):
    it = iter(refs)
    take = lambda n: [next(it) for _ in range(n)]
    own_uv = take(6)
    got = take(5)
    bases, prev, back, weight, wx, wy, before = take(7)
    high_u, high_v = take(3), take(3)
    (rows,) = take(1)
    low_u, low_v = take(3), take(3)
    (turn,) = take(1)
    lift_u = merge_sides(low_u, high_u)
    lift_v = merge_sides(low_v, high_v)
    jumps(own_uv, got, bases, prev, back, 2, [lift_u, lift_v])
    weights = layer_weights(weight, wx, wy)
    u = lift_layers(lift_u, turn.at[0], False)
    v = lift_layers(lift_v, turn.at[1], False)
    sums = [square_sum(lift_u, lift_u), square_sum(lift_u, lift_v), square_sum(lift_v, lift_v)]
    sums += [layer_energy(u, u, weights), layer_energy(u, v, weights), layer_energy(v, v, weights)]
    lanes = lane_of((1, C))
    row = row_of_sums([0.0, 0.0] + sums)
    row = jnp.where(lanes < 2, before[...], row)
    rows[...] = jnp.broadcast_to(row, (C, C))


def steps(totals):
    row = jnp.sum(totals[...], axis=0, keepdims=True)
    lanes = lane_of((1, C))
    gg, gh, guu, guv, gvv, huu, huv, hvv = [jnp.sum(jnp.where(lanes == i, row, 0.0), axis=1, keepdims=True) for i in range(8)]
    one = gg / (gh + EPSILON)
    two = (guu - 2.0 * one * guv + one * one * gvv) / (huu - 2.0 * one * huv + one * one * hvv + EPSILON)
    return one, two


def fourth_kernel(*refs):
    it = iter(refs)
    take = lambda n: [next(it) for _ in range(n)]
    totals, heat, weight, free, resp = take(5)
    lift_1 = take(6)
    lift_u = take(6)
    lift_v = take(6)
    supply, state = take(2)
    high = take(3)
    own = take(6)
    sends = take(5)
    low = take(3)
    mid, turn, cols = take(3)
    held = merge_sides(low, high)
    one, two = steps(totals)
    for i in range(6):
        held[i][...] = one * lift_1[i][...] + two * (lift_u[i][...] - one * lift_v[i][...])
    cols[...] = pack_columns(turn, held[2][...], held[3][...])
    zero_ends(mid)
    zero_ends(state)

    def plane(z, carry):
        supply[z] = heat[z] - column_plane(cols[...], z)
        state[z + 1, INNER, :] = free[z + 1, INNER, :] - one * resp[z + 1, INNER, :]
        return carry

    lax.fori_loop(0, CZ, plane, 0, unroll=2 * UNROLL)
    add_rows(supply, held, -1.0)
    sweep(state, mid, weight, supply)
    sweep(mid, state, weight, supply)
    own_faces(state, own, turn)
    pack_sends(sends, [f[...] for f in own], 0)


def last_kernel(*refs):
    it = iter(refs)
    take = lambda n: [next(it) for _ in range(n)]
    totals, free, resp = take(3)
    held = take(3)
    lift_3 = take(3)
    lift_u = take(3)
    lift_v = take(3)
    (out,) = take(1)
    outs = take(3)
    state, sems = take(2)
    one, two = steps(totals)

    def plane(z, carry):
        state[z] = free[z + 1, INNER, :] - one * resp[z + 1, INNER, :]
        return carry

    part = CZ // PARTS
    copies = []
    for i in range(PARTS):
        lax.fori_loop(i * part, (i + 1) * part, plane, 0, unroll=UNROLL)
        s = pl.ds(i * part, part)
        copies.append(pltpu.make_async_copy(state.at[s], out.at[s], sems.at[i]))
        copies[-1].start()
    for i in range(3):
        outs[i][...] = held[i][...] + one * lift_3[i][...] + two * (lift_u[i][...] - one * lift_v[i][...])
    for c in copies:
        c.wait()


FIELD = jax.ShapeDtypeStruct((CZ, C, C), F32)
PADDED = jax.ShapeDtypeStruct((CZ + 2, C + 2 * PAD, C), F32)
FACE = jax.ShapeDtypeStruct((CZ, C), F32)
SQUARE = jax.ShapeDtypeStruct((C, C), F32)
FACES = [FACE] * 4 + [SQUARE] * 2
LAYERS = jax.ShapeDtypeStruct((4, CZ, C), F32)
ROW = jax.ShapeDtypeStruct((1, C), F32)
SIDE = [FACE, FACE, SQUARE]
S_SIDE = [pltpu.VMEM(f.shape, F32) for f in SIDE]
S_FIELD = pltpu.VMEM((CZ, C, C), F32)
S_PADDED = pltpu.VMEM((CZ + 2, C + 2 * PAD, C), F32)
PIECES = jax.ShapeDtypeStruct((9, C, C), BF16)
S_SQUARE = pltpu.VMEM((C, C), F32)


def sends_of(n, extra):
    small = jax.ShapeDtypeStruct((n * CZ + extra, C), F32)
    return [small] * 4 + [jax.ShapeDtypeStruct((n * C + extra, C), F32)]


def call(kernel, name, outs, scratch, args, us, in_specs=None, out_specs=None):
    return list(
        pl.pallas_call(
            kernel,
            out_shape=tuple(outs),
            in_specs=in_specs or [VM] * len(args),
            out_specs=tuple(out_specs or [VM] * len(outs)),
            scratch_shapes=scratch,
            name=name,
            compiler_params=pltpu.CompilerParams(vmem_limit_bytes=20 * 1024 * 1024),
            cost_estimate=pl.CostEstimate(flops=us * 10**7, transcendentals=0, bytes_accessed=2**20),
        )(*args)
    )


def swap_pairs(axis, start):
    n = lax.axis_size(axis)
    pairs = []
    for i in range(start, n - 1, 2):
        pairs += [(i, i + 1), (i + 1, i)]
    return pairs


def exchange(sends):
    xa, xb, ya, yb, zz = sends
    zz = lax.ppermute(zz, "gz", swap_pairs("gz", 0))
    yb = lax.ppermute(yb, "gy", swap_pairs("gy", 1))
    xb = lax.ppermute(xb, "gx", swap_pairs("gx", 1))
    xa = lax.ppermute(xa, "gx", swap_pairs("gx", 0))
    ya = lax.ppermute(ya, "gy", swap_pairs("gy", 0))
    return [xa, xb, ya, yb, zz]


def gather_rows(rows):
    rows = lax.all_to_all(rows.reshape(C, 1, C), AXES, 0, 0)
    return rows.reshape(C, C)


def body(heat, cond, projection, segment_map):
    proj = projection[0, 0, 0]
    segs = segment_map.reshape(3, 1, C)
    dma = pltpu.SemaphoreType.DMA
    scratch = [S_FIELD, pltpu.VMEM(proj.shape, F32), pltpu.VMEM(segs.shape, jnp.int32), S_PADDED, S_SQUARE, dma((2, PARTS)), dma((2,))]
    outs = [FIELD, PADDED, PIECES, FIELD] + FACES + sends_of(1, C)
    out = call(first_kernel, "first", outs, scratch, [pltpu.with_memory_space_constraint(a, pltpu.MemorySpace.HBM) for a in (heat, cond, proj, segs)], 4, [AWAY] * 4)
    weight, state, bases, heat = out[:4]
    own, sends = out[4:10], out[10:]
    supply = heat
    prev = []
    held = None
    for pair in range(2):
        first = pair == 0
        got = exchange(sends)
        outs = [PADDED] + FACES + ([LAYERS, LAYERS] if first else [])
        out = call(functools.partial(free_kernel, first), "free", outs, [S_PADDED, S_SQUARE], (state, weight, supply), 3)
        free, own_u = out[0], out[1:7]
        if first:
            wx, wy = out[7:]
        args = own + got + [bases] + prev + [weight, wx, wy] + own_u
        stacked = [jax.ShapeDtypeStruct((2 * f.shape[0], C), F32) for f in FACES]
        outs = FACES + stacked + sends_of(2, 0) + ([PIECES, PIECES] if first else [])
        out = call(functools.partial(second_kernel, first), "second", outs, [S_SQUARE], args, 2)
        lift_1, own_uv, sends = out[:6], out[6:12], out[12:17]
        if first:
            prev = out[17:]
        got = exchange(sends)
        resp, sums = call(response_kernel, "response", [PADDED, ROW], [S_FIELD, S_PADDED, S_SQUARE, S_SQUARE], lift_1 + [weight], 3)
        args = own_uv + got + [bases] + prev + [weight, wx, wy, sums]
        outs = SIDE + SIDE + [SQUARE] + (SIDE + SIDE if first else [])
        scratch = ([] if first else S_SIDE + S_SIDE) + [pltpu.VMEM((2, C, C), F32)]
        out = call(functools.partial(third_kernel, first), "third", outs, scratch, args, 2)
        high_u, high_v, rows = out[:3], out[3:6], out[6]
        totals = gather_rows(rows)
        if first:
            args = [totals, heat, weight, free, resp] + lift_1 + merge_sides(out[7:10], high_u) + merge_sides(out[10:13], high_v)
            outs = [FIELD, PADDED] + SIDE + FACES + sends_of(1, 0)
            out = call(fourth_kernel, "fourth", outs, S_SIDE + [S_PADDED, S_SQUARE, S_SQUARE], args, 5)
            supply, state, held, own, sends = out[0], out[1], out[2:5], out[5:11], out[11:]
    args = [totals, free, resp] + held + [lift_1[i] for i in (1, 3, 5)] + high_u + high_v
    state, mx, my, mz = call(last_kernel, "last", [FIELD, FACE, FACE, SQUARE], [S_FIELD, dma((PARTS,))], args, 2, None, [AWAY, VM, VM, VM])
    return state, mx[None, None, None], my[None, None, None], mz[None, None, None]


def solution(mesh):
    field = P("gz", "gx", "gy")
    in_specs = (field, field, P("gz", "gx", "gy", None, None, None), P("gz", "gx", "gy", None, None))
    face = P("gz", "gx", "gy", None, None)
    return jax.shard_map(body, mesh=mesh, in_specs=in_specs, out_specs=(field, face, face, face), check_vma=False)
```

```python
import functools

import jax
import jax.numpy as jnp
from jax import lax
from jax.experimental import pallas as pl
from jax.experimental.pallas import tpu as pltpu
from jax.sharding import PartitionSpec as P

HIGH = lax.Precision.HIGHEST
DAMPING_WEIGHT = 0.8
EPSILON = 1e-06
AXES = ("gx", "gy", "gz")
CZ = 32
C = 128
F32 = jnp.float32
UNROLL = 4
WIDE = 16
PARTS = 4
BLOCK = 16
DEPTH = 8
KEPT = 1.0 - DAMPING_WEIGHT

VM = pl.BlockSpec(memory_space=pltpu.MemorySpace.VMEM)
AWAY = pl.BlockSpec(memory_space=pltpu.MemorySpace.HBM)
BF16 = jnp.bfloat16
PAD = 8


def dot_t(a, b):
    return lax.dot_general(a, b, (((1,), (1,)), ((), ())), precision=HIGH, preferred_element_type=F32)


def parts_of(a):
    first = a.astype(BF16)
    rest = a - first.astype(F32)
    second = rest.astype(BF16)
    third = (rest - second.astype(F32)).astype(BF16)
    return first, second, third


def dot(a, parts, d):
    n = a.shape[0]
    mul = functools.partial(jnp.dot, preferred_element_type=F32)
    a1, a2, a3 = parts_of(a)
    r = mul(jnp.concatenate([a1, a2, a3], axis=0), parts[3 * d])
    s = mul(jnp.concatenate([a1, a2], axis=0), parts[3 * d + 1])
    t = mul(a1, parts[3 * d + 2])
    return r[:n] + (r[n : 2 * n] + s[:n] + (r[2 * n :] + s[n:] + t))


def store_parts(ref, d, a):
    for i, p in enumerate(parts_of(a)):
        ref[3 * d + i] = p


def lane_of(shape):
    return lax.broadcasted_iota(jnp.int32, shape, len(shape) - 1)


def row_of(shape):
    return lax.broadcasted_iota(jnp.int32, shape, len(shape) - 2)


INNER = slice(PAD, PAD + C)


def zero_ends(ref):
    ref[0] = jnp.zeros((C + 2 * PAD, C), F32)
    ref[CZ + 1] = jnp.zeros((C + 2 * PAD, C), F32)
    for z in range(1, CZ + 1):
        ref[z, 0:PAD, :] = jnp.zeros((PAD, C), F32)
        ref[z, PAD + C :, :] = jnp.zeros((PAD, C), F32)


def in_plane(centre):
    shape = centre.shape
    rows = row_of(shape)
    lanes = lane_of(shape)
    near = jnp.where(rows == 0, 0.0, pltpu.roll(centre, 1, 0))
    near = near + jnp.where(rows == shape[0] - 1, 0.0, pltpu.roll(centre, shape[0] - 1, 0))
    near = near + jnp.where(lanes == 0, 0.0, pltpu.roll(centre, 1, 1))
    return near + jnp.where(lanes == C - 1, 0.0, pltpu.roll(centre, C - 1, 1))


def sweep(src, dst, weight, supply):
    lanes = lane_of((BLOCK, C))
    low = lanes == 0
    high = lanes == C - 1

    def planes(i, carry):
        z = i * DEPTH
        for x in range(0, C, BLOCK):
            r = PAD + x
            column = [src[z + j, r : r + BLOCK, :] for j in range(DEPTH + 2)]
            for j in range(DEPTH):
                centre = column[j + 1]
                near = column[j] + column[j + 2]
                near = near + src[z + j + 1, r - 1 : r - 1 + BLOCK, :] + src[z + j + 1, r + 1 : r + 1 + BLOCK, :]
                near = near + jnp.where(low, 0.0, pltpu.roll(centre, 1, 1)) + jnp.where(high, 0.0, pltpu.roll(centre, C - 1, 1))
                dst[z + j + 1, r : r + BLOCK, :] = KEPT * centre + weight[z + j, x : x + BLOCK, :] * (supply[z + j, x : x + BLOCK, :] + near)
        return carry

    lax.fori_loop(0, CZ // DEPTH, planes, 0)


def row_layer(src, base, at, out):
    for z in range(CZ):
        out[z : z + 1, :] = src[z + base, PAD * base + at : PAD * base + at + 1, :]


def column_layers(src, base, turn):
    group = lane_of((C, C)) // 4

    def plane(z, packed):
        return jnp.where(group == z, pltpu.roll(src[z + base, PAD * base : PAD * base + C, :], 4 * z + 2, 1), packed)

    packed = lax.fori_loop(0, CZ, plane, jnp.zeros((C, C), F32), unroll=WIDE)
    turn[...] = packed.T


def layer_rows(i):
    return pl.ds(i, CZ, stride=4)


def pack_columns(turn, low, high):
    turn[...] = jnp.zeros((C, C), F32)
    turn[layer_rows(1), :] = high
    turn[layer_rows(2), :] = low
    return turn[...].T


def column_plane(packed, z):
    lanes = lane_of((C, C))
    edge = (lanes == 0) | (lanes == C - 1)
    return jnp.where(edge, pltpu.roll(packed, C - 2 - 4 * z, 1), 0.0)


def add_rows(dst, faces, sign):
    for z in range(CZ):
        dst[z, 0:1, :] = dst[z, 0:1, :] + sign * faces[0][z : z + 1, :]
        dst[z, C - 1 : C, :] = dst[z, C - 1 : C, :] + sign * faces[1][z : z + 1, :]
    dst[0] = dst[0] + sign * faces[4][...]
    dst[CZ - 1] = dst[CZ - 1] + sign * faces[5][...]


EDGES = (0, 1, C - 2, C - 1)


def rim(low, high, at):
    lanes = lane_of(low.shape)
    a = low if at == 0 else pltpu.roll(low, C - at, 1)
    b = high if at == C - 1 else pltpu.roll(high, C - 1 - at, 1)
    return jnp.where(lanes == 0, a, jnp.where(lanes == C - 1, b, 0.0))


def ends(low, high):
    rows = row_of((CZ, C))
    return jnp.where(rows == 0, low, jnp.where(rows == CZ - 1, high, 0.0))


def lift_layers(faces, turn, inner):
    bx, hx, by, hy, bz, hz = [f[...] for f in faces]
    lanes = lane_of((C, C))
    columns = jnp.where(lanes < 4, pltpu.roll(bz, 2, 1), pltpu.roll(hz, 6, 1)).T
    at = lambda i: columns[i : i + 1, :]
    column = {C - 2: (at(0), at(4)), C - 1: (at(1), at(5)), 0: (at(2), at(6)), 1: (at(3), at(7))}
    edges = EDGES if inner else (0, C - 1)
    on_x = {}
    on_y = {}
    for e in edges:
        on_x[e] = rim(by, hy, e) + ends(bz[e : e + 1, :], hz[e : e + 1, :])
        on_y[e] = rim(bx, hx, e) + ends(*column[e])
    on_x[0] = on_x[0] + bx
    on_x[C - 1] = on_x[C - 1] + hx
    on_y[0] = on_y[0] + by
    on_y[C - 1] = on_y[C - 1] + hy
    packed = pack_columns(turn, by, hy)
    rows = row_of((C, C))
    on_z = {}
    for z in (0, 1, CZ - 2, CZ - 1) if inner else (0, CZ - 1):
        p = column_plane(packed, z)
        p = p + jnp.where(rows == 0, bx[z : z + 1, :], jnp.where(rows == C - 1, hx[z : z + 1, :], 0.0))
        on_z[z] = p + bz if z == 0 else p + hz if z == CZ - 1 else p
    return on_x, on_y, on_z


def layer_weights(weight, wx, wy):
    return (
        {e: wx[i] for i, e in enumerate(EDGES)},
        {e: wy[i] for i, e in enumerate(EDGES)},
        {z: weight[z] for z in (0, 1, CZ - 2, CZ - 1)},
    )


def face_response(layers, weights):
    out = []
    for layer, w, last in zip(layers, weights, (C - 1, C - 1, CZ - 1)):
        for face, inside in ((0, 1), (last, last - 1)):
            once = w[face] * layer[face]
            near = in_plane(once) + w[inside] * layer[inside]
            out.append(KEPT * once + w[face] * (layer[face] + near))
    return out


def fold(t):
    return jnp.sum(t.reshape(t.shape[0] // 8, 8, C), axis=0)


def layer_energy(a, b, weights):
    rows = row_of((CZ, C))
    lanes = lane_of((CZ, C))
    inner = (rows > 0) & (rows < CZ - 1)
    both = inner & (lanes > 0) & (lanes < C - 1)
    acc = jnp.zeros((8, C), F32)
    for layers_a, layers_b, w, last, mask in zip(a, b, weights, (C - 1, C - 1, CZ - 1), (inner, both, None)):
        for e in (0, last):
            t = layers_a[e] * layers_b[e] * w[e]
            acc = acc + fold(t if mask is None else jnp.where(mask, t, 0.0))
    return jnp.sum(acc) / DAMPING_WEIGHT


def places():
    x, y, z = (lax.axis_index(a) for a in AXES)
    more = [i < lax.axis_size(a) - 1 for a, i in zip(AXES, (x, y, z))]
    less = [i > 0 for i in (x, y, z)]
    return (x % 2 == 0, y % 2 == 0, z == 0), more, less


def pick(flag, a, b):
    return lax.select(jnp.broadcast_to(flag, a.shape), a, b)


def pack_sends(sends, faces, index):
    (xeven, yeven, zlow), _, _ = places()
    xa, xb, ya, yb, zz = sends
    for even, a, b, lo, hi in ((xeven, xa, xb, faces[0], faces[1]), (yeven, ya, yb, faces[2], faces[3])):
        s = slice(index * CZ, (index + 1) * CZ)
        a[s, :] = pick(even, hi, lo)
        b[s, :] = pick(even, lo, hi)
    zz[index * C : (index + 1) * C, :] = pick(zlow, faces[5], faces[4])


def own_faces(src, own, turn):
    row_layer(src, 1, 0, own[0])
    row_layer(src, 1, C - 1, own[1])
    column_layers(src, 1, turn)
    own[2][...] = turn[layer_rows(2), :]
    own[3][...] = turn[layer_rows(1), :]
    own[4][...] = src[1, INNER, :]
    own[5][...] = src[CZ, INNER, :]


def first_kernel(heat_in, cond_in, proj_in, segs_in, weight, state, parts, heat, *refs):
    own = refs[:6]
    sends = refs[6:11]
    cond, proj, segs, start, turn, sems, small = refs[11:]
    tables = (pltpu.make_async_copy(proj_in, proj, small.at[0]), pltpu.make_async_copy(segs_in, segs, small.at[1]))
    for c in tables:
        c.start()
    part = CZ // PARTS
    copies = []
    for i in range(PARTS):
        s = pl.ds(i * part, part)
        pair = (
            pltpu.make_async_copy(cond_in.at[s], cond.at[s], sems.at[0, i]),
            pltpu.make_async_copy(heat_in.at[s], heat.at[s], sems.at[1, i]),
        )
        for c in pair:
            c.start()
        copies.append(pair)
    zero_ends(start)
    zero_ends(state)
    for c in tables:
        c.wait()
    for d in range(3):
        onehot = jnp.where(row_of((C, C)) == segs[d], 1.0, 0.0).astype(BF16)
        base = sum(lax.dot_general(onehot, p, (((1,), (1,)), ((), ())), preferred_element_type=F32) for p in reversed(parts_of(proj[d])))
        store_parts(parts, d, base)
        for a in (sends[:2], sends[2:4])[d] if d < 2 else ():
            a[CZ : CZ + C, :] = base
        if d == 2:
            sends[4][C : 2 * C, :] = base

    def plane(z, carry):
        w = DAMPING_WEIGHT / (6.0 + cond[z])
        weight[z] = w
        start[z + 1, INNER, :] = w * heat[z]
        return carry

    for i, pair in enumerate(copies):
        for c in pair:
            c.wait()
        lax.fori_loop(i * part, (i + 1) * part, plane, 0, unroll=UNROLL)
    sweep(start, state, weight, heat)
    own_faces(state, own, turn)
    pack_sends(sends, [f[...] for f in own], 0)


def free_kernel(first, state, weight, supply, *refs):
    out = refs[0]
    own = refs[1:7]
    mid, turn = refs[-2:]
    zero_ends(mid)
    zero_ends(out)
    sweep(state, mid, weight, supply)
    sweep(mid, out, weight, supply)
    own_faces(out, own, turn)
    if first:
        wx, wy = refs[7:9]
        for i, e in enumerate(EDGES):
            row_layer(weight, 0, e, wx.at[i])
        column_layers(weight, 0, turn)
        for i, e in enumerate((2, 3, 0, 1)):
            wy[i] = turn[layer_rows(e), :]


def jumps(own, got, bases, prev_bases, back_bases, n, lifted):
    (xeven, yeven, zlow), more, less = places()
    xa, xb, ya, yb, zz = got
    for d, (even, a, b, rows) in enumerate(((xeven, xa, xb, n * CZ), (yeven, ya, yb, n * CZ), (zlow, zz, zz, n * C))):
        a = a[0:rows, :]
        b = b[0:rows, :]
        up = own[2 * d + 1][...] - dot(pick(even, a, b), bases, d)
        up = jnp.where(more[d], up, 0.0)
        down = pick(even, b, a) - dot(own[2 * d][...], prev_bases, d)
        back = jnp.where(less[d], -dot(down, back_bases, d), 0.0)
        size = rows // n
        for i in range(n):
            lifted[i][2 * d][...] = back[i * size : (i + 1) * size, :]
            lifted[i][2 * d + 1][...] = up[i * size : (i + 1) * size, :]


def square_sum(a, b):
    return jnp.sum(sum(fold(a[i][...] * b[i][...]) for i in (1, 3, 5)))


def row_of_sums(values):
    lanes = lane_of((1, C))
    row = jnp.zeros((1, C), F32)
    for i, v in enumerate(values):
        row = jnp.where(lanes == i, v, row)
    return row


def second_kernel(first, *refs):
    it = iter(refs)
    take = lambda n: [next(it) for _ in range(n)]
    own = take(6)
    got = take(5)
    (bases,) = take(1)
    prev, back = take(2) if not first else (None, None)
    weight, wx, wy = take(3)
    own_u = take(6)
    lifted = take(6)
    own_uv = take(6)
    sends = take(5)
    if first:
        prev, back = take(2)
    (turn,) = take(1)
    (xeven, yeven, _), _, _ = places()
    if first:
        xa, xb, ya, yb, zz = got
        for d, base in enumerate((pick(xeven, xb[CZ:, :], xa[CZ:, :]), pick(yeven, yb[CZ:, :], ya[CZ:, :]), zz[C:, :])):
            store_parts(prev, d, base)
            store_parts(back, d, base.T)
    jumps(own, got, bases, prev, back, 1, [lifted])
    response = face_response(lift_layers(lifted, turn, True), layer_weights(weight, wx, wy))
    free = [f[...] for f in own_u]
    for o, u, v in zip(own_uv, free, response):
        n = u.shape[0]
        o[0:n, :] = u
        o[n:, :] = v
    pack_sends(sends, free, 0)
    pack_sends(sends, response, 1)


def response_kernel(*refs):
    lifted = refs[:6]
    weight, resp, sums, lift, mid, turn, cols = refs[6:]
    cols[...] = pack_columns(turn, lifted[2][...], lifted[3][...])

    def plane(z, carry):
        lift[z] = column_plane(cols[...], z)
        return carry

    lax.fori_loop(0, CZ, plane, 0, unroll=WIDE)
    add_rows(lift, lifted, 1.0)
    zero_ends(mid)
    zero_ends(resp)

    def scale(z, acc):
        once = weight[z] * lift[z]
        mid[z + 1, INNER, :] = once
        return acc + fold(once * lift[z])

    acc = lax.fori_loop(0, CZ, scale, jnp.zeros((8, C), F32), unroll=UNROLL)
    sweep(mid, resp, weight, lift)
    sums[...] = row_of_sums([square_sum(lifted, lifted), jnp.sum(acc) / DAMPING_WEIGHT])


def merge_sides(low, high):
    return [f for pair in zip(low, high) for f in pair]


def third_kernel(first, *refs):
    it = iter(refs)
    take = lambda n: [next(it) for _ in range(n)]
    own_uv = take(6)
    got = take(5)
    bases, prev, back, weight, wx, wy, before = take(7)
    high_u, high_v = take(3), take(3)
    (rows,) = take(1)
    low_u, low_v = take(3), take(3)
    (turn,) = take(1)
    lift_u = merge_sides(low_u, high_u)
    lift_v = merge_sides(low_v, high_v)
    jumps(own_uv, got, bases, prev, back, 2, [lift_u, lift_v])
    weights = layer_weights(weight, wx, wy)
    u = lift_layers(lift_u, turn.at[0], False)
    v = lift_layers(lift_v, turn.at[1], False)
    sums = [square_sum(lift_u, lift_u), square_sum(lift_u, lift_v), square_sum(lift_v, lift_v)]
    sums += [layer_energy(u, u, weights), layer_energy(u, v, weights), layer_energy(v, v, weights)]
    lanes = lane_of((1, C))
    row = row_of_sums([0.0, 0.0] + sums)
    row = jnp.where(lanes < 2, before[...], row)
    rows[...] = jnp.broadcast_to(row, (C, C))


def steps(totals):
    row = jnp.sum(totals[...], axis=0, keepdims=True)
    lanes = lane_of((1, C))
    gg, gh, guu, guv, gvv, huu, huv, hvv = [jnp.sum(jnp.where(lanes == i, row, 0.0), axis=1, keepdims=True) for i in range(8)]
    one = gg / (gh + EPSILON)
    two = (guu - 2.0 * one * guv + one * one * gvv) / (huu - 2.0 * one * huv + one * one * hvv + EPSILON)
    return one, two


def fourth_kernel(*refs):
    it = iter(refs)
    take = lambda n: [next(it) for _ in range(n)]
    totals, heat, weight, free, resp = take(5)
    lift_1 = take(6)
    lift_u = take(6)
    lift_v = take(6)
    supply, state = take(2)
    high = take(3)
    own = take(6)
    sends = take(5)
    low = take(3)
    mid, turn, cols = take(3)
    held = merge_sides(low, high)
    one, two = steps(totals)
    for i in range(6):
        held[i][...] = one * lift_1[i][...] + two * (lift_u[i][...] - one * lift_v[i][...])
    cols[...] = pack_columns(turn, held[2][...], held[3][...])
    zero_ends(mid)
    zero_ends(state)

    def plane(z, carry):
        supply[z] = heat[z] - column_plane(cols[...], z)
        state[z + 1, INNER, :] = free[z + 1, INNER, :] - one * resp[z + 1, INNER, :]
        return carry

    lax.fori_loop(0, CZ, plane, 0, unroll=2 * UNROLL)
    add_rows(supply, held, -1.0)
    sweep(state, mid, weight, supply)
    sweep(mid, state, weight, supply)
    own_faces(state, own, turn)
    pack_sends(sends, [f[...] for f in own], 0)


def last_kernel(*refs):
    it = iter(refs)
    take = lambda n: [next(it) for _ in range(n)]
    totals, free, resp = take(3)
    held = take(3)
    lift_3 = take(3)
    lift_u = take(3)
    lift_v = take(3)
    (out,) = take(1)
    outs = take(3)
    state, sems = take(2)
    one, two = steps(totals)

    def plane(z, carry):
        state[z] = free[z + 1, INNER, :] - one * resp[z + 1, INNER, :]
        return carry

    part = CZ // PARTS
    copies = []
    for i in range(PARTS):
        lax.fori_loop(i * part, (i + 1) * part, plane, 0, unroll=UNROLL)
        s = pl.ds(i * part, part)
        copies.append(pltpu.make_async_copy(state.at[s], out.at[s], sems.at[i]))
        copies[-1].start()
    for i in range(3):
        outs[i][...] = held[i][...] + one * lift_3[i][...] + two * (lift_u[i][...] - one * lift_v[i][...])
    for c in copies:
        c.wait()


FIELD = jax.ShapeDtypeStruct((CZ, C, C), F32)
PADDED = jax.ShapeDtypeStruct((CZ + 2, C + 2 * PAD, C), F32)
FACE = jax.ShapeDtypeStruct((CZ, C), F32)
SQUARE = jax.ShapeDtypeStruct((C, C), F32)
FACES = [FACE] * 4 + [SQUARE] * 2
LAYERS = jax.ShapeDtypeStruct((4, CZ, C), F32)
ROW = jax.ShapeDtypeStruct((1, C), F32)
SIDE = [FACE, FACE, SQUARE]
S_SIDE = [pltpu.VMEM(f.shape, F32) for f in SIDE]
S_FIELD = pltpu.VMEM((CZ, C, C), F32)
S_PADDED = pltpu.VMEM((CZ + 2, C + 2 * PAD, C), F32)
PIECES = jax.ShapeDtypeStruct((9, C, C), BF16)
S_SQUARE = pltpu.VMEM((C, C), F32)


def sends_of(n, extra):
    small = jax.ShapeDtypeStruct((n * CZ + extra, C), F32)
    return [small] * 4 + [jax.ShapeDtypeStruct((n * C + extra, C), F32)]


def call(kernel, name, outs, scratch, args, us, in_specs=None, out_specs=None):
    return list(
        pl.pallas_call(
            kernel,
            out_shape=tuple(outs),
            in_specs=in_specs or [VM] * len(args),
            out_specs=tuple(out_specs or [VM] * len(outs)),
            scratch_shapes=scratch,
            name=name,
            compiler_params=pltpu.CompilerParams(vmem_limit_bytes=20 * 1024 * 1024),
            cost_estimate=pl.CostEstimate(flops=us * 10**7, transcendentals=0, bytes_accessed=2**20),
        )(*args)
    )


def swap_pairs(axis, start):
    n = lax.axis_size(axis)
    pairs = []
    for i in range(start, n, 2):
        j = (i + 1) % n
        pairs += [(i, j), (j, i)]
    return pairs


def exchange(sends):
    xa, xb, ya, yb, zz = sends
    zz = lax.ppermute(zz, "gz", swap_pairs("gz", 0))
    yb = lax.ppermute(yb, "gy", swap_pairs("gy", 1))
    xb = lax.ppermute(xb, "gx", swap_pairs("gx", 1))
    xa = lax.ppermute(xa, "gx", swap_pairs("gx", 0))
    ya = lax.ppermute(ya, "gy", swap_pairs("gy", 0))
    return [xa, xb, ya, yb, zz]


def gather_rows(rows):
    rows = lax.all_to_all(rows.reshape(C, 1, C), AXES, 0, 0)
    return rows.reshape(C, C)


def body(heat, cond, projection, segment_map):
    proj = projection[0, 0, 0]
    segs = segment_map.reshape(3, 1, C)
    dma = pltpu.SemaphoreType.DMA
    scratch = [S_FIELD, pltpu.VMEM(proj.shape, F32), pltpu.VMEM(segs.shape, jnp.int32), S_PADDED, S_SQUARE, dma((2, PARTS)), dma((2,))]
    outs = [FIELD, PADDED, PIECES, FIELD] + FACES + sends_of(1, C)
    out = call(first_kernel, "first", outs, scratch, [pltpu.with_memory_space_constraint(a, pltpu.MemorySpace.HBM) for a in (heat, cond, proj, segs)], 4, [AWAY] * 4)
    weight, state, bases, heat = out[:4]
    own, sends = out[4:10], out[10:]
    supply = heat
    prev = []
    held = None
    for pair in range(2):
        first = pair == 0
        got = exchange(sends)
        outs = [PADDED] + FACES + ([LAYERS, LAYERS] if first else [])
        out = call(functools.partial(free_kernel, first), "free", outs, [S_PADDED, S_SQUARE], (state, weight, supply), 3)
        free, own_u = out[0], out[1:7]
        if first:
            wx, wy = out[7:]
        args = own + got + [bases] + prev + [weight, wx, wy] + own_u
        stacked = [jax.ShapeDtypeStruct((2 * f.shape[0], C), F32) for f in FACES]
        outs = FACES + stacked + sends_of(2, 0) + ([PIECES, PIECES] if first else [])
        out = call(functools.partial(second_kernel, first), "second", outs, [S_SQUARE], args, 2)
        lift_1, own_uv, sends = out[:6], out[6:12], out[12:17]
        if first:
            prev = out[17:]
        got = exchange(sends)
        resp, sums = call(response_kernel, "response", [PADDED, ROW], [S_FIELD, S_PADDED, S_SQUARE, S_SQUARE], lift_1 + [weight], 3)
        args = own_uv + got + [bases] + prev + [weight, wx, wy, sums]
        outs = SIDE + SIDE + [SQUARE] + (SIDE + SIDE if first else [])
        scratch = ([] if first else S_SIDE + S_SIDE) + [pltpu.VMEM((2, C, C), F32)]
        out = call(functools.partial(third_kernel, first), "third", outs, scratch, args, 2)
        high_u, high_v, rows = out[:3], out[3:6], out[6]
        totals = gather_rows(rows)
        if first:
            args = [totals, heat, weight, free, resp] + lift_1 + merge_sides(out[7:10], high_u) + merge_sides(out[10:13], high_v)
            outs = [FIELD, PADDED] + SIDE + FACES + sends_of(1, 0)
            out = call(fourth_kernel, "fourth", outs, S_SIDE + [S_PADDED, S_SQUARE, S_SQUARE], args, 5)
            supply, state, held, own, sends = out[0], out[1], out[2:5], out[5:11], out[11:]
    args = [totals, free, resp] + held + [lift_1[i] for i in (1, 3, 5)] + high_u + high_v
    state, mx, my, mz = call(last_kernel, "last", [FIELD, FACE, FACE, SQUARE], [S_FIELD, dma((PARTS,))], args, 2, None, [AWAY, VM, VM, VM])
    return state, mx[None, None, None], my[None, None, None], mz[None, None, None]


def solution(mesh):
    field = P("gz", "gx", "gy")
    in_specs = (field, field, P("gz", "gx", "gy", None, None, None), P("gz", "gx", "gy", None, None))
    face = P("gz", "gx", "gy", None, None)
    return jax.shard_map(body, mesh=mesh, in_specs=in_specs, out_specs=(field, face, face, face), check_vma=False)
```

```python
import functools

import jax
import jax.numpy as jnp
from jax import lax
from jax.experimental import pallas as pl
from jax.experimental.pallas import tpu as pltpu
from jax.sharding import PartitionSpec as P

HIGH = lax.Precision.HIGHEST
DAMPING_WEIGHT = 0.8
EPSILON = 1e-06
AXES = ("gx", "gy", "gz")
CZ = 32
C = 128
F32 = jnp.float32
UNROLL = 4
WIDE = 16
BLOCK = 16
DEPTH = 8
PARTS = CZ // DEPTH
KEPT = 1.0 - DAMPING_WEIGHT

VM = pl.BlockSpec(memory_space=pltpu.MemorySpace.VMEM)
AWAY = pl.BlockSpec(memory_space=pltpu.MemorySpace.HBM)
BF16 = jnp.bfloat16
PAD = 8


def dot_t(a, b):
    return lax.dot_general(a, b, (((1,), (1,)), ((), ())), precision=HIGH, preferred_element_type=F32)


def parts_of(a):
    first = a.astype(BF16)
    rest = a - first.astype(F32)
    second = rest.astype(BF16)
    third = (rest - second.astype(F32)).astype(BF16)
    return first, second, third


def dot(a, parts, d):
    n = a.shape[0]
    mul = functools.partial(jnp.dot, preferred_element_type=F32)
    a1, a2, a3 = parts_of(a)
    r = mul(jnp.concatenate([a1, a2, a3], axis=0), parts[3 * d])
    s = mul(jnp.concatenate([a1, a2], axis=0), parts[3 * d + 1])
    t = mul(a1, parts[3 * d + 2])
    return r[:n] + (r[n : 2 * n] + s[:n] + (r[2 * n :] + s[n:] + t))


def store_parts(ref, d, a):
    for i, p in enumerate(parts_of(a)):
        ref[3 * d + i] = p


def lane_of(shape):
    return lax.broadcasted_iota(jnp.int32, shape, len(shape) - 1)


def row_of(shape):
    return lax.broadcasted_iota(jnp.int32, shape, len(shape) - 2)


INNER = slice(PAD, PAD + C)


def zero_ends(ref):
    ref[0] = jnp.zeros((C + 2 * PAD, C), F32)
    ref[CZ + 1] = jnp.zeros((C + 2 * PAD, C), F32)
    for z in range(1, CZ + 1):
        ref[z, 0:PAD, :] = jnp.zeros((PAD, C), F32)
        ref[z, PAD + C :, :] = jnp.zeros((PAD, C), F32)


def in_plane(centre):
    shape = centre.shape
    rows = row_of(shape)
    lanes = lane_of(shape)
    near = jnp.where(rows == 0, 0.0, pltpu.roll(centre, 1, 0))
    near = near + jnp.where(rows == shape[0] - 1, 0.0, pltpu.roll(centre, shape[0] - 1, 0))
    near = near + jnp.where(lanes == 0, 0.0, pltpu.roll(centre, 1, 1))
    return near + jnp.where(lanes == C - 1, 0.0, pltpu.roll(centre, C - 1, 1))


def sweep_planes(src, dst, weight, supply, i):
    lanes = lane_of((BLOCK, C))
    low = lanes == 0
    high = lanes == C - 1
    z = i * DEPTH
    for x in range(0, C, BLOCK):
        r = PAD + x
        column = [src[z + j, r : r + BLOCK, :] for j in range(DEPTH + 2)]
        for j in range(DEPTH):
            centre = column[j + 1]
            near = column[j] + column[j + 2]
            near = near + src[z + j + 1, r - 1 : r - 1 + BLOCK, :] + src[z + j + 1, r + 1 : r + 1 + BLOCK, :]
            near = near + jnp.where(low, 0.0, pltpu.roll(centre, 1, 1)) + jnp.where(high, 0.0, pltpu.roll(centre, C - 1, 1))
            dst[z + j + 1, r : r + BLOCK, :] = KEPT * centre + weight[z + j, x : x + BLOCK, :] * (supply[z + j, x : x + BLOCK, :] + near)


def sweep(src, dst, weight, supply):
    def planes(i, carry):
        sweep_planes(src, dst, weight, supply, i)
        return carry

    lax.fori_loop(0, CZ // DEPTH, planes, 0)


def row_layer(src, base, at, out):
    for z in range(CZ):
        out[z : z + 1, :] = src[z + base, PAD * base + at : PAD * base + at + 1, :]


def column_layers(src, base, turn):
    group = lane_of((C, C)) // 4

    def plane(z, packed):
        return jnp.where(group == z, pltpu.roll(src[z + base, PAD * base : PAD * base + C, :], 4 * z + 2, 1), packed)

    packed = lax.fori_loop(0, CZ, plane, jnp.zeros((C, C), F32), unroll=WIDE)
    turn[...] = packed.T


def layer_rows(i):
    return pl.ds(i, CZ, stride=4)


def pack_columns(turn, low, high):
    turn[...] = jnp.zeros((C, C), F32)
    turn[layer_rows(1), :] = high
    turn[layer_rows(2), :] = low
    return turn[...].T


def column_plane(packed, z):
    lanes = lane_of((C, C))
    edge = (lanes == 0) | (lanes == C - 1)
    return jnp.where(edge, pltpu.roll(packed, C - 2 - 4 * z, 1), 0.0)


def add_rows(dst, faces, sign):
    for z in range(CZ):
        dst[z, 0:1, :] = dst[z, 0:1, :] + sign * faces[0][z : z + 1, :]
        dst[z, C - 1 : C, :] = dst[z, C - 1 : C, :] + sign * faces[1][z : z + 1, :]
    dst[0] = dst[0] + sign * faces[4][...]
    dst[CZ - 1] = dst[CZ - 1] + sign * faces[5][...]


EDGES = (0, 1, C - 2, C - 1)


def rim(low, high, at):
    lanes = lane_of(low.shape)
    a = low if at == 0 else pltpu.roll(low, C - at, 1)
    b = high if at == C - 1 else pltpu.roll(high, C - 1 - at, 1)
    return jnp.where(lanes == 0, a, jnp.where(lanes == C - 1, b, 0.0))


def ends(low, high):
    rows = row_of((CZ, C))
    return jnp.where(rows == 0, low, jnp.where(rows == CZ - 1, high, 0.0))


def lift_layers(faces, turn, inner):
    bx, hx, by, hy, bz, hz = [f[...] for f in faces]
    lanes = lane_of((C, C))
    columns = jnp.where(lanes < 4, pltpu.roll(bz, 2, 1), pltpu.roll(hz, 6, 1)).T
    at = lambda i: columns[i : i + 1, :]
    column = {C - 2: (at(0), at(4)), C - 1: (at(1), at(5)), 0: (at(2), at(6)), 1: (at(3), at(7))}
    edges = EDGES if inner else (0, C - 1)
    on_x = {}
    on_y = {}
    for e in edges:
        on_x[e] = rim(by, hy, e) + ends(bz[e : e + 1, :], hz[e : e + 1, :])
        on_y[e] = rim(bx, hx, e) + ends(*column[e])
    on_x[0] = on_x[0] + bx
    on_x[C - 1] = on_x[C - 1] + hx
    on_y[0] = on_y[0] + by
    on_y[C - 1] = on_y[C - 1] + hy
    packed = pack_columns(turn, by, hy)
    rows = row_of((C, C))
    on_z = {}
    for z in (0, 1, CZ - 2, CZ - 1) if inner else (0, CZ - 1):
        p = column_plane(packed, z)
        p = p + jnp.where(rows == 0, bx[z : z + 1, :], jnp.where(rows == C - 1, hx[z : z + 1, :], 0.0))
        on_z[z] = p + bz if z == 0 else p + hz if z == CZ - 1 else p
    return on_x, on_y, on_z


def layer_weights(weight, wx, wy):
    return (
        {e: wx[i] for i, e in enumerate(EDGES)},
        {e: wy[i] for i, e in enumerate(EDGES)},
        {z: weight[z] for z in (0, 1, CZ - 2, CZ - 1)},
    )


def face_response(layers, weights):
    out = []
    for layer, w, last in zip(layers, weights, (C - 1, C - 1, CZ - 1)):
        for face, inside in ((0, 1), (last, last - 1)):
            once = w[face] * layer[face]
            near = in_plane(once) + w[inside] * layer[inside]
            out.append(KEPT * once + w[face] * (layer[face] + near))
    return out


def fold(t):
    return jnp.sum(t.reshape(t.shape[0] // 8, 8, C), axis=0)


def layer_energy(a, b, weights):
    rows = row_of((CZ, C))
    lanes = lane_of((CZ, C))
    inner = (rows > 0) & (rows < CZ - 1)
    both = inner & (lanes > 0) & (lanes < C - 1)
    acc = jnp.zeros((8, C), F32)
    for layers_a, layers_b, w, last, mask in zip(a, b, weights, (C - 1, C - 1, CZ - 1), (inner, both, None)):
        for e in (0, last):
            t = layers_a[e] * layers_b[e] * w[e]
            acc = acc + fold(t if mask is None else jnp.where(mask, t, 0.0))
    return jnp.sum(acc) / DAMPING_WEIGHT


def places():
    x, y, z = (lax.axis_index(a) for a in AXES)
    more = [i < lax.axis_size(a) - 1 for a, i in zip(AXES, (x, y, z))]
    less = [i > 0 for i in (x, y, z)]
    return (x % 2 == 0, y % 2 == 0, z == 0), more, less


def pick(flag, a, b):
    return lax.select(jnp.broadcast_to(flag, a.shape), a, b)


def pack_sends(sends, faces, index):
    (xeven, yeven, zlow), _, _ = places()
    xa, xb, ya, yb, zz = sends
    for even, a, b, lo, hi in ((xeven, xa, xb, faces[0], faces[1]), (yeven, ya, yb, faces[2], faces[3])):
        s = slice(index * CZ, (index + 1) * CZ)
        a[s, :] = pick(even, hi, lo)
        b[s, :] = pick(even, lo, hi)
    zz[index * C : (index + 1) * C, :] = pick(zlow, faces[5], faces[4])


def own_faces(src, own, turn):
    row_layer(src, 1, 0, own[0])
    row_layer(src, 1, C - 1, own[1])
    column_layers(src, 1, turn)
    own[2][...] = turn[layer_rows(2), :]
    own[3][...] = turn[layer_rows(1), :]
    own[4][...] = src[1, INNER, :]
    own[5][...] = src[CZ, INNER, :]


def first_kernel(heat_in, cond_in, proj_in, segs_in, weight, state, parts, heat, wx, wy, *refs):
    own = refs[:6]
    sends = refs[6:11]
    cond, proj, segs, start, turn, pack, sems, small = refs[11:]
    tables = (pltpu.make_async_copy(proj_in, proj, small.at[0]), pltpu.make_async_copy(segs_in, segs, small.at[1]))

    def copies(i):
        s = pl.ds(i * DEPTH, DEPTH)
        return (
            pltpu.make_async_copy(cond_in.at[s], cond.at[s], sems.at[0, i]),
            pltpu.make_async_copy(heat_in.at[s], heat.at[s], sems.at[1, i]),
        )

    for i in range(PARTS):
        for c in copies(i) + (tables if i == 0 else ()):
            c.start()
    zero_ends(start)
    zero_ends(state)
    pack[...] = jnp.zeros((C, C), F32)
    for c in tables:
        c.wait()
    for d in range(3):
        onehot = jnp.where(row_of((C, C)) == segs[d], 1.0, 0.0).astype(BF16)
        base = sum(lax.dot_general(onehot, p, (((1,), (1,)), ((), ())), preferred_element_type=F32) for p in reversed(parts_of(proj[d])))
        store_parts(parts, d, base)
        for a in (sends[:2], sends[2:4])[d] if d < 2 else ():
            a[CZ : CZ + C, :] = base
        if d == 2:
            sends[4][C : 2 * C, :] = base
    group = lane_of((C, C)) // 4

    def part(i, carry):
        for c in copies(i):
            c.wait()
        packed = pack[...]
        for j in range(DEPTH):
            z = i * DEPTH + j
            w = DAMPING_WEIGHT / (6.0 + cond[z])
            weight[z] = w
            start[z + 1, INNER, :] = w * heat[z]
            packed = jnp.where(group == z, pltpu.roll(w, 4 * z + 2, 1), packed)
        pack[...] = packed

        @pl.when(i > 0)
        def _():
            sweep_planes(start, state, weight, heat, i - 1)

        return carry

    lax.fori_loop(0, PARTS, part, 0)
    sweep_planes(start, state, weight, heat, PARTS - 1)
    own_faces(state, own, turn)
    pack_sends(sends, [f[...] for f in own], 0)
    for i, e in enumerate(EDGES):
        row_layer(weight, 0, e, wx.at[i])
    turn[...] = pack[...].T
    for i, e in enumerate((2, 3, 0, 1)):
        wy[i] = turn[layer_rows(e), :]


def free_kernel(state, weight, supply, out, *refs):
    own = refs[:6]
    mid, turn = refs[6:]
    zero_ends(mid)
    zero_ends(out)
    sweep(state, mid, weight, supply)
    sweep(mid, out, weight, supply)
    own_faces(out, own, turn)


def jumps(own, got, bases, prev_bases, back_bases, n, lifted):
    (xeven, yeven, zlow), more, less = places()
    xa, xb, ya, yb, zz = got
    for d, (even, a, b, rows) in enumerate(((xeven, xa, xb, n * CZ), (yeven, ya, yb, n * CZ), (zlow, zz, zz, n * C))):
        a = a[0:rows, :]
        b = b[0:rows, :]
        up = own[2 * d + 1][...] - dot(pick(even, a, b), bases, d)
        up = jnp.where(more[d], up, 0.0)
        down = pick(even, b, a) - dot(own[2 * d][...], prev_bases, d)
        back = jnp.where(less[d], -dot(down, back_bases, d), 0.0)
        size = rows // n
        for i in range(n):
            lifted[i][2 * d][...] = back[i * size : (i + 1) * size, :]
            lifted[i][2 * d + 1][...] = up[i * size : (i + 1) * size, :]


def square_sum(a, b):
    return jnp.sum(sum(fold(a[i][...] * b[i][...]) for i in (1, 3, 5)))


def row_of_sums(values):
    lanes = lane_of((1, C))
    row = jnp.zeros((1, C), F32)
    for i, v in enumerate(values):
        row = jnp.where(lanes == i, v, row)
    return row


def second_kernel(first, *refs):
    it = iter(refs)
    take = lambda n: [next(it) for _ in range(n)]
    own = take(6)
    got = take(5)
    (bases,) = take(1)
    prev, back = take(2) if not first else (None, None)
    weight, wx, wy = take(3)
    own_u = take(6)
    lifted = take(6)
    own_uv = take(6)
    sends = take(5)
    if first:
        prev, back = take(2)
    (turn,) = take(1)
    (xeven, yeven, _), _, _ = places()
    if first:
        xa, xb, ya, yb, zz = got
        for d, base in enumerate((pick(xeven, xb[CZ:, :], xa[CZ:, :]), pick(yeven, yb[CZ:, :], ya[CZ:, :]), zz[C:, :])):
            store_parts(prev, d, base)
            store_parts(back, d, base.T)
    jumps(own, got, bases, prev, back, 1, [lifted])
    response = face_response(lift_layers(lifted, turn, True), layer_weights(weight, wx, wy))
    free = [f[...] for f in own_u]
    for o, u, v in zip(own_uv, free, response):
        n = u.shape[0]
        o[0:n, :] = u
        o[n:, :] = v
    pack_sends(sends, free, 0)
    pack_sends(sends, response, 1)


def response_kernel(*refs):
    lifted = refs[:6]
    weight, resp, sums, lift, mid, turn, cols = refs[6:]
    cols[...] = pack_columns(turn, lifted[2][...], lifted[3][...])

    def plane(z, carry):
        lift[z] = column_plane(cols[...], z)
        return carry

    lax.fori_loop(0, CZ, plane, 0, unroll=WIDE)
    add_rows(lift, lifted, 1.0)
    zero_ends(mid)
    zero_ends(resp)

    def scale(z, acc):
        once = weight[z] * lift[z]
        mid[z + 1, INNER, :] = once
        return acc + fold(once * lift[z])

    acc = lax.fori_loop(0, CZ, scale, jnp.zeros((8, C), F32), unroll=UNROLL)
    sweep(mid, resp, weight, lift)
    sums[...] = row_of_sums([square_sum(lifted, lifted), jnp.sum(acc) / DAMPING_WEIGHT])


def merge_sides(low, high):
    return [f for pair in zip(low, high) for f in pair]


def third_kernel(first, *refs):
    it = iter(refs)
    take = lambda n: [next(it) for _ in range(n)]
    own_uv = take(6)
    got = take(5)
    bases, prev, back, weight, wx, wy, before = take(7)
    high_u, high_v = take(3), take(3)
    (rows,) = take(1)
    low_u, low_v = take(3), take(3)
    (turn,) = take(1)
    lift_u = merge_sides(low_u, high_u)
    lift_v = merge_sides(low_v, high_v)
    jumps(own_uv, got, bases, prev, back, 2, [lift_u, lift_v])
    weights = layer_weights(weight, wx, wy)
    u = lift_layers(lift_u, turn.at[0], False)
    v = lift_layers(lift_v, turn.at[1], False)
    sums = [square_sum(lift_u, lift_u), square_sum(lift_u, lift_v), square_sum(lift_v, lift_v)]
    sums += [layer_energy(u, u, weights), layer_energy(u, v, weights), layer_energy(v, v, weights)]
    lanes = lane_of((1, C))
    row = row_of_sums([0.0, 0.0] + sums)
    row = jnp.where(lanes < 2, before[...], row)
    rows[...] = jnp.broadcast_to(row, (C, C))


def steps(totals):
    row = jnp.sum(totals[...], axis=0, keepdims=True)
    lanes = lane_of((1, C))
    gg, gh, guu, guv, gvv, huu, huv, hvv = [jnp.sum(jnp.where(lanes == i, row, 0.0), axis=1, keepdims=True) for i in range(8)]
    one = gg / (gh + EPSILON)
    two = (guu - 2.0 * one * guv + one * one * gvv) / (huu - 2.0 * one * huv + one * one * hvv + EPSILON)
    return one, two


def fourth_kernel(*refs):
    it = iter(refs)
    take = lambda n: [next(it) for _ in range(n)]
    totals, heat, weight, free, resp = take(5)
    lift_1 = take(6)
    lift_u = take(6)
    lift_v = take(6)
    supply, state = take(2)
    high = take(3)
    own = take(6)
    sends = take(5)
    low = take(3)
    mid, turn, cols = take(3)
    held = merge_sides(low, high)
    one, two = steps(totals)
    for i in range(6):
        held[i][...] = one * lift_1[i][...] + two * (lift_u[i][...] - one * lift_v[i][...])
    cols[...] = pack_columns(turn, held[2][...], held[3][...])
    zero_ends(mid)
    zero_ends(state)

    def plane(z, carry):
        supply[z] = heat[z] - column_plane(cols[...], z)
        state[z + 1, INNER, :] = free[z + 1, INNER, :] - one * resp[z + 1, INNER, :]
        return carry

    lax.fori_loop(0, CZ, plane, 0, unroll=2 * UNROLL)
    add_rows(supply, held, -1.0)
    sweep(state, mid, weight, supply)
    sweep(mid, state, weight, supply)
    own_faces(state, own, turn)
    pack_sends(sends, [f[...] for f in own], 0)


def last_kernel(*refs):
    it = iter(refs)
    take = lambda n: [next(it) for _ in range(n)]
    totals, free, resp = take(3)
    held = take(3)
    lift_3 = take(3)
    lift_u = take(3)
    lift_v = take(3)
    (out,) = take(1)
    outs = take(3)
    state, sems = take(2)
    one, two = steps(totals)

    def plane(z, carry):
        state[z] = free[z + 1, INNER, :] - one * resp[z + 1, INNER, :]
        return carry

    copies = []
    for i in range(PARTS):
        lax.fori_loop(i * DEPTH, (i + 1) * DEPTH, plane, 0, unroll=UNROLL)
        s = pl.ds(i * DEPTH, DEPTH)
        copies.append(pltpu.make_async_copy(state.at[s], out.at[s], sems.at[i]))
        copies[-1].start()
    for i in range(3):
        outs[i][...] = held[i][...] + one * lift_3[i][...] + two * (lift_u[i][...] - one * lift_v[i][...])
    for c in copies:
        c.wait()


FIELD = jax.ShapeDtypeStruct((CZ, C, C), F32)
PADDED = jax.ShapeDtypeStruct((CZ + 2, C + 2 * PAD, C), F32)
FACE = jax.ShapeDtypeStruct((CZ, C), F32)
SQUARE = jax.ShapeDtypeStruct((C, C), F32)
FACES = [FACE] * 4 + [SQUARE] * 2
LAYERS = jax.ShapeDtypeStruct((4, CZ, C), F32)
ROW = jax.ShapeDtypeStruct((1, C), F32)
SIDE = [FACE, FACE, SQUARE]
S_SIDE = [pltpu.VMEM(f.shape, F32) for f in SIDE]
S_FIELD = pltpu.VMEM((CZ, C, C), F32)
S_PADDED = pltpu.VMEM((CZ + 2, C + 2 * PAD, C), F32)
PIECES = jax.ShapeDtypeStruct((9, C, C), BF16)
S_SQUARE = pltpu.VMEM((C, C), F32)


def sends_of(n, extra):
    small = jax.ShapeDtypeStruct((n * CZ + extra, C), F32)
    return [small] * 4 + [jax.ShapeDtypeStruct((n * C + extra, C), F32)]


def call(kernel, name, outs, scratch, args, us, in_specs=None, out_specs=None):
    return list(
        pl.pallas_call(
            kernel,
            out_shape=tuple(outs),
            in_specs=in_specs or [VM] * len(args),
            out_specs=tuple(out_specs or [VM] * len(outs)),
            scratch_shapes=scratch,
            name=name,
            compiler_params=pltpu.CompilerParams(vmem_limit_bytes=20 * 1024 * 1024),
            cost_estimate=pl.CostEstimate(flops=us * 10**7, transcendentals=0, bytes_accessed=2**20),
        )(*args)
    )


def swap_pairs(axis, start):
    n = lax.axis_size(axis)
    pairs = [(i, i) for i in range(start)]
    for i in range(start, n - 1, 2):
        pairs += [(i, i + 1), (i + 1, i)]
    return pairs + [(i, i) for i in range(n - start, n)]


def exchange(sends):
    xa, xb, ya, yb, zz = sends
    zz = lax.ppermute(zz, "gz", swap_pairs("gz", 0))
    yb = lax.ppermute(yb, "gy", swap_pairs("gy", 1))
    xb = lax.ppermute(xb, "gx", swap_pairs("gx", 1))
    xa = lax.ppermute(xa, "gx", swap_pairs("gx", 0))
    ya = lax.ppermute(ya, "gy", swap_pairs("gy", 0))
    return [xa, xb, ya, yb, zz]


def gather_rows(rows):
    rows = lax.all_to_all(rows.reshape(C, 1, C), AXES, 0, 0)
    return rows.reshape(C, C)


def body(heat, cond, projection, segment_map):
    proj = projection[0, 0, 0]
    segs = segment_map.reshape(3, 1, C)
    dma = pltpu.SemaphoreType.DMA
    scratch = [S_FIELD, pltpu.VMEM(proj.shape, F32), pltpu.VMEM(segs.shape, jnp.int32), S_PADDED, S_SQUARE, S_SQUARE, dma((2, PARTS)), dma((2,))]
    outs = [FIELD, PADDED, PIECES, FIELD, LAYERS, LAYERS] + FACES + sends_of(1, C)
    out = call(first_kernel, "first", outs, scratch, [pltpu.with_memory_space_constraint(a, pltpu.MemorySpace.HBM) for a in (heat, cond, proj, segs)], 4, [AWAY] * 4)
    weight, state, bases, heat, wx, wy = out[:6]
    own, sends = out[6:12], out[12:]
    supply = heat
    prev = []
    held = None
    for pair in range(2):
        first = pair == 0
        got = exchange(sends)
        out = call(free_kernel, "free", [PADDED] + FACES, [S_PADDED, S_SQUARE], (state, weight, supply), 3)
        free, own_u = out[0], out[1:]
        args = own + got + [bases] + prev + [weight, wx, wy] + own_u
        stacked = [jax.ShapeDtypeStruct((2 * f.shape[0], C), F32) for f in FACES]
        outs = FACES + stacked + sends_of(2, 0) + ([PIECES, PIECES] if first else [])
        out = call(functools.partial(second_kernel, first), "second", outs, [S_SQUARE], args, 2)
        lift_1, own_uv, sends = out[:6], out[6:12], out[12:17]
        if first:
            prev = out[17:]
        got = exchange(sends)
        resp, sums = call(response_kernel, "response", [PADDED, ROW], [S_FIELD, S_PADDED, S_SQUARE, S_SQUARE], lift_1 + [weight], 3)
        args = own_uv + got + [bases] + prev + [weight, wx, wy, sums]
        outs = SIDE + SIDE + [SQUARE] + (SIDE + SIDE if first else [])
        scratch = ([] if first else S_SIDE + S_SIDE) + [pltpu.VMEM((2, C, C), F32)]
        out = call(functools.partial(third_kernel, first), "third", outs, scratch, args, 2)
        high_u, high_v, rows = out[:3], out[3:6], out[6]
        totals = gather_rows(rows)
        if first:
            args = [totals, heat, weight, free, resp] + lift_1 + merge_sides(out[7:10], high_u) + merge_sides(out[10:13], high_v)
            outs = [FIELD, PADDED] + SIDE + FACES + sends_of(1, 0)
            out = call(fourth_kernel, "fourth", outs, S_SIDE + [S_PADDED, S_SQUARE, S_SQUARE], args, 5)
            supply, state, held, own, sends = out[0], out[1], out[2:5], out[5:11], out[11:]
    args = [totals, free, resp] + held + [lift_1[i] for i in (1, 3, 5)] + high_u + high_v
    state, mx, my, mz = call(last_kernel, "last", [FIELD, FACE, FACE, SQUARE], [S_FIELD, dma((PARTS,))], args, 2, None, [AWAY, VM, VM, VM])
    return state, mx[None, None, None], my[None, None, None], mz[None, None, None]


def solution(mesh):
    field = P("gz", "gx", "gy")
    in_specs = (field, field, P("gz", "gx", "gy", None, None, None), P("gz", "gx", "gy", None, None))
    face = P("gz", "gx", "gy", None, None)
    return jax.shard_map(body, mesh=mesh, in_specs=in_specs, out_specs=(field, face, face, face), check_vma=False)
```

```python
import functools

import jax
import jax.numpy as jnp
from jax import lax
from jax.experimental import pallas as pl
from jax.experimental.pallas import tpu as pltpu
from jax.sharding import PartitionSpec as P

HIGH = lax.Precision.HIGHEST
DAMPING_WEIGHT = 0.8
EPSILON = 1e-06
AXES = ("gx", "gy", "gz")
CZ = 32
C = 128
F32 = jnp.float32
UNROLL = 4
WIDE = 16
DEPTH = 8
PARTS = CZ // DEPTH
KEPT = 1.0 - DAMPING_WEIGHT

VM = pl.BlockSpec(memory_space=pltpu.MemorySpace.VMEM)
AWAY = pl.BlockSpec(memory_space=pltpu.MemorySpace.HBM)
BF16 = jnp.bfloat16
PAD = 8


def dot_t(a, b):
    return lax.dot_general(a, b, (((1,), (1,)), ((), ())), precision=HIGH, preferred_element_type=F32)


def parts_of(a):
    first = a.astype(BF16)
    rest = a - first.astype(F32)
    second = rest.astype(BF16)
    third = (rest - second.astype(F32)).astype(BF16)
    return first, second, third


def dot(a, parts, d):
    n = a.shape[0]
    mul = functools.partial(jnp.dot, preferred_element_type=F32)
    a1, a2, a3 = parts_of(a)
    r = mul(jnp.concatenate([a1, a2, a3], axis=0), parts[3 * d])
    s = mul(jnp.concatenate([a1, a2], axis=0), parts[3 * d + 1])
    t = mul(a1, parts[3 * d + 2])
    return r[:n] + (r[n : 2 * n] + s[:n] + (r[2 * n :] + s[n:] + t))


def store_parts(ref, d, a):
    for i, p in enumerate(parts_of(a)):
        ref[3 * d + i] = p


def lane_of(shape):
    return lax.broadcasted_iota(jnp.int32, shape, len(shape) - 1)


def row_of(shape):
    return lax.broadcasted_iota(jnp.int32, shape, len(shape) - 2)


INNER = slice(PAD, PAD + C)


def zero_ends(ref):
    ref[0] = jnp.zeros((C + 2 * PAD, C), F32)
    ref[CZ + 1] = jnp.zeros((C + 2 * PAD, C), F32)
    for z in range(1, CZ + 1):
        ref[z, 0:PAD, :] = jnp.zeros((PAD, C), F32)
        ref[z, PAD + C :, :] = jnp.zeros((PAD, C), F32)


def in_plane(centre):
    shape = centre.shape
    rows = row_of(shape)
    lanes = lane_of(shape)
    near = jnp.where(rows == 0, 0.0, pltpu.roll(centre, 1, 0))
    near = near + jnp.where(rows == shape[0] - 1, 0.0, pltpu.roll(centre, shape[0] - 1, 0))
    near = near + jnp.where(lanes == 0, 0.0, pltpu.roll(centre, 1, 1))
    return near + jnp.where(lanes == C - 1, 0.0, pltpu.roll(centre, C - 1, 1))


def sweep_planes(src, dst, weight, supply, z, depth, block):
    lanes = lane_of((block, C))
    low = lanes == 0
    high = lanes == C - 1
    for x in range(0, C, block):
        r = PAD + x
        column = [src[z + j, r : r + block, :] for j in range(depth + 2)]
        for j in range(depth):
            centre = column[j + 1]
            near = column[j] + column[j + 2]
            near = near + src[z + j + 1, r - 1 : r - 1 + block, :] + src[z + j + 1, r + 1 : r + 1 + block, :]
            near = near + jnp.where(low, 0.0, pltpu.roll(centre, 1, 1)) + jnp.where(high, 0.0, pltpu.roll(centre, C - 1, 1))
            dst[z + j + 1, r : r + block, :] = KEPT * centre + weight[z + j, x : x + block, :] * (supply[z + j, x : x + block, :] + near)


def sweep(src, dst, weight, supply):
    def planes(i, carry):
        sweep_planes(src, dst, weight, supply, i * WIDE, WIDE, 8)
        return carry

    lax.fori_loop(0, CZ // WIDE, planes, 0)


def row_layer(src, base, at, out):
    for z in range(CZ):
        out[z : z + 1, :] = src[z + base, PAD * base + at : PAD * base + at + 1, :]


def column_layers(src, base, turn):
    group = lane_of((C, C)) // 4

    def plane(z, packed):
        return jnp.where(group == z, pltpu.roll(src[z + base, PAD * base : PAD * base + C, :], 4 * z + 2, 1), packed)

    packed = lax.fori_loop(0, CZ, plane, jnp.zeros((C, C), F32), unroll=CZ)
    turn[...] = packed.T


def layer_rows(i):
    return pl.ds(i, CZ, stride=4)


def pack_columns(turn, low, high):
    turn[...] = jnp.zeros((C, C), F32)
    turn[layer_rows(1), :] = high
    turn[layer_rows(2), :] = low
    return turn[...].T


def column_plane(packed, z):
    lanes = lane_of((C, C))
    edge = (lanes == 0) | (lanes == C - 1)
    return jnp.where(edge, pltpu.roll(packed, C - 2 - 4 * z, 1), 0.0)


def add_rows(dst, faces, sign):
    for z in range(CZ):
        dst[z, 0:1, :] = dst[z, 0:1, :] + sign * faces[0][z : z + 1, :]
        dst[z, C - 1 : C, :] = dst[z, C - 1 : C, :] + sign * faces[1][z : z + 1, :]
    dst[0] = dst[0] + sign * faces[4][...]
    dst[CZ - 1] = dst[CZ - 1] + sign * faces[5][...]


EDGES = (0, 1, C - 2, C - 1)


def rim(low, high, at):
    lanes = lane_of(low.shape)
    a = low if at == 0 else pltpu.roll(low, C - at, 1)
    b = high if at == C - 1 else pltpu.roll(high, C - 1 - at, 1)
    return jnp.where(lanes == 0, a, jnp.where(lanes == C - 1, b, 0.0))


def ends(low, high):
    rows = row_of((CZ, C))
    return jnp.where(rows == 0, low, jnp.where(rows == CZ - 1, high, 0.0))


def lift_layers(faces, turn, inner):
    bx, hx, by, hy, bz, hz = [f[...] for f in faces]
    lanes = lane_of((C, C))
    columns = jnp.where(lanes < 4, pltpu.roll(bz, 2, 1), pltpu.roll(hz, 6, 1)).T
    at = lambda i: columns[i : i + 1, :]
    column = {C - 2: (at(0), at(4)), C - 1: (at(1), at(5)), 0: (at(2), at(6)), 1: (at(3), at(7))}
    edges = EDGES if inner else (0, C - 1)
    on_x = {}
    on_y = {}
    for e in edges:
        on_x[e] = rim(by, hy, e) + ends(bz[e : e + 1, :], hz[e : e + 1, :])
        on_y[e] = rim(bx, hx, e) + ends(*column[e])
    on_x[0] = on_x[0] + bx
    on_x[C - 1] = on_x[C - 1] + hx
    on_y[0] = on_y[0] + by
    on_y[C - 1] = on_y[C - 1] + hy
    packed = pack_columns(turn, by, hy)
    rows = row_of((C, C))
    on_z = {}
    for z in (0, 1, CZ - 2, CZ - 1) if inner else (0, CZ - 1):
        p = column_plane(packed, z)
        p = p + jnp.where(rows == 0, bx[z : z + 1, :], jnp.where(rows == C - 1, hx[z : z + 1, :], 0.0))
        on_z[z] = p + bz if z == 0 else p + hz if z == CZ - 1 else p
    return on_x, on_y, on_z


def layer_weights(weight, wx, wy):
    return (
        {e: wx[i] for i, e in enumerate(EDGES)},
        {e: wy[i] for i, e in enumerate(EDGES)},
        {z: weight[z] for z in (0, 1, CZ - 2, CZ - 1)},
    )


def face_response(layers, weights):
    out = []
    for layer, w, last in zip(layers, weights, (C - 1, C - 1, CZ - 1)):
        for face, inside in ((0, 1), (last, last - 1)):
            once = w[face] * layer[face]
            near = in_plane(once) + w[inside] * layer[inside]
            out.append(KEPT * once + w[face] * (layer[face] + near))
    return out


def fold(t):
    return jnp.sum(t.reshape(t.shape[0] // 8, 8, C), axis=0)


def layer_energy(a, b, weights):
    rows = row_of((CZ, C))
    lanes = lane_of((CZ, C))
    inner = (rows > 0) & (rows < CZ - 1)
    both = inner & (lanes > 0) & (lanes < C - 1)
    acc = jnp.zeros((8, C), F32)
    for layers_a, layers_b, w, last, mask in zip(a, b, weights, (C - 1, C - 1, CZ - 1), (inner, both, None)):
        for e in (0, last):
            t = layers_a[e] * layers_b[e] * w[e]
            acc = acc + fold(t if mask is None else jnp.where(mask, t, 0.0))
    return jnp.sum(acc) / DAMPING_WEIGHT


def places():
    x, y, z = (lax.axis_index(a) for a in AXES)
    more = [i < lax.axis_size(a) - 1 for a, i in zip(AXES, (x, y, z))]
    less = [i > 0 for i in (x, y, z)]
    return (x % 2 == 0, y % 2 == 0, z == 0), more, less


def pick(flag, a, b):
    return lax.select(jnp.broadcast_to(flag, a.shape), a, b)


def pack_sends(sends, faces, index):
    (xeven, yeven, zlow), _, _ = places()
    xa, xb, ya, yb, zz = sends
    for even, a, b, lo, hi in ((xeven, xa, xb, faces[0], faces[1]), (yeven, ya, yb, faces[2], faces[3])):
        s = slice(index * CZ, (index + 1) * CZ)
        a[s, :] = pick(even, hi, lo)
        b[s, :] = pick(even, lo, hi)
    zz[index * C : (index + 1) * C, :] = pick(zlow, faces[5], faces[4])


def own_faces(src, own, turn):
    row_layer(src, 1, 0, own[0])
    row_layer(src, 1, C - 1, own[1])
    column_layers(src, 1, turn)
    own[2][...] = turn[layer_rows(2), :]
    own[3][...] = turn[layer_rows(1), :]
    own[4][...] = src[1, INNER, :]
    own[5][...] = src[CZ, INNER, :]


def first_kernel(heat_in, cond_in, proj_in, segs_in, weight, state, parts, heat, wx, wy, *refs):
    own = refs[:6]
    sends = refs[6:11]
    cond, proj, segs, start, turn, pack, sems, small = refs[11:]
    tables = (pltpu.make_async_copy(proj_in, proj, small.at[0]), pltpu.make_async_copy(segs_in, segs, small.at[1]))

    def copies(i):
        s = pl.ds(i * DEPTH, DEPTH)
        return (
            pltpu.make_async_copy(cond_in.at[s], cond.at[s], sems.at[0, i]),
            pltpu.make_async_copy(heat_in.at[s], heat.at[s], sems.at[1, i]),
        )

    for c in tables:
        c.start()
    for i in range(PARTS):
        for c in copies(i):
            c.start()
    zero_ends(start)
    zero_ends(state)
    pack[...] = jnp.zeros((C, C), F32)
    for c in tables:
        c.wait()
    for d in range(3):
        onehot = jnp.where(row_of((C, C)) == segs[d], 1.0, 0.0).astype(BF16)
        base = sum(lax.dot_general(onehot, p, (((1,), (1,)), ((), ())), preferred_element_type=F32) for p in reversed(parts_of(proj[d])))
        store_parts(parts, d, base)
        for a in (sends[:2], sends[2:4])[d] if d < 2 else ():
            a[CZ : CZ + C, :] = base
        if d == 2:
            sends[4][C : 2 * C, :] = base
    group = lane_of((C, C)) // 4

    def part(i, carry):
        for c in copies(i):
            c.wait()
        packed = pack[...]
        for j in range(DEPTH):
            z = i * DEPTH + j
            w = DAMPING_WEIGHT / (6.0 + cond[z])
            weight[z] = w
            start[z + 1, INNER, :] = w * heat[z]
            packed = jnp.where(group == z, pltpu.roll(w, 4 * z + 2, 1), packed)
        pack[...] = packed

        @pl.when(i > 0)
        def _():
            sweep_planes(start, state, weight, heat, (i - 1) * DEPTH, DEPTH, 16)

        return carry

    lax.fori_loop(0, PARTS, part, 0)
    sweep_planes(start, state, weight, heat, CZ - DEPTH, DEPTH, 16)
    own_faces(state, own, turn)
    pack_sends(sends, [f[...] for f in own], 0)
    for i, e in enumerate(EDGES):
        row_layer(weight, 0, e, wx.at[i])
    turn[...] = pack[...].T
    for i, e in enumerate((2, 3, 0, 1)):
        wy[i] = turn[layer_rows(e), :]


def free_kernel(state, weight, supply, out, *refs):
    own = refs[:6]
    mid, turn = refs[6:]
    zero_ends(mid)
    zero_ends(out)
    sweep(state, mid, weight, supply)
    sweep(mid, out, weight, supply)
    own_faces(out, own, turn)


def jumps(own, got, bases, prev_bases, back_bases, n, lifted):
    (xeven, yeven, zlow), more, less = places()
    xa, xb, ya, yb, zz = got
    for d, (even, a, b, rows) in enumerate(((xeven, xa, xb, n * CZ), (yeven, ya, yb, n * CZ), (zlow, zz, zz, n * C))):
        a = a[0:rows, :]
        b = b[0:rows, :]
        up = own[2 * d + 1][...] - dot(pick(even, a, b), bases, d)
        up = jnp.where(more[d], up, 0.0)
        down = pick(even, b, a) - dot(own[2 * d][...], prev_bases, d)
        back = jnp.where(less[d], -dot(down, back_bases, d), 0.0)
        size = rows // n
        for i in range(n):
            lifted[i][2 * d][...] = back[i * size : (i + 1) * size, :]
            lifted[i][2 * d + 1][...] = up[i * size : (i + 1) * size, :]


def square_sum(a, b):
    return jnp.sum(sum(fold(a[i][...] * b[i][...]) for i in (1, 3, 5)))


def row_of_sums(values):
    lanes = lane_of((1, C))
    row = jnp.zeros((1, C), F32)
    for i, v in enumerate(values):
        row = jnp.where(lanes == i, v, row)
    return row


def second_kernel(first, *refs):
    it = iter(refs)
    take = lambda n: [next(it) for _ in range(n)]
    own = take(6)
    got = take(5)
    (bases,) = take(1)
    prev, back = take(2) if not first else (None, None)
    weight, wx, wy = take(3)
    own_u = take(6)
    lifted = take(6)
    own_uv = take(6)
    sends = take(5)
    if first:
        prev, back = take(2)
    (turn,) = take(1)
    (xeven, yeven, _), _, _ = places()
    if first:
        xa, xb, ya, yb, zz = got
        for d, base in enumerate((pick(xeven, xb[CZ:, :], xa[CZ:, :]), pick(yeven, yb[CZ:, :], ya[CZ:, :]), zz[C:, :])):
            store_parts(prev, d, base)
            store_parts(back, d, base.T)
    jumps(own, got, bases, prev, back, 1, [lifted])
    response = face_response(lift_layers(lifted, turn, True), layer_weights(weight, wx, wy))
    free = [f[...] for f in own_u]
    for o, u, v in zip(own_uv, free, response):
        n = u.shape[0]
        o[0:n, :] = u
        o[n:, :] = v
    pack_sends(sends, free, 0)
    pack_sends(sends, response, 1)


def response_kernel(*refs):
    lifted = refs[:6]
    weight, resp, sums, lift, mid, turn, cols = refs[6:]
    cols[...] = pack_columns(turn, lifted[2][...], lifted[3][...])

    def plane(z, carry):
        lift[z] = column_plane(cols[...], z)
        return carry

    lax.fori_loop(0, CZ, plane, 0, unroll=WIDE)
    add_rows(lift, lifted, 1.0)
    zero_ends(mid)
    zero_ends(resp)

    def scale(z, acc):
        once = weight[z] * lift[z]
        mid[z + 1, INNER, :] = once
        return acc + fold(once * lift[z])

    acc = lax.fori_loop(0, CZ, scale, jnp.zeros((8, C), F32), unroll=UNROLL)
    sweep(mid, resp, weight, lift)
    sums[...] = row_of_sums([square_sum(lifted, lifted), jnp.sum(acc) / DAMPING_WEIGHT])


def merge_sides(low, high):
    return [f for pair in zip(low, high) for f in pair]


def third_kernel(first, *refs):
    it = iter(refs)
    take = lambda n: [next(it) for _ in range(n)]
    own_uv = take(6)
    got = take(5)
    bases, prev, back, weight, wx, wy, before = take(7)
    high_u, high_v = take(3), take(3)
    (rows,) = take(1)
    low_u, low_v = take(3), take(3)
    (turn,) = take(1)
    lift_u = merge_sides(low_u, high_u)
    lift_v = merge_sides(low_v, high_v)
    jumps(own_uv, got, bases, prev, back, 2, [lift_u, lift_v])
    weights = layer_weights(weight, wx, wy)
    u = lift_layers(lift_u, turn.at[0], False)
    v = lift_layers(lift_v, turn.at[1], False)
    sums = [square_sum(lift_u, lift_u), square_sum(lift_u, lift_v), square_sum(lift_v, lift_v)]
    sums += [layer_energy(u, u, weights), layer_energy(u, v, weights), layer_energy(v, v, weights)]
    lanes = lane_of((1, C))
    row = row_of_sums([0.0, 0.0] + sums)
    row = jnp.where(lanes < 2, before[...], row)
    rows[...] = jnp.broadcast_to(row, (C, C))


def steps(totals):
    row = jnp.sum(totals[...], axis=0, keepdims=True)
    lanes = lane_of((1, C))
    gg, gh, guu, guv, gvv, huu, huv, hvv = [jnp.sum(jnp.where(lanes == i, row, 0.0), axis=1, keepdims=True) for i in range(8)]
    one = gg / (gh + EPSILON)
    two = (guu - 2.0 * one * guv + one * one * gvv) / (huu - 2.0 * one * huv + one * one * hvv + EPSILON)
    return one, two


def fourth_kernel(*refs):
    it = iter(refs)
    take = lambda n: [next(it) for _ in range(n)]
    totals, heat, weight, free, resp = take(5)
    lift_1 = take(6)
    lift_u = take(6)
    lift_v = take(6)
    supply, state = take(2)
    high = take(3)
    own = take(6)
    sends = take(5)
    low = take(3)
    mid, turn, cols = take(3)
    held = merge_sides(low, high)
    one, two = steps(totals)
    for i in range(6):
        held[i][...] = one * lift_1[i][...] + two * (lift_u[i][...] - one * lift_v[i][...])
    cols[...] = pack_columns(turn, held[2][...], held[3][...])
    zero_ends(mid)
    zero_ends(state)

    def plane(z, carry):
        supply[z] = heat[z] - column_plane(cols[...], z)
        state[z + 1, INNER, :] = free[z + 1, INNER, :] - one * resp[z + 1, INNER, :]
        return carry

    lax.fori_loop(0, CZ, plane, 0, unroll=WIDE)
    add_rows(supply, held, -1.0)
    sweep(state, mid, weight, supply)
    sweep(mid, state, weight, supply)
    own_faces(state, own, turn)
    pack_sends(sends, [f[...] for f in own], 0)


def last_kernel(*refs):
    it = iter(refs)
    take = lambda n: [next(it) for _ in range(n)]
    totals, free, resp = take(3)
    held = take(3)
    lift_3 = take(3)
    lift_u = take(3)
    lift_v = take(3)
    (out,) = take(1)
    outs = take(3)
    state, sems = take(2)
    one, two = steps(totals)

    def plane(z, carry):
        state[z] = free[z + 1, INNER, :] - one * resp[z + 1, INNER, :]
        return carry

    copies = []
    for i in range(PARTS):
        lax.fori_loop(i * DEPTH, (i + 1) * DEPTH, plane, 0, unroll=UNROLL)
        s = pl.ds(i * DEPTH, DEPTH)
        copies.append(pltpu.make_async_copy(state.at[s], out.at[s], sems.at[i]))
        copies[-1].start()
    for i in range(3):
        outs[i][...] = held[i][...] + one * lift_3[i][...] + two * (lift_u[i][...] - one * lift_v[i][...])
    for c in copies:
        c.wait()


FIELD = jax.ShapeDtypeStruct((CZ, C, C), F32)
PADDED = jax.ShapeDtypeStruct((CZ + 2, C + 2 * PAD, C), F32)
FACE = jax.ShapeDtypeStruct((CZ, C), F32)
SQUARE = jax.ShapeDtypeStruct((C, C), F32)
FACES = [FACE] * 4 + [SQUARE] * 2
LAYERS = jax.ShapeDtypeStruct((4, CZ, C), F32)
ROW = jax.ShapeDtypeStruct((1, C), F32)
SIDE = [FACE, FACE, SQUARE]
S_SIDE = [pltpu.VMEM(f.shape, F32) for f in SIDE]
S_FIELD = pltpu.VMEM((CZ, C, C), F32)
S_PADDED = pltpu.VMEM((CZ + 2, C + 2 * PAD, C), F32)
PIECES = jax.ShapeDtypeStruct((9, C, C), BF16)
S_SQUARE = pltpu.VMEM((C, C), F32)


def sends_of(n, extra):
    small = jax.ShapeDtypeStruct((n * CZ + extra, C), F32)
    return [small] * 4 + [jax.ShapeDtypeStruct((n * C + extra, C), F32)]


def call(kernel, name, outs, scratch, args, us, in_specs=None, out_specs=None):
    return list(
        pl.pallas_call(
            kernel,
            out_shape=tuple(outs),
            in_specs=in_specs or [VM] * len(args),
            out_specs=tuple(out_specs or [VM] * len(outs)),
            scratch_shapes=scratch,
            name=name,
            compiler_params=pltpu.CompilerParams(vmem_limit_bytes=20 * 1024 * 1024),
            cost_estimate=pl.CostEstimate(flops=us * 10**7, transcendentals=0, bytes_accessed=2**20),
        )(*args)
    )


def swap_pairs(axis, start):
    n = lax.axis_size(axis)
    pairs = []
    for i in range(start, n, 2):
        j = (i + 1) % n
        pairs += [(i, j), (j, i)]
    return pairs


def exchange(sends):
    xa, xb, ya, yb, zz = sends
    zz = lax.ppermute(zz, "gz", swap_pairs("gz", 0))
    yb = lax.ppermute(yb, "gy", swap_pairs("gy", 1))
    xb = lax.ppermute(xb, "gx", swap_pairs("gx", 1))
    xa = lax.ppermute(xa, "gx", swap_pairs("gx", 0))
    ya = lax.ppermute(ya, "gy", swap_pairs("gy", 0))
    return [xa, xb, ya, yb, zz]


def gather_rows(rows):
    rows = lax.all_to_all(rows.reshape(C, 1, C), AXES, 0, 0)
    return rows.reshape(C, C)


def body(heat, cond, projection, segment_map):
    proj = projection[0, 0, 0]
    segs = segment_map.reshape(3, 1, C)
    dma = pltpu.SemaphoreType.DMA
    scratch = [S_FIELD, pltpu.VMEM(proj.shape, F32), pltpu.VMEM(segs.shape, jnp.int32), S_PADDED, S_SQUARE, S_SQUARE, dma((2, PARTS)), dma((2,))]
    outs = [FIELD, PADDED, PIECES, FIELD, LAYERS, LAYERS] + FACES + sends_of(1, C)
    out = call(first_kernel, "first", outs, scratch, [pltpu.with_memory_space_constraint(a, pltpu.MemorySpace.HBM) for a in (heat, cond, proj, segs)], 4, [AWAY] * 4)
    weight, state, bases, heat, wx, wy = out[:6]
    own, sends = out[6:12], out[12:]
    supply = heat
    prev = []
    held = None
    for pair in range(2):
        first = pair == 0
        got = exchange(sends)
        out = call(free_kernel, "free", [PADDED] + FACES, [S_PADDED, S_SQUARE], (state, weight, supply), 3)
        free, own_u = out[0], out[1:]
        args = own + got + [bases] + prev + [weight, wx, wy] + own_u
        stacked = [jax.ShapeDtypeStruct((2 * f.shape[0], C), F32) for f in FACES]
        outs = FACES + stacked + sends_of(2, 0) + ([PIECES, PIECES] if first else [])
        out = call(functools.partial(second_kernel, first), "second", outs, [S_SQUARE], args, 2)
        lift_1, own_uv, sends = out[:6], out[6:12], out[12:17]
        if first:
            prev = out[17:]
        got = exchange(sends)
        resp, sums = call(response_kernel, "response", [PADDED, ROW], [S_FIELD, S_PADDED, S_SQUARE, S_SQUARE], lift_1 + [weight], 3)
        args = own_uv + got + [bases] + prev + [weight, wx, wy, sums]
        outs = SIDE + SIDE + [SQUARE] + (SIDE + SIDE if first else [])
        scratch = ([] if first else S_SIDE + S_SIDE) + [pltpu.VMEM((2, C, C), F32)]
        out = call(functools.partial(third_kernel, first), "third", outs, scratch, args, 2)
        high_u, high_v, rows = out[:3], out[3:6], out[6]
        totals = gather_rows(rows)
        if first:
            args = [totals, heat, weight, free, resp] + lift_1 + merge_sides(out[7:10], high_u) + merge_sides(out[10:13], high_v)
            outs = [FIELD, PADDED] + SIDE + FACES + sends_of(1, 0)
            out = call(fourth_kernel, "fourth", outs, S_SIDE + [S_PADDED, S_SQUARE, S_SQUARE], args, 5)
            supply, state, held, own, sends = out[0], out[1], out[2:5], out[5:11], out[11:]
    args = [totals, free, resp] + held + [lift_1[i] for i in (1, 3, 5)] + high_u + high_v
    state, mx, my, mz = call(last_kernel, "last", [FIELD, FACE, FACE, SQUARE], [S_FIELD, dma((PARTS,))], args, 2, None, [AWAY, VM, VM, VM])
    return state, mx[None, None, None], my[None, None, None], mz[None, None, None]


def solution(mesh):
    field = P("gz", "gx", "gy")
    in_specs = (field, field, P("gz", "gx", "gy", None, None, None), P("gz", "gx", "gy", None, None))
    face = P("gz", "gx", "gy", None, None)
    return jax.shard_map(body, mesh=mesh, in_specs=in_specs, out_specs=(field, face, face, face), check_vma=False)
```

```python
import functools

import jax
import jax.numpy as jnp
from jax import lax
from jax.experimental import pallas as pl
from jax.experimental.pallas import tpu as pltpu
from jax.sharding import PartitionSpec as P

DAMPING_WEIGHT = 0.8
EPSILON = 1e-06
AXES = ("gx", "gy", "gz")
CZ = 32
C = 128
F32 = jnp.float32
UNROLL = 4
WIDE = 16
DEPTH = 8
PARTS = CZ // DEPTH
KEPT = 1.0 - DAMPING_WEIGHT

VM = pl.BlockSpec(memory_space=pltpu.MemorySpace.VMEM)
AWAY = pl.BlockSpec(memory_space=pltpu.MemorySpace.HBM)
BF16 = jnp.bfloat16
PAD = 8


def parts_of(a):
    first = a.astype(BF16)
    rest = a - first.astype(F32)
    second = rest.astype(BF16)
    third = (rest - second.astype(F32)).astype(BF16)
    return first, second, third


def dot(a, parts, d):
    n = a.shape[0]
    mul = functools.partial(jnp.dot, preferred_element_type=F32)
    a1, a2, a3 = parts_of(a)
    r = mul(jnp.concatenate([a1, a2, a3], axis=0), parts[d, :, 0 : 2 * C])
    t = mul(a1, parts[d, :, 2 * C :])
    small = r[2 * n :, :C] + r[n : 2 * n, C:] + t
    return r[:n, :C] + (r[n : 2 * n, :C] + r[:n, C:] + small)


def store_parts(ref, d, a):
    for i, p in enumerate(parts_of(a)):
        ref[d, :, i * C : (i + 1) * C] = p


def lane_of(shape):
    return lax.broadcasted_iota(jnp.int32, shape, len(shape) - 1)


def row_of(shape):
    return lax.broadcasted_iota(jnp.int32, shape, len(shape) - 2)


INNER = slice(PAD, PAD + C)


def zero_ends(ref):
    ref[0] = jnp.zeros((C + 2 * PAD, C), F32)
    ref[CZ + 1] = jnp.zeros((C + 2 * PAD, C), F32)
    for z in range(1, CZ + 1):
        ref[z, 0:PAD, :] = jnp.zeros((PAD, C), F32)
        ref[z, PAD + C :, :] = jnp.zeros((PAD, C), F32)


def in_plane(centre):
    shape = centre.shape
    rows = row_of(shape)
    lanes = lane_of(shape)
    near = jnp.where(rows == 0, 0.0, pltpu.roll(centre, 1, 0))
    near = near + jnp.where(rows == shape[0] - 1, 0.0, pltpu.roll(centre, shape[0] - 1, 0))
    near = near + jnp.where(lanes == 0, 0.0, pltpu.roll(centre, 1, 1))
    return near + jnp.where(lanes == C - 1, 0.0, pltpu.roll(centre, C - 1, 1))


def sweep_planes(src, dst, weight, supply, z, depth, block):
    lanes = lane_of((block, C))
    low = lanes == 0
    high = lanes == C - 1
    for x in range(0, C, block):
        r = PAD + x
        column = [src[z + j, r : r + block, :] for j in range(depth + 2)]
        for j in range(depth):
            centre = column[j + 1]
            near = column[j] + column[j + 2]
            near = near + src[z + j + 1, r - 1 : r - 1 + block, :] + src[z + j + 1, r + 1 : r + 1 + block, :]
            near = near + jnp.where(low, 0.0, pltpu.roll(centre, 1, 1)) + jnp.where(high, 0.0, pltpu.roll(centre, C - 1, 1))
            dst[z + j + 1, r : r + block, :] = KEPT * centre + weight[z + j, x : x + block, :] * (supply[z + j, x : x + block, :] + near)


def sweep(src, dst, weight, supply):
    def planes(i, carry):
        sweep_planes(src, dst, weight, supply, i * WIDE, WIDE, 8)
        return carry

    lax.fori_loop(0, CZ // WIDE, planes, 0)


def row_layer(src, base, at, out):
    for z in range(CZ):
        out[z : z + 1, :] = src[z + base, PAD * base + at : PAD * base + at + 1, :]


def column_layers(src, base, turn):
    group = lane_of((C, C)) // 4

    def plane(z, packed):
        return jnp.where(group == z, pltpu.roll(src[z + base, PAD * base : PAD * base + C, :], 4 * z + 2, 1), packed)

    packed = lax.fori_loop(0, CZ, plane, jnp.zeros((C, C), F32), unroll=CZ)
    turn[...] = packed.T


def layer_rows(i):
    return pl.ds(i, CZ, stride=4)


def pack_columns(turn, low, high):
    turn[...] = jnp.zeros((C, C), F32)
    turn[layer_rows(1), :] = high
    turn[layer_rows(2), :] = low
    return turn[...].T


def column_plane(packed, z):
    lanes = lane_of((C, C))
    edge = (lanes == 0) | (lanes == C - 1)
    return jnp.where(edge, pltpu.roll(packed, C - 2 - 4 * z, 1), 0.0)


def add_rows(dst, faces, sign):
    for z in range(CZ):
        dst[z, 0:1, :] = dst[z, 0:1, :] + sign * faces[0][z : z + 1, :]
        dst[z, C - 1 : C, :] = dst[z, C - 1 : C, :] + sign * faces[1][z : z + 1, :]
    dst[0] = dst[0] + sign * faces[4][...]
    dst[CZ - 1] = dst[CZ - 1] + sign * faces[5][...]


EDGES = (0, 1, C - 2, C - 1)


def rim(low, high, at):
    lanes = lane_of(low.shape)
    a = low if at == 0 else pltpu.roll(low, C - at, 1)
    b = high if at == C - 1 else pltpu.roll(high, C - 1 - at, 1)
    return jnp.where(lanes == 0, a, jnp.where(lanes == C - 1, b, 0.0))


def ends(low, high):
    rows = row_of((CZ, C))
    return jnp.where(rows == 0, low, jnp.where(rows == CZ - 1, high, 0.0))


def lift_layers(faces, turn, inner):
    bx, hx, by, hy, bz, hz = [f[...] for f in faces]
    lanes = lane_of((C, C))
    columns = jnp.where(lanes < 4, pltpu.roll(bz, 2, 1), pltpu.roll(hz, 6, 1)).T
    at = lambda i: columns[i : i + 1, :]
    column = {C - 2: (at(0), at(4)), C - 1: (at(1), at(5)), 0: (at(2), at(6)), 1: (at(3), at(7))}
    edges = EDGES if inner else (0, C - 1)
    on_x = {}
    on_y = {}
    for e in edges:
        on_x[e] = rim(by, hy, e) + ends(bz[e : e + 1, :], hz[e : e + 1, :])
        on_y[e] = rim(bx, hx, e) + ends(*column[e])
    on_x[0] = on_x[0] + bx
    on_x[C - 1] = on_x[C - 1] + hx
    on_y[0] = on_y[0] + by
    on_y[C - 1] = on_y[C - 1] + hy
    packed = pack_columns(turn, by, hy)
    rows = row_of((C, C))
    on_z = {}
    for z in (0, 1, CZ - 2, CZ - 1) if inner else (0, CZ - 1):
        p = column_plane(packed, z)
        p = p + jnp.where(rows == 0, bx[z : z + 1, :], jnp.where(rows == C - 1, hx[z : z + 1, :], 0.0))
        on_z[z] = p + bz if z == 0 else p + hz if z == CZ - 1 else p
    return on_x, on_y, on_z


def layer_weights(weight, wx, wy):
    return (
        {e: wx[i] for i, e in enumerate(EDGES)},
        {e: wy[i] for i, e in enumerate(EDGES)},
        {z: weight[z] for z in (0, 1, CZ - 2, CZ - 1)},
    )


def face_response(layers, weights):
    out = []
    for layer, w, last in zip(layers, weights, (C - 1, C - 1, CZ - 1)):
        for face, inside in ((0, 1), (last, last - 1)):
            once = w[face] * layer[face]
            near = in_plane(once) + w[inside] * layer[inside]
            out.append(KEPT * once + w[face] * (layer[face] + near))
    return out


def fold(t):
    return jnp.sum(t.reshape(t.shape[0] // 8, 8, C), axis=0)


def layer_energy(a, b, weights):
    rows = row_of((CZ, C))
    lanes = lane_of((CZ, C))
    inner = (rows > 0) & (rows < CZ - 1)
    both = inner & (lanes > 0) & (lanes < C - 1)
    acc = jnp.zeros((8, C), F32)
    for layers_a, layers_b, w, last, mask in zip(a, b, weights, (C - 1, C - 1, CZ - 1), (inner, both, None)):
        for e in (0, last):
            t = layers_a[e] * layers_b[e] * w[e]
            acc = acc + fold(t if mask is None else jnp.where(mask, t, 0.0))
    return jnp.sum(acc) / DAMPING_WEIGHT


def places():
    x, y, z = (lax.axis_index(a) for a in AXES)
    more = [i < lax.axis_size(a) - 1 for a, i in zip(AXES, (x, y, z))]
    less = [i > 0 for i in (x, y, z)]
    return (x % 2 == 0, y % 2 == 0, z == 0), more, less


def pick(flag, a, b):
    return lax.select(jnp.broadcast_to(flag, a.shape), a, b)


def pack_sends(sends, faces, index):
    (xeven, yeven, zlow), _, _ = places()
    xa, xb, ya, yb, zz = sends
    for even, a, b, lo, hi in ((xeven, xa, xb, faces[0], faces[1]), (yeven, ya, yb, faces[2], faces[3])):
        s = slice(index * CZ, (index + 1) * CZ)
        a[s, :] = pick(even, hi, lo)
        b[s, :] = pick(even, lo, hi)
    zz[index * C : (index + 1) * C, :] = pick(zlow, faces[5], faces[4])


def own_faces(src, own, turn):
    row_layer(src, 1, 0, own[0])
    row_layer(src, 1, C - 1, own[1])
    column_layers(src, 1, turn)
    own[2][...] = turn[layer_rows(2), :]
    own[3][...] = turn[layer_rows(1), :]
    own[4][...] = src[1, INNER, :]
    own[5][...] = src[CZ, INNER, :]


def first_kernel(heat_in, cond_in, proj_in, segs_in, weight, state, parts, heat, wx, wy, *refs):
    own = refs[:6]
    sends = refs[6:11]
    cond, proj, segs, start, turn, pack, sems, small = refs[11:]
    tables = (pltpu.make_async_copy(proj_in, proj, small.at[0]), pltpu.make_async_copy(segs_in, segs, small.at[1]))

    def copies(i):
        s = pl.ds(i * DEPTH, DEPTH)
        return (
            pltpu.make_async_copy(cond_in.at[s], cond.at[s], sems.at[0, i]),
            pltpu.make_async_copy(heat_in.at[s], heat.at[s], sems.at[1, i]),
        )

    for c in tables:
        c.start()
    for i in range(PARTS):
        for c in copies(i):
            c.start()
    zero_ends(start)
    zero_ends(state)
    pack[...] = jnp.zeros((C, C), F32)
    group = lane_of((C, C)) // 4

    def part(i, carry):
        for c in copies(i):
            c.wait()
        packed = pack[...]
        for j in range(DEPTH):
            z = i * DEPTH + j
            w = DAMPING_WEIGHT / (6.0 + cond[z])
            weight[z] = w
            start[z + 1, INNER, :] = w * heat[z]
            packed = jnp.where(group == z, pltpu.roll(w, 4 * z + 2, 1), packed)
        pack[...] = packed

        @pl.when(i > 0)
        def _():
            sweep_planes(start, state, weight, heat, (i - 1) * DEPTH, DEPTH, 16)

        return carry

    lax.fori_loop(0, PARTS, part, 0)
    sweep_planes(start, state, weight, heat, CZ - DEPTH, DEPTH, 16)
    for c in tables:
        c.wait()
    for d in range(3):
        onehot = jnp.where(row_of((C, C)) == segs[d], 1.0, 0.0).astype(BF16)
        base = sum(lax.dot_general(onehot, p, (((1,), (1,)), ((), ())), preferred_element_type=F32) for p in reversed(parts_of(proj[d])))
        store_parts(parts, d, base)
        for a in (sends[:2], sends[2:4])[d] if d < 2 else ():
            a[CZ : CZ + C, :] = base
        if d == 2:
            sends[4][C : 2 * C, :] = base
    own_faces(state, own, turn)
    pack_sends(sends, [f[...] for f in own], 0)
    for i, e in enumerate(EDGES):
        row_layer(weight, 0, e, wx.at[i])
    turn[...] = pack[...].T
    for i, e in enumerate((2, 3, 0, 1)):
        wy[i] = turn[layer_rows(e), :]


def free_kernel(state, weight, supply, out, *refs):
    own = refs[:6]
    mid, turn = refs[6:]
    zero_ends(mid)
    zero_ends(out)
    sweep(state, mid, weight, supply)
    sweep(mid, out, weight, supply)
    own_faces(out, own, turn)


def jumps(own, got, bases, prev_bases, back_bases, n, lifted):
    (xeven, yeven, zlow), more, less = places()
    xa, xb, ya, yb, zz = got
    for d, (even, a, b, rows) in enumerate(((xeven, xa, xb, n * CZ), (yeven, ya, yb, n * CZ), (zlow, zz, zz, n * C))):
        a = a[0:rows, :]
        b = b[0:rows, :]
        up = own[2 * d + 1][...] - dot(pick(even, a, b), bases, d)
        up = jnp.where(more[d], up, 0.0)
        down = pick(even, b, a) - dot(own[2 * d][...], prev_bases, d)
        back = jnp.where(less[d], -dot(down, back_bases, d), 0.0)
        size = rows // n
        for i in range(n):
            lifted[i][2 * d][...] = back[i * size : (i + 1) * size, :]
            lifted[i][2 * d + 1][...] = up[i * size : (i + 1) * size, :]


def square_sum(a, b):
    return jnp.sum(sum(fold(a[i][...] * b[i][...]) for i in (1, 3, 5)))


def row_of_sums(values):
    lanes = lane_of((1, C))
    row = jnp.zeros((1, C), F32)
    for i, v in enumerate(values):
        row = jnp.where(lanes == i, v, row)
    return row


def second_kernel(first, *refs):
    it = iter(refs)
    take = lambda n: [next(it) for _ in range(n)]
    own = take(6)
    got = take(5)
    (bases,) = take(1)
    prev, back = take(2) if not first else (None, None)
    weight, wx, wy = take(3)
    own_u = take(6)
    lifted = take(6)
    own_uv = take(6)
    sends = take(5)
    if first:
        prev, back = take(2)
    (turn,) = take(1)
    (xeven, yeven, _), _, _ = places()
    if first:
        xa, xb, ya, yb, zz = got
        for d, base in enumerate((pick(xeven, xb[CZ:, :], xa[CZ:, :]), pick(yeven, yb[CZ:, :], ya[CZ:, :]), zz[C:, :])):
            store_parts(prev, d, base)
            store_parts(back, d, base.T)
    jumps(own, got, bases, prev, back, 1, [lifted])
    response = face_response(lift_layers(lifted, turn, True), layer_weights(weight, wx, wy))
    free = [f[...] for f in own_u]
    for o, u, v in zip(own_uv, free, response):
        n = u.shape[0]
        o[0:n, :] = u
        o[n:, :] = v
    pack_sends(sends, free, 0)
    pack_sends(sends, response, 1)


def response_kernel(*refs):
    lifted = refs[:6]
    weight, resp, sums, lift, mid, turn, cols = refs[6:]
    cols[...] = pack_columns(turn, lifted[2][...], lifted[3][...])

    def plane(z, carry):
        lift[z] = column_plane(cols[...], z)
        return carry

    lax.fori_loop(0, CZ, plane, 0, unroll=WIDE)
    add_rows(lift, lifted, 1.0)
    zero_ends(mid)
    zero_ends(resp)

    def scale(z, acc):
        once = weight[z] * lift[z]
        mid[z + 1, INNER, :] = once
        return acc + fold(once * lift[z])

    acc = lax.fori_loop(0, CZ, scale, jnp.zeros((8, C), F32), unroll=UNROLL)
    sweep(mid, resp, weight, lift)
    sums[...] = row_of_sums([square_sum(lifted, lifted), jnp.sum(acc) / DAMPING_WEIGHT])


def merge_sides(low, high):
    return [f for pair in zip(low, high) for f in pair]


def third_kernel(*refs):
    it = iter(refs)
    take = lambda n: [next(it) for _ in range(n)]
    own_uv = take(6)
    got = take(5)
    bases, prev, back, weight, wx, wy, before = take(7)
    high_u, high_v = take(3), take(3)
    (rows,) = take(1)
    low_u, low_v = take(3), take(3)
    (turn,) = take(1)
    lift_u = merge_sides(low_u, high_u)
    lift_v = merge_sides(low_v, high_v)
    jumps(own_uv, got, bases, prev, back, 2, [lift_u, lift_v])
    weights = layer_weights(weight, wx, wy)
    u = lift_layers(lift_u, turn.at[0], False)
    v = lift_layers(lift_v, turn.at[1], False)
    sums = [square_sum(lift_u, lift_u), square_sum(lift_u, lift_v), square_sum(lift_v, lift_v)]
    sums += [layer_energy(u, u, weights), layer_energy(u, v, weights), layer_energy(v, v, weights)]
    lanes = lane_of((1, C))
    row = row_of_sums([0.0, 0.0] + sums)
    row = jnp.where(lanes < 2, before[...], row)
    rows[...] = jnp.broadcast_to(row, (C, C))


def steps(totals):
    row = jnp.sum(totals[...], axis=0, keepdims=True)
    lanes = lane_of((1, C))
    gg, gh, guu, guv, gvv, huu, huv, hvv = [jnp.sum(jnp.where(lanes == i, row, 0.0), axis=1, keepdims=True) for i in range(8)]
    one = gg / (gh + EPSILON)
    two = (guu - 2.0 * one * guv + one * one * gvv) / (huu - 2.0 * one * huv + one * one * hvv + EPSILON)
    return one, two


def fourth_kernel(*refs):
    it = iter(refs)
    take = lambda n: [next(it) for _ in range(n)]
    totals, heat, weight, free, resp = take(5)
    lift_1 = take(6)
    lift_u = take(6)
    lift_v = take(6)
    supply, state = take(2)
    high = take(3)
    own = take(6)
    sends = take(5)
    low = take(3)
    mid, turn, cols = take(3)
    held = merge_sides(low, high)
    one, two = steps(totals)
    for i in range(6):
        held[i][...] = one * lift_1[i][...] + two * (lift_u[i][...] - one * lift_v[i][...])
    cols[...] = pack_columns(turn, held[2][...], held[3][...])
    zero_ends(mid)
    zero_ends(state)

    def plane(z, carry):
        supply[z] = heat[z] - column_plane(cols[...], z)
        state[z + 1, INNER, :] = free[z + 1, INNER, :] - one * resp[z + 1, INNER, :]
        return carry

    lax.fori_loop(0, CZ, plane, 0, unroll=WIDE)
    add_rows(supply, held, -1.0)
    sweep(state, mid, weight, supply)
    sweep(mid, state, weight, supply)
    own_faces(state, own, turn)
    pack_sends(sends, [f[...] for f in own], 0)


def last_kernel(*refs):
    it = iter(refs)
    take = lambda n: [next(it) for _ in range(n)]
    totals, free, resp = take(3)
    held = take(3)
    lift_3 = take(3)
    lift_u = take(3)
    lift_v = take(3)
    (out,) = take(1)
    outs = take(3)
    state, sems = take(2)
    one, two = steps(totals)

    def plane(z, carry):
        state[z] = free[z + 1, INNER, :] - one * resp[z + 1, INNER, :]
        return carry

    copies = []
    for i in range(PARTS):
        lax.fori_loop(i * DEPTH, (i + 1) * DEPTH, plane, 0, unroll=UNROLL)
        s = pl.ds(i * DEPTH, DEPTH)
        copies.append(pltpu.make_async_copy(state.at[s], out.at[s], sems.at[i]))
        copies[-1].start()
    for i in range(3):
        outs[i][...] = held[i][...] + one * lift_3[i][...] + two * (lift_u[i][...] - one * lift_v[i][...])
    for c in copies:
        c.wait()


FIELD = jax.ShapeDtypeStruct((CZ, C, C), F32)
PADDED = jax.ShapeDtypeStruct((CZ + 2, C + 2 * PAD, C), F32)
FACE = jax.ShapeDtypeStruct((CZ, C), F32)
SQUARE = jax.ShapeDtypeStruct((C, C), F32)
FACES = [FACE] * 4 + [SQUARE] * 2
LAYERS = jax.ShapeDtypeStruct((4, CZ, C), F32)
ROW = jax.ShapeDtypeStruct((1, C), F32)
SIDE = [FACE, FACE, SQUARE]
S_SIDE = [pltpu.VMEM(f.shape, F32) for f in SIDE]
S_FIELD = pltpu.VMEM((CZ, C, C), F32)
S_PADDED = pltpu.VMEM((CZ + 2, C + 2 * PAD, C), F32)
PIECES = jax.ShapeDtypeStruct((3, C, 3 * C), BF16)
S_SQUARE = pltpu.VMEM((C, C), F32)


def sends_of(n, extra):
    small = jax.ShapeDtypeStruct((n * CZ + extra, C), F32)
    return [small] * 4 + [jax.ShapeDtypeStruct((n * C + extra, C), F32)]


def call(kernel, outs, scratch, args, us, in_specs=None, out_specs=None):
    return list(
        pl.pallas_call(
            kernel,
            out_shape=tuple(outs),
            in_specs=in_specs or [VM] * len(args),
            out_specs=tuple(out_specs or [VM] * len(outs)),
            scratch_shapes=scratch,
            compiler_params=pltpu.CompilerParams(vmem_limit_bytes=20 * 1024 * 1024),
            cost_estimate=pl.CostEstimate(flops=us * 10**7, transcendentals=0, bytes_accessed=2**20),
        )(*args)
    )


def swap_pairs(along, start):
    nx, ny = lax.axis_size("gx"), lax.axis_size("gy")
    place = lambda x, y: x * ny + y
    pairs = []
    for x in range(nx):
        for y in range(ny):
            i, n = (x, nx) if along == "x" else (y, ny)
            j = i + 1 if i % 2 == start else i - 1
            if 0 <= j < n:
                other = place(j, y) if along == "x" else place(x, j)
            else:
                other = place(x, y ^ 1) if along == "x" else place(x ^ 1, y)
            pairs.append((place(x, y), other))
    return pairs


def exchange(sends):
    xa, xb, ya, yb, zz = sends
    both = ("gx", "gy")
    xa = lax.ppermute(xa, both, swap_pairs("x", 0))
    yb = lax.ppermute(yb, both, swap_pairs("y", 1))
    zz = lax.ppermute(zz, "gz", [(0, 1), (1, 0)])
    xb = lax.ppermute(xb, both, swap_pairs("x", 1))
    ya = lax.ppermute(ya, both, swap_pairs("y", 0))
    return [xa, xb, ya, yb, zz]


def gather_rows(rows):
    rows = lax.all_to_all(rows.reshape(C, 1, C), AXES, 0, 0)
    return rows.reshape(C, C)


def body(heat, cond, projection, segment_map):
    proj = projection[0, 0, 0]
    segs = segment_map.reshape(3, 1, C)
    dma = pltpu.SemaphoreType.DMA
    scratch = [S_FIELD, pltpu.VMEM(proj.shape, F32), pltpu.VMEM(segs.shape, jnp.int32), S_PADDED, S_SQUARE, S_SQUARE, dma((2, PARTS)), dma((2,))]
    outs = [FIELD, PADDED, PIECES, FIELD, LAYERS, LAYERS] + FACES + sends_of(1, C)
    out = call(first_kernel, outs, scratch, [pltpu.with_memory_space_constraint(a, pltpu.MemorySpace.HBM) for a in (heat, cond, proj, segs)], 4, [AWAY] * 4)
    weight, state, bases, heat, wx, wy = out[:6]
    own, sends = out[6:12], out[12:]
    supply = heat
    prev = []
    held = None
    for pair in range(2):
        first = pair == 0
        got = exchange(sends)
        out = call(free_kernel, [PADDED] + FACES, [S_PADDED, S_SQUARE], (state, weight, supply), 3)
        free, own_u = out[0], out[1:]
        args = own + got + [bases] + prev + [weight, wx, wy] + own_u
        stacked = [jax.ShapeDtypeStruct((2 * f.shape[0], C), F32) for f in FACES]
        outs = FACES + stacked + sends_of(2, 0) + ([PIECES, PIECES] if first else [])
        out = call(functools.partial(second_kernel, first), outs, [S_SQUARE], args, 2)
        lift_1, own_uv, sends = out[:6], out[6:12], out[12:17]
        if first:
            prev = out[17:]
        got = exchange(sends)
        resp, sums = call(response_kernel, [PADDED, ROW], [S_FIELD, S_PADDED, S_SQUARE, S_SQUARE], lift_1 + [weight], 3)
        args = own_uv + got + [bases] + prev + [weight, wx, wy, sums]
        outs = SIDE + SIDE + [SQUARE] + (SIDE + SIDE if first else [])
        scratch = ([] if first else S_SIDE + S_SIDE) + [pltpu.VMEM((2, C, C), F32)]
        out = call(third_kernel, outs, scratch, args, 2)
        high_u, high_v, rows = out[:3], out[3:6], out[6]
        totals = gather_rows(rows)
        if first:
            args = [totals, heat, weight, free, resp] + lift_1 + merge_sides(out[7:10], high_u) + merge_sides(out[10:13], high_v)
            outs = [FIELD, PADDED] + SIDE + FACES + sends_of(1, 0)
            out = call(fourth_kernel, outs, S_SIDE + [S_PADDED, S_SQUARE, S_SQUARE], args, 5)
            supply, state, held, own, sends = out[0], out[1], out[2:5], out[5:11], out[11:]
    args = [totals, free, resp] + held + [lift_1[i] for i in (1, 3, 5)] + high_u + high_v
    state, mx, my, mz = call(last_kernel, [FIELD, FACE, FACE, SQUARE], [S_FIELD, dma((PARTS,))], args, 2, None, [AWAY, VM, VM, VM])
    return state, mx[None, None, None], my[None, None, None], mz[None, None, None]


def solution(mesh):
    field = P("gz", "gx", "gy")
    in_specs = (field, field, P("gz", "gx", "gy", None, None, None), P("gz", "gx", "gy", None, None))
    face = P("gz", "gx", "gy", None, None)
    return jax.shard_map(body, mesh=mesh, in_specs=in_specs, out_specs=(field, face, face, face), check_vma=False)
```

```python
import functools

import jax
import jax.numpy as jnp
from jax import lax
from jax.experimental import pallas as pl
from jax.experimental.pallas import tpu as pltpu
from jax.sharding import PartitionSpec as P

DAMPING_WEIGHT = 0.8
EPSILON = 1e-06
AXES = ("gx", "gy", "gz")
CZ = 32
C = 128
F32 = jnp.float32
UNROLL = 4
WIDE = 16
DEPTH = 8
PARTS = CZ // DEPTH
KEPT = 1.0 - DAMPING_WEIGHT

VM = pl.BlockSpec(memory_space=pltpu.MemorySpace.VMEM)
AWAY = pl.BlockSpec(memory_space=pltpu.MemorySpace.HBM)
BF16 = jnp.bfloat16
PAD = 8


def parts_of(a):
    first = a.astype(BF16)
    rest = a - first.astype(F32)
    second = rest.astype(BF16)
    third = (rest - second.astype(F32)).astype(BF16)
    return first, second, third


def dot(a, parts, d):
    n = a.shape[0]
    mul = functools.partial(jnp.dot, preferred_element_type=F32)
    a1, a2, a3 = parts_of(a)
    r = mul(jnp.concatenate([a1, a2, a3], axis=0), parts[d, :, 0 : 2 * C])
    t = mul(a1, parts[d, :, 2 * C :])
    small = r[2 * n :, :C] + r[n : 2 * n, C:] + t
    return r[:n, :C] + (r[n : 2 * n, :C] + r[:n, C:] + small)


def store_parts(ref, d, a):
    for i, p in enumerate(parts_of(a)):
        ref[d, :, i * C : (i + 1) * C] = p


def lane_of(shape):
    return lax.broadcasted_iota(jnp.int32, shape, len(shape) - 1)


def row_of(shape):
    return lax.broadcasted_iota(jnp.int32, shape, len(shape) - 2)


INNER = slice(PAD, PAD + C)


def zero_ends(ref):
    ref[0] = jnp.zeros((C + 2 * PAD, C), F32)
    ref[CZ + 1] = jnp.zeros((C + 2 * PAD, C), F32)
    for z in range(1, CZ + 1):
        ref[z, 0:PAD, :] = jnp.zeros((PAD, C), F32)
        ref[z, PAD + C :, :] = jnp.zeros((PAD, C), F32)


def in_plane(centre):
    shape = centre.shape
    rows = row_of(shape)
    lanes = lane_of(shape)
    near = jnp.where(rows == 0, 0.0, pltpu.roll(centre, 1, 0))
    near = near + jnp.where(rows == shape[0] - 1, 0.0, pltpu.roll(centre, shape[0] - 1, 0))
    near = near + jnp.where(lanes == 0, 0.0, pltpu.roll(centre, 1, 1))
    return near + jnp.where(lanes == C - 1, 0.0, pltpu.roll(centre, C - 1, 1))


def sweep_planes(src, dst, weight, supply, z, depth, block, rows=None):
    lanes = lane_of((block, C))
    low = lanes == 0
    high = lanes == C - 1
    for x in range(0, C, block) if rows is None else rows:
        r = PAD + x
        column = [src[z + j, r : r + block, :] for j in range(depth + 2)]
        for j in range(depth):
            centre = column[j + 1]
            near = column[j] + column[j + 2]
            near = near + src[z + j + 1, r - 1 : r - 1 + block, :] + src[z + j + 1, r + 1 : r + 1 + block, :]
            near = near + jnp.where(low, 0.0, pltpu.roll(centre, 1, 1)) + jnp.where(high, 0.0, pltpu.roll(centre, C - 1, 1))
            dst[z + j + 1, r : r + block, :] = KEPT * centre + weight[z + j, x : x + block, :] * (supply[z + j, x : x + block, :] + near)


def sweep(src, dst, weight, supply):
    sweep_planes(src, dst, weight, supply, 0, CZ, 8)


def row_layer(src, base, at, out):
    for z in range(CZ):
        out[z : z + 1, :] = src[z + base, PAD * base + at : PAD * base + at + 1, :]


def column_layers(src, base, turn):
    group = lane_of((C, C)) // 4

    def plane(z, packed):
        return jnp.where(group == z, pltpu.roll(src[z + base, PAD * base : PAD * base + C, :], 4 * z + 2, 1), packed)

    packed = lax.fori_loop(0, CZ, plane, jnp.zeros((C, C), F32), unroll=CZ)
    turn[...] = packed.T


def layer_rows(i):
    return pl.ds(i, CZ, stride=4)


def pack_columns(turn, low, high):
    turn[...] = jnp.zeros((C, C), F32)
    turn[layer_rows(1), :] = high
    turn[layer_rows(2), :] = low
    return turn[...].T


def column_plane(packed, z):
    lanes = lane_of((C, C))
    edge = (lanes == 0) | (lanes == C - 1)
    return jnp.where(edge, pltpu.roll(packed, C - 2 - 4 * z, 1), 0.0)


def add_rows(dst, faces, sign):
    for z in range(CZ):
        dst[z, 0:1, :] = dst[z, 0:1, :] + sign * faces[0][z : z + 1, :]
        dst[z, C - 1 : C, :] = dst[z, C - 1 : C, :] + sign * faces[1][z : z + 1, :]
    dst[0] = dst[0] + sign * faces[4][...]
    dst[CZ - 1] = dst[CZ - 1] + sign * faces[5][...]


EDGES = (0, 1, C - 2, C - 1)


def rim(low, high, at):
    lanes = lane_of(low.shape)
    a = low if at == 0 else pltpu.roll(low, C - at, 1)
    b = high if at == C - 1 else pltpu.roll(high, C - 1 - at, 1)
    return jnp.where(lanes == 0, a, jnp.where(lanes == C - 1, b, 0.0))


def ends(low, high):
    rows = row_of((CZ, C))
    return jnp.where(rows == 0, low, jnp.where(rows == CZ - 1, high, 0.0))


def lift_layers(faces, turn, inner):
    bx, hx, by, hy, bz, hz = [f[...] for f in faces]
    lanes = lane_of((C, C))
    columns = jnp.where(lanes < 4, pltpu.roll(bz, 2, 1), pltpu.roll(hz, 6, 1)).T
    at = lambda i: columns[i : i + 1, :]
    column = {C - 2: (at(0), at(4)), C - 1: (at(1), at(5)), 0: (at(2), at(6)), 1: (at(3), at(7))}
    edges = EDGES if inner else (0, C - 1)
    on_x = {}
    on_y = {}
    for e in edges:
        on_x[e] = rim(by, hy, e) + ends(bz[e : e + 1, :], hz[e : e + 1, :])
        on_y[e] = rim(bx, hx, e) + ends(*column[e])
    on_x[0] = on_x[0] + bx
    on_x[C - 1] = on_x[C - 1] + hx
    on_y[0] = on_y[0] + by
    on_y[C - 1] = on_y[C - 1] + hy
    packed = pack_columns(turn, by, hy)
    rows = row_of((C, C))
    on_z = {}
    for z in (0, 1, CZ - 2, CZ - 1) if inner else (0, CZ - 1):
        p = column_plane(packed, z)
        p = p + jnp.where(rows == 0, bx[z : z + 1, :], jnp.where(rows == C - 1, hx[z : z + 1, :], 0.0))
        on_z[z] = p + bz if z == 0 else p + hz if z == CZ - 1 else p
    return on_x, on_y, on_z


def layer_weights(weight, wx, wy):
    return (
        {e: wx[i] for i, e in enumerate(EDGES)},
        {e: wy[i] for i, e in enumerate(EDGES)},
        {z: weight[z] for z in (0, 1, CZ - 2, CZ - 1)},
    )


def face_response(layers, weights):
    out = []
    for layer, w, last in zip(layers, weights, (C - 1, C - 1, CZ - 1)):
        for face, inside in ((0, 1), (last, last - 1)):
            once = w[face] * layer[face]
            near = in_plane(once) + w[inside] * layer[inside]
            out.append(KEPT * once + w[face] * (layer[face] + near))
    return out


def fold(t):
    return jnp.sum(t.reshape(t.shape[0] // 8, 8, C), axis=0)


def layer_energy(a, b, weights):
    rows = row_of((CZ, C))
    lanes = lane_of((CZ, C))
    inner = (rows > 0) & (rows < CZ - 1)
    both = inner & (lanes > 0) & (lanes < C - 1)
    acc = jnp.zeros((8, C), F32)
    for layers_a, layers_b, w, last, mask in zip(a, b, weights, (C - 1, C - 1, CZ - 1), (inner, both, None)):
        for e in (0, last):
            t = layers_a[e] * layers_b[e] * w[e]
            acc = acc + fold(t if mask is None else jnp.where(mask, t, 0.0))
    return jnp.sum(acc) / DAMPING_WEIGHT


def places():
    x, y, z = (lax.axis_index(a) for a in AXES)
    more = [i < lax.axis_size(a) - 1 for a, i in zip(AXES, (x, y, z))]
    less = [i > 0 for i in (x, y, z)]
    return (x % 2 == 0, y % 2 == 0, z == 0), more, less


def pick(flag, a, b):
    return lax.select(jnp.broadcast_to(flag, a.shape), a, b)


def pack_sends(sends, faces, index):
    (xeven, yeven, zlow), _, _ = places()
    xa, xb, ya, yb, zz = sends
    for even, a, b, lo, hi in ((xeven, xa, xb, faces[0], faces[1]), (yeven, ya, yb, faces[2], faces[3])):
        s = slice(index * CZ, (index + 1) * CZ)
        a[s, :] = pick(even, hi, lo)
        b[s, :] = pick(even, lo, hi)
    zz[index * C : (index + 1) * C, :] = pick(zlow, faces[5], faces[4])


def own_faces(src, own, turn):
    row_layer(src, 1, 0, own[0])
    row_layer(src, 1, C - 1, own[1])
    column_layers(src, 1, turn)
    own[2][...] = turn[layer_rows(2), :]
    own[3][...] = turn[layer_rows(1), :]
    own[4][...] = src[1, INNER, :]
    own[5][...] = src[CZ, INNER, :]


def first_kernel(heat_in, cond_in, proj_in, segs_in, weight, state, parts, heat, wx, wy, *refs):
    own = refs[:6]
    sends = refs[6:11]
    cond, proj, segs, start, turn, pack, sems, small = refs[11:]
    tables = (pltpu.make_async_copy(proj_in, proj, small.at[0]), pltpu.make_async_copy(segs_in, segs, small.at[1]))

    def copies(i):
        s = pl.ds(i * DEPTH, DEPTH)
        return (
            pltpu.make_async_copy(cond_in.at[s], cond.at[s], sems.at[0, i]),
            pltpu.make_async_copy(heat_in.at[s], heat.at[s], sems.at[1, i]),
        )

    for c in tables:
        c.start()
    for i in range(PARTS):
        for c in copies(i):
            c.start()
    zero_ends(start)
    zero_ends(state)
    pack[...] = jnp.zeros((C, C), F32)
    group = lane_of((C, C)) // 4

    def part(i, carry):
        for c in copies(i):
            c.wait()
        packed = pack[...]
        for j in range(DEPTH):
            z = i * DEPTH + j
            w = DAMPING_WEIGHT / (6.0 + cond[z])
            weight[z] = w
            start[z + 1, INNER, :] = w * heat[z]
            packed = jnp.where(group == z, pltpu.roll(w, 4 * z + 2, 1), packed)
        pack[...] = packed

        @pl.when(i > 0)
        def _():
            sweep_planes(start, state, weight, heat, (i - 1) * DEPTH, DEPTH, 16)

        return carry

    lax.fori_loop(0, PARTS, part, 0)
    sweep_planes(start, state, weight, heat, CZ - DEPTH, DEPTH, 16)
    for c in tables:
        c.wait()
    for d in range(3):
        onehot = jnp.where(row_of((C, C)) == segs[d], 1.0, 0.0).astype(BF16)
        base = sum(lax.dot_general(onehot, p, (((1,), (1,)), ((), ())), preferred_element_type=F32) for p in reversed(parts_of(proj[d])))
        store_parts(parts, d, base)
        for a in (sends[:2], sends[2:4])[d] if d < 2 else ():
            a[CZ : CZ + C, :] = base
        if d == 2:
            sends[4][C : 2 * C, :] = base
    own_faces(state, own, turn)
    pack_sends(sends, [f[...] for f in own], 0)
    for i, e in enumerate(EDGES):
        row_layer(weight, 0, e, wx.at[i])
    turn[...] = pack[...].T
    for i, e in enumerate((2, 3, 0, 1)):
        wy[i] = turn[layer_rows(e), :]


def free_kernel(state, weight, supply, out, *refs):
    own = refs[:6]
    mid, turn = refs[6:]
    zero_ends(mid)
    zero_ends(out)
    sweep(state, mid, weight, supply)
    sweep(mid, out, weight, supply)
    own_faces(out, own, turn)


def jumps(own, got, bases, prev_bases, back_bases, n, lifted):
    (xeven, yeven, zlow), more, less = places()
    xa, xb, ya, yb, zz = got
    for d, (even, a, b, rows) in enumerate(((xeven, xa, xb, n * CZ), (yeven, ya, yb, n * CZ), (zlow, zz, zz, n * C))):
        a = a[0:rows, :]
        b = b[0:rows, :]
        up = own[2 * d + 1][...] - dot(pick(even, a, b), bases, d)
        up = jnp.where(more[d], up, 0.0)
        down = pick(even, b, a) - dot(own[2 * d][...], prev_bases, d)
        back = jnp.where(less[d], -dot(down, back_bases, d), 0.0)
        size = rows // n
        for i in range(n):
            lifted[i][2 * d][...] = back[i * size : (i + 1) * size, :]
            lifted[i][2 * d + 1][...] = up[i * size : (i + 1) * size, :]


def square_sum(a, b):
    return jnp.sum(sum(fold(a[i][...] * b[i][...]) for i in (1, 3, 5)))


def row_of_sums(values):
    lanes = lane_of((1, C))
    row = jnp.zeros((1, C), F32)
    for i, v in enumerate(values):
        row = jnp.where(lanes == i, v, row)
    return row


def second_kernel(first, *refs):
    it = iter(refs)
    take = lambda n: [next(it) for _ in range(n)]
    own = take(6)
    got = take(5)
    (bases,) = take(1)
    prev, back = take(2) if not first else (None, None)
    weight, wx, wy = take(3)
    own_u = take(6)
    lifted = take(6)
    own_uv = take(6)
    sends = take(5)
    if first:
        prev, back = take(2)
    (turn,) = take(1)
    (xeven, yeven, _), _, _ = places()
    if first:
        xa, xb, ya, yb, zz = got
        for d, base in enumerate((pick(xeven, xb[CZ:, :], xa[CZ:, :]), pick(yeven, yb[CZ:, :], ya[CZ:, :]), zz[C:, :])):
            store_parts(prev, d, base)
            store_parts(back, d, base.T)
    jumps(own, got, bases, prev, back, 1, [lifted])
    response = face_response(lift_layers(lifted, turn, True), layer_weights(weight, wx, wy))
    free = [f[...] for f in own_u]
    for o, u, v in zip(own_uv, free, response):
        n = u.shape[0]
        o[0:n, :] = u
        o[n:, :] = v
    pack_sends(sends, free, 0)
    pack_sends(sends, response, 1)


def response_kernel(*refs):
    lifted = refs[:6]
    low_y, high_y, weight, wx, wy, resp, sums, lift, mid, turn, cols = refs[6:]
    layers = lift_layers(lifted, turn, False)
    sums[...] = row_of_sums([square_sum(lifted, lifted), layer_energy(layers, layers, layer_weights(weight, wx, wy))])
    cols[...] = pack_columns(turn, lifted[2][...], lifted[3][...])
    turn[layer_rows(0), :] = wy[2] * (wy[3] * lifted[3][...])
    turn[layer_rows(1), :] = high_y[CZ:, :]
    turn[layer_rows(2), :] = low_y[CZ:, :]
    turn[layer_rows(3), :] = wy[1] * (wy[0] * lifted[2][...])
    turn[...] = turn[...].T
    zero_ends(mid)
    zero_ends(resp)
    lanes = lane_of((C, C))
    beside = (lanes < 2) | (lanes >= C - 2)

    def plane(z, carry):
        resp[z + 1, INNER, :] = jnp.where(beside, pltpu.roll(turn[...], C - 2 - 4 * z, 1), 0.0)
        return carry

    lax.fori_loop(0, CZ, plane, 0, unroll=WIDE)
    near_x = ((0, 16), (C - 16, C))
    near_z = (0, 1, 2, CZ - 3, CZ - 2, CZ - 1)
    edge = (lanes == 0) | (lanes == C - 1)
    for z in range(CZ):
        for a, b in ((0, C),) if z in near_z else near_x:
            lift[z, a:b, :] = jnp.where(edge[a:b], pltpu.roll(cols[a:b, :], C - 2 - 4 * z, 1), 0.0)
    add_rows(lift, lifted, 1.0)
    for z in range(CZ):
        for a, b in ((0, C),) if z in near_z else near_x:
            mid[z + 1, PAD + a : PAD + b, :] = weight[z, a:b, :] * lift[z, a:b, :]
    sweep_planes(mid, resp, weight, lift, 0, CZ, 8, (0, C - 8))
    for z in (0, CZ - 2):
        sweep_planes(mid, resp, weight, lift, z, 2, 8, range(8, C - 8, 8))


def merge_sides(low, high):
    return [f for pair in zip(low, high) for f in pair]


def third_kernel(*refs):
    it = iter(refs)
    take = lambda n: [next(it) for _ in range(n)]
    own_uv = take(6)
    got = take(5)
    bases, prev, back, weight, wx, wy, before = take(7)
    high_u, high_v = take(3), take(3)
    (rows,) = take(1)
    low_u, low_v = take(3), take(3)
    (turn,) = take(1)
    lift_u = merge_sides(low_u, high_u)
    lift_v = merge_sides(low_v, high_v)
    jumps(own_uv, got, bases, prev, back, 2, [lift_u, lift_v])
    weights = layer_weights(weight, wx, wy)
    u = lift_layers(lift_u, turn.at[0], False)
    v = lift_layers(lift_v, turn.at[1], False)
    sums = [square_sum(lift_u, lift_u), square_sum(lift_u, lift_v), square_sum(lift_v, lift_v)]
    sums += [layer_energy(u, u, weights), layer_energy(u, v, weights), layer_energy(v, v, weights)]
    lanes = lane_of((1, C))
    row = row_of_sums([0.0, 0.0] + sums)
    row = jnp.where(lanes < 2, before[...], row)
    rows[...] = jnp.broadcast_to(row, (C, C))


def steps(totals):
    row = jnp.sum(totals[...], axis=0, keepdims=True)
    lanes = lane_of((1, C))
    gg, gh, guu, guv, gvv, huu, huv, hvv = [jnp.sum(jnp.where(lanes == i, row, 0.0), axis=1, keepdims=True) for i in range(8)]
    one = gg / (gh + EPSILON)
    two = (guu - 2.0 * one * guv + one * one * gvv) / (huu - 2.0 * one * huv + one * one * hvv + EPSILON)
    return one, two


def fourth_kernel(*refs):
    it = iter(refs)
    take = lambda n: [next(it) for _ in range(n)]
    totals, heat, weight, free, resp = take(5)
    lift_1 = take(6)
    lift_u = take(6)
    lift_v = take(6)
    supply, state = take(2)
    high = take(3)
    own = take(6)
    sends = take(5)
    low = take(3)
    mid, turn, cols = take(3)
    held = merge_sides(low, high)
    one, two = steps(totals)
    for i in range(6):
        held[i][...] = one * lift_1[i][...] + two * (lift_u[i][...] - one * lift_v[i][...])
    cols[...] = pack_columns(turn, held[2][...], held[3][...])
    zero_ends(mid)
    zero_ends(state)

    def plane(z, carry):
        supply[z] = heat[z] - column_plane(cols[...], z)
        state[z + 1, INNER, :] = free[z + 1, INNER, :] - one * resp[z + 1, INNER, :]
        return carry

    lax.fori_loop(0, CZ, plane, 0, unroll=WIDE)
    add_rows(supply, held, -1.0)
    sweep(state, mid, weight, supply)
    sweep(mid, state, weight, supply)
    own_faces(state, own, turn)
    pack_sends(sends, [f[...] for f in own], 0)


def last_kernel(*refs):
    it = iter(refs)
    take = lambda n: [next(it) for _ in range(n)]
    totals, free, resp = take(3)
    held = take(3)
    lift_3 = take(3)
    lift_u = take(3)
    lift_v = take(3)
    (out,) = take(1)
    outs = take(3)
    state, sems = take(2)
    one, two = steps(totals)

    def plane(z, carry):
        state[z] = free[z + 1, INNER, :] - one * resp[z + 1, INNER, :]
        return carry

    copies = []
    for i in range(PARTS):
        lax.fori_loop(i * DEPTH, (i + 1) * DEPTH, plane, 0, unroll=UNROLL)
        s = pl.ds(i * DEPTH, DEPTH)
        copies.append(pltpu.make_async_copy(state.at[s], out.at[s], sems.at[i]))
        copies[-1].start()
    for i in range(3):
        outs[i][...] = held[i][...] + one * lift_3[i][...] + two * (lift_u[i][...] - one * lift_v[i][...])
    for c in copies:
        c.wait()


FIELD = jax.ShapeDtypeStruct((CZ, C, C), F32)
PADDED = jax.ShapeDtypeStruct((CZ + 2, C + 2 * PAD, C), F32)
FACE = jax.ShapeDtypeStruct((CZ, C), F32)
SQUARE = jax.ShapeDtypeStruct((C, C), F32)
FACES = [FACE] * 4 + [SQUARE] * 2
LAYERS = jax.ShapeDtypeStruct((4, CZ, C), F32)
ROW = jax.ShapeDtypeStruct((1, C), F32)
SIDE = [FACE, FACE, SQUARE]
S_SIDE = [pltpu.VMEM(f.shape, F32) for f in SIDE]
S_FIELD = pltpu.VMEM((CZ, C, C), F32)
S_PADDED = pltpu.VMEM((CZ + 2, C + 2 * PAD, C), F32)
PIECES = jax.ShapeDtypeStruct((3, C, 3 * C), BF16)
S_SQUARE = pltpu.VMEM((C, C), F32)


def sends_of(n, extra):
    small = jax.ShapeDtypeStruct((n * CZ + extra, C), F32)
    return [small] * 4 + [jax.ShapeDtypeStruct((n * C + extra, C), F32)]


def call(kernel, outs, scratch, args, us, in_specs=None, out_specs=None):
    return list(
        pl.pallas_call(
            kernel,
            out_shape=tuple(outs),
            in_specs=in_specs or [VM] * len(args),
            out_specs=tuple(out_specs or [VM] * len(outs)),
            scratch_shapes=scratch,
            compiler_params=pltpu.CompilerParams(vmem_limit_bytes=20 * 1024 * 1024),
            cost_estimate=pl.CostEstimate(flops=us * 10**7, transcendentals=0, bytes_accessed=2**20),
        )(*args)
    )


def swap_pairs(along, start):
    nx, ny = lax.axis_size("gx"), lax.axis_size("gy")
    place = lambda x, y: x * ny + y
    pairs = []
    for x in range(nx):
        for y in range(ny):
            i, n = (x, nx) if along == "x" else (y, ny)
            j = i + 1 if i % 2 == start else i - 1
            if 0 <= j < n:
                other = place(j, y) if along == "x" else place(x, j)
            else:
                other = place(x, y ^ 1) if along == "x" else place(x ^ 1, y)
            pairs.append((place(x, y), other))
    return pairs


def exchange(sends):
    xa, xb, ya, yb, zz = sends
    both = ("gx", "gy")
    xa = lax.ppermute(xa, both, swap_pairs("x", 0))
    yb = lax.ppermute(yb, both, swap_pairs("y", 1))
    zz = lax.ppermute(zz, "gz", [(0, 1), (1, 0)])
    xb = lax.ppermute(xb, both, swap_pairs("x", 1))
    ya = lax.ppermute(ya, both, swap_pairs("y", 0))
    return [xa, xb, ya, yb, zz]


def gather_rows(rows):
    rows = lax.all_to_all(rows.reshape(C, 1, C), AXES, 0, 0)
    return rows.reshape(C, C)


def body(heat, cond, projection, segment_map):
    proj = projection[0, 0, 0]
    segs = segment_map.reshape(3, 1, C)
    dma = pltpu.SemaphoreType.DMA
    scratch = [S_FIELD, pltpu.VMEM(proj.shape, F32), pltpu.VMEM(segs.shape, jnp.int32), S_PADDED, S_SQUARE, S_SQUARE, dma((2, PARTS)), dma((2,))]
    outs = [FIELD, PADDED, PIECES, FIELD, LAYERS, LAYERS] + FACES + sends_of(1, C)
    out = call(first_kernel, outs, scratch, [pltpu.with_memory_space_constraint(a, pltpu.MemorySpace.HBM) for a in (heat, cond, proj, segs)], 4, [AWAY] * 4)
    weight, state, bases, heat, wx, wy = out[:6]
    own, sends = out[6:12], out[12:]
    supply = heat
    prev = []
    held = None
    for pair in range(2):
        first = pair == 0
        got = exchange(sends)
        out = call(free_kernel, [PADDED] + FACES, [S_PADDED, S_SQUARE], (state, weight, supply), 3)
        free, own_u = out[0], out[1:]
        args = own + got + [bases] + prev + [weight, wx, wy] + own_u
        stacked = [jax.ShapeDtypeStruct((2 * f.shape[0], C), F32) for f in FACES]
        outs = FACES + stacked + sends_of(2, 0) + ([PIECES, PIECES] if first else [])
        out = call(functools.partial(second_kernel, first), outs, [S_SQUARE], args, 2)
        lift_1, own_uv, sends = out[:6], out[6:12], out[12:17]
        if first:
            prev = out[17:]
        got = exchange(sends)
        args = lift_1 + own_uv[2:4] + [weight, wx, wy]
        resp, sums = call(response_kernel, [PADDED, ROW], [S_FIELD, S_PADDED, S_SQUARE, S_SQUARE], args, 3)
        args = own_uv + got + [bases] + prev + [weight, wx, wy, sums]
        outs = SIDE + SIDE + [SQUARE] + (SIDE + SIDE if first else [])
        scratch = ([] if first else S_SIDE + S_SIDE) + [pltpu.VMEM((2, C, C), F32)]
        out = call(third_kernel, outs, scratch, args, 2)
        high_u, high_v, rows = out[:3], out[3:6], out[6]
        totals = gather_rows(rows)
        if first:
            args = [totals, heat, weight, free, resp] + lift_1 + merge_sides(out[7:10], high_u) + merge_sides(out[10:13], high_v)
            outs = [FIELD, PADDED] + SIDE + FACES + sends_of(1, 0)
            out = call(fourth_kernel, outs, S_SIDE + [S_PADDED, S_SQUARE, S_SQUARE], args, 5)
            supply, state, held, own, sends = out[0], out[1], out[2:5], out[5:11], out[11:]
    args = [totals, free, resp] + held + [lift_1[i] for i in (1, 3, 5)] + high_u + high_v
    state, mx, my, mz = call(last_kernel, [FIELD, FACE, FACE, SQUARE], [S_FIELD, dma((PARTS,))], args, 2, None, [AWAY, VM, VM, VM])
    return state, mx[None, None, None], my[None, None, None], mz[None, None, None]


def solution(mesh):
    field = P("gz", "gx", "gy")
    in_specs = (field, field, P("gz", "gx", "gy", None, None, None), P("gz", "gx", "gy", None, None))
    face = P("gz", "gx", "gy", None, None)
    return jax.shard_map(body, mesh=mesh, in_specs=in_specs, out_specs=(field, face, face, face), check_vma=False)
```

```python
import functools

import jax
import jax.numpy as jnp
from jax import lax
from jax.experimental import pallas as pl
from jax.experimental.pallas import tpu as pltpu
from jax.sharding import PartitionSpec as P

DAMPING_WEIGHT = 0.8
EPSILON = 1e-06
AXES = ("gx", "gy", "gz")
CZ = 32
C = 128
F32 = jnp.float32
UNROLL = 4
WIDE = 16
DEPTH = 8
PARTS = CZ // DEPTH
KEPT = 1.0 - DAMPING_WEIGHT

VM = pl.BlockSpec(memory_space=pltpu.MemorySpace.VMEM)
AWAY = pl.BlockSpec(memory_space=pltpu.MemorySpace.HBM)
BF16 = jnp.bfloat16
PAD = 8


def parts_of(a):
    first = a.astype(BF16)
    rest = a - first.astype(F32)
    second = rest.astype(BF16)
    third = (rest - second.astype(F32)).astype(BF16)
    return first, second, third


def dot(a, parts, d):
    n = a.shape[0]
    mul = functools.partial(jnp.dot, preferred_element_type=F32)
    a1, a2, a3 = parts_of(a)
    r = mul(jnp.concatenate([a1, a2, a3], axis=0), parts[d, :, 0 : 2 * C])
    t = mul(a1, parts[d, :, 2 * C :])
    small = r[2 * n :, :C] + r[n : 2 * n, C:] + t
    return r[:n, :C] + (r[n : 2 * n, :C] + r[:n, C:] + small)


def store_parts(ref, d, a):
    for i, p in enumerate(parts_of(a)):
        ref[d, :, i * C : (i + 1) * C] = p


def lane_of(shape):
    return lax.broadcasted_iota(jnp.int32, shape, len(shape) - 1)


def row_of(shape):
    return lax.broadcasted_iota(jnp.int32, shape, len(shape) - 2)


INNER = slice(PAD, PAD + C)


def zero_ends(ref):
    ref[0] = jnp.zeros((C + 2 * PAD, C), F32)
    ref[CZ + 1] = jnp.zeros((C + 2 * PAD, C), F32)
    for z in range(1, CZ + 1):
        ref[z, 0:PAD, :] = jnp.zeros((PAD, C), F32)
        ref[z, PAD + C :, :] = jnp.zeros((PAD, C), F32)


def in_plane(centre):
    shape = centre.shape
    rows = row_of(shape)
    lanes = lane_of(shape)
    near = jnp.where(rows == 0, 0.0, pltpu.roll(centre, 1, 0))
    near = near + jnp.where(rows == shape[0] - 1, 0.0, pltpu.roll(centre, shape[0] - 1, 0))
    near = near + jnp.where(lanes == 0, 0.0, pltpu.roll(centre, 1, 1))
    return near + jnp.where(lanes == C - 1, 0.0, pltpu.roll(centre, C - 1, 1))


def sweep_planes(src, dst, weight, supply, z, depth, block, rows=None):
    lanes = lane_of((block, C))
    low = lanes == 0
    high = lanes == C - 1
    for x in range(0, C, block) if rows is None else rows:
        r = PAD + x
        column = [src[z + j, r : r + block, :] for j in range(depth + 2)]
        for j in range(depth):
            centre = column[j + 1]
            near = column[j] + column[j + 2]
            near = near + src[z + j + 1, r - 1 : r - 1 + block, :] + src[z + j + 1, r + 1 : r + 1 + block, :]
            near = near + jnp.where(low, 0.0, pltpu.roll(centre, 1, 1)) + jnp.where(high, 0.0, pltpu.roll(centre, C - 1, 1))
            dst[z + j + 1, r : r + block, :] = KEPT * centre + weight[z + j, x : x + block, :] * (supply[z + j, x : x + block, :] + near)


def sweep(src, dst, weight, supply):
    sweep_planes(src, dst, weight, supply, 0, CZ, 8)


def row_layer(src, base, at, out):
    for z in range(CZ):
        out[z : z + 1, :] = src[z + base, PAD * base + at : PAD * base + at + 1, :]


def column_layers(src, base, turn):
    group = lane_of((C, C)) // 4

    def plane(z, packed):
        return jnp.where(group == z, pltpu.roll(src[z + base, PAD * base : PAD * base + C, :], 4 * z + 2, 1), packed)

    packed = lax.fori_loop(0, CZ, plane, jnp.zeros((C, C), F32), unroll=CZ)
    turn[...] = packed.T


def layer_rows(i):
    return pl.ds(i, CZ, stride=4)


def pack_columns(turn, low, high):
    turn[...] = jnp.zeros((C, C), F32)
    turn[layer_rows(1), :] = high
    turn[layer_rows(2), :] = low
    return turn[...].T


def column_plane(packed, z):
    lanes = lane_of((C, C))
    edge = (lanes == 0) | (lanes == C - 1)
    return jnp.where(edge, pltpu.roll(packed, C - 2 - 4 * z, 1), 0.0)


def add_rows(dst, faces, sign):
    for z in range(CZ):
        dst[z, 0:1, :] = dst[z, 0:1, :] + sign * faces[0][z : z + 1, :]
        dst[z, C - 1 : C, :] = dst[z, C - 1 : C, :] + sign * faces[1][z : z + 1, :]
    dst[0] = dst[0] + sign * faces[4][...]
    dst[CZ - 1] = dst[CZ - 1] + sign * faces[5][...]


EDGES = (0, 1, C - 2, C - 1)


def rim(low, high, at):
    lanes = lane_of(low.shape)
    a = low if at == 0 else pltpu.roll(low, C - at, 1)
    b = high if at == C - 1 else pltpu.roll(high, C - 1 - at, 1)
    return jnp.where(lanes == 0, a, jnp.where(lanes == C - 1, b, 0.0))


def ends(low, high):
    rows = row_of((CZ, C))
    return jnp.where(rows == 0, low, jnp.where(rows == CZ - 1, high, 0.0))


def lift_layers(faces, turn, inner):
    bx, hx, by, hy, bz, hz = [f[...] for f in faces]
    lanes = lane_of((C, C))
    columns = jnp.where(lanes < 4, pltpu.roll(bz, 2, 1), pltpu.roll(hz, 6, 1)).T
    at = lambda i: columns[i : i + 1, :]
    column = {C - 2: (at(0), at(4)), C - 1: (at(1), at(5)), 0: (at(2), at(6)), 1: (at(3), at(7))}
    edges = EDGES if inner else (0, C - 1)
    on_x = {}
    on_y = {}
    for e in edges:
        on_x[e] = rim(by, hy, e) + ends(bz[e : e + 1, :], hz[e : e + 1, :])
        on_y[e] = rim(bx, hx, e) + ends(*column[e])
    on_x[0] = on_x[0] + bx
    on_x[C - 1] = on_x[C - 1] + hx
    on_y[0] = on_y[0] + by
    on_y[C - 1] = on_y[C - 1] + hy
    packed = pack_columns(turn, by, hy)
    rows = row_of((C, C))
    on_z = {}
    for z in (0, 1, CZ - 2, CZ - 1) if inner else (0, CZ - 1):
        p = column_plane(packed, z)
        p = p + jnp.where(rows == 0, bx[z : z + 1, :], jnp.where(rows == C - 1, hx[z : z + 1, :], 0.0))
        on_z[z] = p + bz if z == 0 else p + hz if z == CZ - 1 else p
    return on_x, on_y, on_z


def layer_weights(weight, wx, wy):
    return (
        {e: wx[i] for i, e in enumerate(EDGES)},
        {e: wy[i] for i, e in enumerate(EDGES)},
        {z: weight[z] for z in (0, 1, CZ - 2, CZ - 1)},
    )


def face_response(layers, weights):
    out = []
    for layer, w, last in zip(layers, weights, (C - 1, C - 1, CZ - 1)):
        for face, inside in ((0, 1), (last, last - 1)):
            once = w[face] * layer[face]
            near = in_plane(once) + w[inside] * layer[inside]
            out.append(KEPT * once + w[face] * (layer[face] + near))
    return out


def fold(t):
    return jnp.sum(t.reshape(t.shape[0] // 8, 8, C), axis=0)


def layer_energy(a, b, weights):
    rows = row_of((CZ, C))
    lanes = lane_of((CZ, C))
    inner = (rows > 0) & (rows < CZ - 1)
    both = inner & (lanes > 0) & (lanes < C - 1)
    acc = jnp.zeros((8, C), F32)
    for layers_a, layers_b, w, last, mask in zip(a, b, weights, (C - 1, C - 1, CZ - 1), (inner, both, None)):
        for e in (0, last):
            t = layers_a[e] * layers_b[e] * w[e]
            acc = acc + fold(t if mask is None else jnp.where(mask, t, 0.0))
    return acc * (1.0 / DAMPING_WEIGHT)


def places():
    x, y, z = (lax.axis_index(a) for a in AXES)
    more = [i < lax.axis_size(a) - 1 for a, i in zip(AXES, (x, y, z))]
    less = [i > 0 for i in (x, y, z)]
    return (x % 2 == 0, y % 2 == 0, z == 0), more, less


def pick(flag, a, b):
    return lax.select(jnp.broadcast_to(flag, a.shape), a, b)


def pack_sends(sends, faces, index):
    (xeven, yeven, zlow), _, _ = places()
    xa, xb, ya, yb, zz = sends
    for even, a, b, lo, hi in ((xeven, xa, xb, faces[0], faces[1]), (yeven, ya, yb, faces[2], faces[3])):
        s = slice(index * CZ, (index + 1) * CZ)
        a[s, :] = pick(even, hi, lo)
        b[s, :] = pick(even, lo, hi)
    zz[index * C : (index + 1) * C, :] = pick(zlow, faces[5], faces[4])


def own_faces(src, own, turn):
    row_layer(src, 1, 0, own[0])
    row_layer(src, 1, C - 1, own[1])
    column_layers(src, 1, turn)
    own[2][...] = turn[layer_rows(2), :]
    own[3][...] = turn[layer_rows(1), :]
    own[4][...] = src[1, INNER, :]
    own[5][...] = src[CZ, INNER, :]


def first_kernel(heat_in, cond_in, proj_in, segs_in, weight, state, parts, heat, wx, wy, *refs):
    own = refs[:6]
    sends = refs[6:11]
    cond, proj, segs, start, turn, pack, sems, small = refs[11:]
    tables = (pltpu.make_async_copy(proj_in, proj, small.at[0]), pltpu.make_async_copy(segs_in, segs, small.at[1]))

    def copies(i):
        s = pl.ds(i * DEPTH, DEPTH)
        return (
            pltpu.make_async_copy(cond_in.at[s], cond.at[s], sems.at[0, i]),
            pltpu.make_async_copy(heat_in.at[s], heat.at[s], sems.at[1, i]),
        )

    for c in tables:
        c.start()
    for i in range(PARTS):
        for c in copies(i):
            c.start()
    zero_ends(start)
    zero_ends(state)
    pack[...] = jnp.zeros((C, C), F32)
    group = lane_of((C, C)) // 4

    def part(i, carry):
        for c in copies(i):
            c.wait()
        packed = pack[...]
        for j in range(DEPTH):
            z = i * DEPTH + j
            w = DAMPING_WEIGHT / (6.0 + cond[z])
            weight[z] = w
            start[z + 1, INNER, :] = w * heat[z]
            packed = jnp.where(group == z, pltpu.roll(w, 4 * z + 2, 1), packed)
        pack[...] = packed

        @pl.when(i > 0)
        def _():
            sweep_planes(start, state, weight, heat, (i - 1) * DEPTH, DEPTH, 16)

        return carry

    lax.fori_loop(0, PARTS, part, 0)
    sweep_planes(start, state, weight, heat, CZ - DEPTH, DEPTH, 16)
    for c in tables:
        c.wait()
    for d in range(3):
        onehot = jnp.where(row_of((C, C)) == segs[d], 1.0, 0.0).astype(BF16)
        base = sum(lax.dot_general(onehot, p, (((1,), (1,)), ((), ())), preferred_element_type=F32) for p in reversed(parts_of(proj[d])))
        store_parts(parts, d, base)
        for a in (sends[:2], sends[2:4])[d] if d < 2 else ():
            a[CZ : CZ + C, :] = base
        if d == 2:
            sends[4][C : 2 * C, :] = base
    own_faces(state, own, turn)
    pack_sends(sends, [f[...] for f in own], 0)
    for i, e in enumerate(EDGES):
        row_layer(weight, 0, e, wx.at[i])
    turn[...] = pack[...].T
    for i, e in enumerate((2, 3, 0, 1)):
        wy[i] = turn[layer_rows(e), :]


def free_kernel(state, weight, supply, out, *refs):
    own = refs[:6]
    mid, turn = refs[6:]
    zero_ends(mid)
    zero_ends(out)
    sweep(state, mid, weight, supply)
    sweep(mid, out, weight, supply)
    own_faces(out, own, turn)


def jumps(own, got, bases, prev_bases, back_bases, n, lifted):
    (xeven, yeven, zlow), more, less = places()
    xa, xb, ya, yb, zz = got
    for d, (even, a, b, rows) in enumerate(((xeven, xa, xb, n * CZ), (yeven, ya, yb, n * CZ), (zlow, zz, zz, n * C))):
        a = a[0:rows, :]
        b = b[0:rows, :]
        up = own[2 * d + 1][...] - dot(pick(even, a, b), bases, d)
        up = jnp.where(more[d], up, 0.0)
        down = pick(even, b, a) - dot(own[2 * d][...], prev_bases, d)
        back = jnp.where(less[d], -dot(down, back_bases, d), 0.0)
        size = rows // n
        for i in range(n):
            lifted[i][2 * d][...] = back[i * size : (i + 1) * size, :]
            lifted[i][2 * d + 1][...] = up[i * size : (i + 1) * size, :]


def square_sum(a, b):
    return sum(fold(a[i][...] * b[i][...]) for i in (1, 3, 5))


def row_of_sums(partials, base):
    rows = row_of((8, C))
    stacked = jnp.zeros((8, C), F32)
    for i, p in enumerate(partials):
        stacked = jnp.where(rows == base + i, jnp.sum(p, axis=0, keepdims=True), stacked)
    totals = jnp.sum(stacked, axis=1, keepdims=True)
    return jnp.sum(jnp.where(lane_of((8, C)) == rows, totals, 0.0), axis=0, keepdims=True)


def second_kernel(first, *refs):
    it = iter(refs)
    take = lambda n: [next(it) for _ in range(n)]
    own = take(6)
    got = take(5)
    (bases,) = take(1)
    prev, back = take(2) if not first else (None, None)
    weight, wx, wy = take(3)
    own_u = take(6)
    lifted = take(6)
    own_uv = take(6)
    sends = take(5)
    if first:
        prev, back = take(2)
    (turn,) = take(1)
    (xeven, yeven, _), _, _ = places()
    if first:
        xa, xb, ya, yb, zz = got
        for d, base in enumerate((pick(xeven, xb[CZ:, :], xa[CZ:, :]), pick(yeven, yb[CZ:, :], ya[CZ:, :]), zz[C:, :])):
            store_parts(prev, d, base)
            store_parts(back, d, base.T)
    jumps(own, got, bases, prev, back, 1, [lifted])
    response = face_response(lift_layers(lifted, turn, True), layer_weights(weight, wx, wy))
    free = [f[...] for f in own_u]
    for o, u, v in zip(own_uv, free, response):
        n = u.shape[0]
        o[0:n, :] = u
        o[n:, :] = v
    pack_sends(sends, free, 0)
    pack_sends(sends, response, 1)


def response_kernel(*refs):
    lifted = refs[:6]
    low_y, high_y, weight, wx, wy, resp, sums, lift, mid, turn, cols = refs[6:]
    layers = lift_layers(lifted, turn, False)
    sums[...] = row_of_sums([square_sum(lifted, lifted), layer_energy(layers, layers, layer_weights(weight, wx, wy))], 0)
    cols[...] = pack_columns(turn, lifted[2][...], lifted[3][...])
    turn[layer_rows(0), :] = wy[2] * (wy[3] * lifted[3][...])
    turn[layer_rows(1), :] = high_y[CZ:, :]
    turn[layer_rows(2), :] = low_y[CZ:, :]
    turn[layer_rows(3), :] = wy[1] * (wy[0] * lifted[2][...])
    turn[...] = turn[...].T
    zero_ends(mid)
    zero_ends(resp)
    lanes = lane_of((C, C))
    beside = (lanes < 2) | (lanes >= C - 2)

    def plane(z, carry):
        resp[z + 1, INNER, :] = jnp.where(beside, pltpu.roll(turn[...], C - 2 - 4 * z, 1), 0.0)
        return carry

    lax.fori_loop(0, CZ, plane, 0, unroll=WIDE)
    near_x = ((0, 16), (C - 16, C))
    near_z = (0, 1, 2, CZ - 3, CZ - 2, CZ - 1)
    edge = (lanes == 0) | (lanes == C - 1)
    for z in range(CZ):
        for a, b in ((0, C),) if z in near_z else near_x:
            lift[z, a:b, :] = jnp.where(edge[a:b], pltpu.roll(cols[a:b, :], C - 2 - 4 * z, 1), 0.0)
    add_rows(lift, lifted, 1.0)
    for z in range(CZ):
        for a, b in ((0, C),) if z in near_z else near_x:
            mid[z + 1, PAD + a : PAD + b, :] = weight[z, a:b, :] * lift[z, a:b, :]
    sweep_planes(mid, resp, weight, lift, 0, CZ, 8, (0, C - 8))
    for z in (0, CZ - 2):
        sweep_planes(mid, resp, weight, lift, z, 2, 8, range(8, C - 8, 8))


def merge_sides(low, high):
    return [f for pair in zip(low, high) for f in pair]


def third_kernel(*refs):
    it = iter(refs)
    take = lambda n: [next(it) for _ in range(n)]
    own_uv = take(6)
    got = take(5)
    bases, prev, back, weight, wx, wy, before = take(7)
    high_u, high_v = take(3), take(3)
    (rows,) = take(1)
    low_u, low_v = take(3), take(3)
    (turn,) = take(1)
    lift_u = merge_sides(low_u, high_u)
    lift_v = merge_sides(low_v, high_v)
    jumps(own_uv, got, bases, prev, back, 2, [lift_u, lift_v])
    weights = layer_weights(weight, wx, wy)
    u = lift_layers(lift_u, turn.at[0], False)
    v = lift_layers(lift_v, turn.at[1], False)
    sums = [square_sum(lift_u, lift_u), square_sum(lift_u, lift_v), square_sum(lift_v, lift_v)]
    sums += [layer_energy(u, u, weights), layer_energy(u, v, weights), layer_energy(v, v, weights)]
    rows[...] = jnp.broadcast_to(before[...] + row_of_sums(sums, 2), (C, C))


def steps(totals):
    row = jnp.sum(totals[...], axis=0, keepdims=True)
    lanes = lane_of((1, C))
    gg, gh, guu, guv, gvv, huu, huv, hvv = [jnp.sum(jnp.where(lanes == i, row, 0.0), axis=1, keepdims=True) for i in range(8)]
    one = gg / (gh + EPSILON)
    two = (guu - 2.0 * one * guv + one * one * gvv) / (huu - 2.0 * one * huv + one * one * hvv + EPSILON)
    return one, two


def fourth_kernel(*refs):
    it = iter(refs)
    take = lambda n: [next(it) for _ in range(n)]
    totals, heat, weight, free, resp = take(5)
    lift_1 = take(6)
    lift_u = take(6)
    lift_v = take(6)
    supply, state = take(2)
    high = take(3)
    own = take(6)
    sends = take(5)
    low = take(3)
    mid, turn, cols = take(3)
    held = merge_sides(low, high)
    one, two = steps(totals)
    for i in range(6):
        held[i][...] = one * lift_1[i][...] + two * (lift_u[i][...] - one * lift_v[i][...])
    cols[...] = pack_columns(turn, held[2][...], held[3][...])
    zero_ends(mid)
    zero_ends(state)

    def plane(z, carry):
        supply[z] = heat[z] - column_plane(cols[...], z)
        state[z + 1, INNER, :] = free[z + 1, INNER, :] - one * resp[z + 1, INNER, :]
        return carry

    lax.fori_loop(0, CZ, plane, 0, unroll=WIDE)
    add_rows(supply, held, -1.0)
    sweep(state, mid, weight, supply)
    sweep(mid, state, weight, supply)
    own_faces(state, own, turn)
    pack_sends(sends, [f[...] for f in own], 0)


def last_kernel(*refs):
    it = iter(refs)
    take = lambda n: [next(it) for _ in range(n)]
    totals, free, resp = take(3)
    held = take(3)
    lift_3 = take(3)
    lift_u = take(3)
    lift_v = take(3)
    (out,) = take(1)
    outs = take(3)
    state, sems = take(2)
    one, two = steps(totals)

    def plane(z, carry):
        state[z] = free[z + 1, INNER, :] - one * resp[z + 1, INNER, :]
        return carry

    copies = []
    for i in range(PARTS):
        lax.fori_loop(i * DEPTH, (i + 1) * DEPTH, plane, 0, unroll=UNROLL)
        s = pl.ds(i * DEPTH, DEPTH)
        copies.append(pltpu.make_async_copy(state.at[s], out.at[s], sems.at[i]))
        copies[-1].start()
    for i in range(3):
        outs[i][...] = held[i][...] + one * lift_3[i][...] + two * (lift_u[i][...] - one * lift_v[i][...])
    for c in copies:
        c.wait()


FIELD = jax.ShapeDtypeStruct((CZ, C, C), F32)
PADDED = jax.ShapeDtypeStruct((CZ + 2, C + 2 * PAD, C), F32)
FACE = jax.ShapeDtypeStruct((CZ, C), F32)
SQUARE = jax.ShapeDtypeStruct((C, C), F32)
FACES = [FACE] * 4 + [SQUARE] * 2
LAYERS = jax.ShapeDtypeStruct((4, CZ, C), F32)
ROW = jax.ShapeDtypeStruct((1, C), F32)
SIDE = [FACE, FACE, SQUARE]
S_SIDE = [pltpu.VMEM(f.shape, F32) for f in SIDE]
S_FIELD = pltpu.VMEM((CZ, C, C), F32)
S_PADDED = pltpu.VMEM((CZ + 2, C + 2 * PAD, C), F32)
PIECES = jax.ShapeDtypeStruct((3, C, 3 * C), BF16)
S_SQUARE = pltpu.VMEM((C, C), F32)


def sends_of(n, extra):
    small = jax.ShapeDtypeStruct((n * CZ + extra, C), F32)
    return [small] * 4 + [jax.ShapeDtypeStruct((n * C + extra, C), F32)]


def call(kernel, outs, scratch, args, us, in_specs=None, out_specs=None):
    return list(
        pl.pallas_call(
            kernel,
            out_shape=tuple(outs),
            in_specs=in_specs or [VM] * len(args),
            out_specs=tuple(out_specs or [VM] * len(outs)),
            scratch_shapes=scratch,
            compiler_params=pltpu.CompilerParams(vmem_limit_bytes=20 * 1024 * 1024),
            cost_estimate=pl.CostEstimate(flops=us * 10**7, transcendentals=0, bytes_accessed=2**20),
        )(*args)
    )


def swap_pairs(along, start):
    nx, ny = lax.axis_size("gx"), lax.axis_size("gy")
    place = lambda x, y: x * ny + y
    pairs = []
    for x in range(nx):
        for y in range(ny):
            i, n = (x, nx) if along == "x" else (y, ny)
            j = i + 1 if i % 2 == start else i - 1
            if 0 <= j < n:
                other = place(j, y) if along == "x" else place(x, j)
            else:
                other = place(x, y ^ 1) if along == "x" else place(x ^ 1, y)
            pairs.append((place(x, y), other))
    return pairs


def exchange(sends):
    xa, xb, ya, yb, zz = sends
    both = ("gx", "gy")
    xa = lax.ppermute(xa, both, swap_pairs("x", 0))
    yb = lax.ppermute(yb, both, swap_pairs("y", 1))
    zz = lax.ppermute(zz, "gz", [(0, 1), (1, 0)])
    xb = lax.ppermute(xb, both, swap_pairs("x", 1))
    ya = lax.ppermute(ya, both, swap_pairs("y", 0))
    return [xa, xb, ya, yb, zz]


def gather_rows(rows):
    rows = lax.all_to_all(rows.reshape(C, 1, C), AXES, 0, 0)
    return rows.reshape(C, C)


def body(heat, cond, projection, segment_map):
    proj = projection[0, 0, 0]
    segs = segment_map.reshape(3, 1, C)
    dma = pltpu.SemaphoreType.DMA
    scratch = [S_FIELD, pltpu.VMEM(proj.shape, F32), pltpu.VMEM(segs.shape, jnp.int32), S_PADDED, S_SQUARE, S_SQUARE, dma((2, PARTS)), dma((2,))]
    outs = [FIELD, PADDED, PIECES, FIELD, LAYERS, LAYERS] + FACES + sends_of(1, C)
    out = call(first_kernel, outs, scratch, [pltpu.with_memory_space_constraint(a, pltpu.MemorySpace.HBM) for a in (heat, cond, proj, segs)], 4, [AWAY] * 4)
    weight, state, bases, heat, wx, wy = out[:6]
    own, sends = out[6:12], out[12:]
    supply = heat
    prev = []
    held = None
    for pair in range(2):
        first = pair == 0
        got = exchange(sends)
        out = call(free_kernel, [PADDED] + FACES, [S_PADDED, S_SQUARE], (state, weight, supply), 3)
        free, own_u = out[0], out[1:]
        args = own + got + [bases] + prev + [weight, wx, wy] + own_u
        stacked = [jax.ShapeDtypeStruct((2 * f.shape[0], C), F32) for f in FACES]
        outs = FACES + stacked + sends_of(2, 0) + ([PIECES, PIECES] if first else [])
        out = call(functools.partial(second_kernel, first), outs, [S_SQUARE], args, 2)
        lift_1, own_uv, sends = out[:6], out[6:12], out[12:17]
        if first:
            prev = out[17:]
        got = exchange(sends)
        args = lift_1 + own_uv[2:4] + [weight, wx, wy]
        resp, sums = call(response_kernel, [PADDED, ROW], [S_FIELD, S_PADDED, S_SQUARE, S_SQUARE], args, 3)
        args = own_uv + got + [bases] + prev + [weight, wx, wy, sums]
        outs = SIDE + SIDE + [SQUARE] + (SIDE + SIDE if first else [])
        scratch = ([] if first else S_SIDE + S_SIDE) + [pltpu.VMEM((2, C, C), F32)]
        out = call(third_kernel, outs, scratch, args, 2)
        high_u, high_v, rows = out[:3], out[3:6], out[6]
        totals = gather_rows(rows)
        if first:
            args = [totals, heat, weight, free, resp] + lift_1 + merge_sides(out[7:10], high_u) + merge_sides(out[10:13], high_v)
            outs = [FIELD, PADDED] + SIDE + FACES + sends_of(1, 0)
            out = call(fourth_kernel, outs, S_SIDE + [S_PADDED, S_SQUARE, S_SQUARE], args, 5)
            supply, state, held, own, sends = out[0], out[1], out[2:5], out[5:11], out[11:]
    args = [totals, free, resp] + held + [lift_1[i] for i in (1, 3, 5)] + high_u + high_v
    state, mx, my, mz = call(last_kernel, [FIELD, FACE, FACE, SQUARE], [S_FIELD, dma((PARTS,))], args, 2, None, [AWAY, VM, VM, VM])
    return state, mx[None, None, None], my[None, None, None], mz[None, None, None]


def solution(mesh):
    field = P("gz", "gx", "gy")
    in_specs = (field, field, P("gz", "gx", "gy", None, None, None), P("gz", "gx", "gy", None, None))
    face = P("gz", "gx", "gy", None, None)
    return jax.shard_map(body, mesh=mesh, in_specs=in_specs, out_specs=(field, face, face, face), check_vma=False)
```

```python
import functools

import jax
import jax.numpy as jnp
from jax import lax
from jax.experimental import pallas as pl
from jax.experimental.pallas import tpu as pltpu
from jax.sharding import PartitionSpec as P

DAMPING_WEIGHT = 0.8
EPSILON = 1e-06
AXES = ("gx", "gy", "gz")
CZ = 32
C = 128
F32 = jnp.float32
UNROLL = 4
WIDE = 16
DEPTH = 8
PARTS = CZ // DEPTH
KEPT = 1.0 - DAMPING_WEIGHT

VM = pl.BlockSpec(memory_space=pltpu.MemorySpace.VMEM)
AWAY = pl.BlockSpec(memory_space=pltpu.MemorySpace.HBM)
BF16 = jnp.bfloat16
PAD = 8


def parts_of(a, count):
    parts = []
    for _ in range(count):
        parts.append(a.astype(BF16))
        a = a - parts[-1].astype(F32)
    return parts


def dot(a, parts, d):
    n = a.shape[0]
    r = jnp.dot(jnp.concatenate(parts_of(a, 2), axis=0), parts[d], preferred_element_type=F32)
    return r[:n, :C] + (r[n:, :C] + r[:n, C:] + r[n:, C:])


def store_parts(ref, d, a):
    for i, p in enumerate(parts_of(a, 2)):
        ref[d, :, i * C : (i + 1) * C] = p


def lane_of(shape):
    return lax.broadcasted_iota(jnp.int32, shape, len(shape) - 1)


def row_of(shape):
    return lax.broadcasted_iota(jnp.int32, shape, len(shape) - 2)


INNER = slice(PAD, PAD + C)


def zero_ends(ref):
    ref[0] = jnp.zeros((C + 2 * PAD, C), F32)
    ref[CZ + 1] = jnp.zeros((C + 2 * PAD, C), F32)
    for z in range(1, CZ + 1):
        ref[z, 0:PAD, :] = jnp.zeros((PAD, C), F32)
        ref[z, PAD + C :, :] = jnp.zeros((PAD, C), F32)


def in_plane(centre):
    shape = centre.shape
    rows = row_of(shape)
    lanes = lane_of(shape)
    near = jnp.where(rows == 0, 0.0, pltpu.roll(centre, 1, 0))
    near = near + jnp.where(rows == shape[0] - 1, 0.0, pltpu.roll(centre, shape[0] - 1, 0))
    near = near + jnp.where(lanes == 0, 0.0, pltpu.roll(centre, 1, 1))
    return near + jnp.where(lanes == C - 1, 0.0, pltpu.roll(centre, C - 1, 1))


def sweep_planes(src, dst, weight, supply, z, depth, block, rows=None):
    lanes = lane_of((block, C))
    low = lanes == 0
    high = lanes == C - 1
    for x in range(0, C, block) if rows is None else rows:
        r = PAD + x
        column = [src[z + j, r : r + block, :] for j in range(depth + 2)]
        for j in range(depth):
            centre = column[j + 1]
            near = column[j] + column[j + 2]
            near = near + src[z + j + 1, r - 1 : r - 1 + block, :] + src[z + j + 1, r + 1 : r + 1 + block, :]
            near = near + jnp.where(low, 0.0, pltpu.roll(centre, 1, 1)) + jnp.where(high, 0.0, pltpu.roll(centre, C - 1, 1))
            dst[z + j + 1, r : r + block, :] = KEPT * centre + weight[z + j, x : x + block, :] * (supply[z + j, x : x + block, :] + near)


def sweep(src, dst, weight, supply):
    sweep_planes(src, dst, weight, supply, 0, CZ, 8)


def row_layer(src, base, at, out):
    for z in range(CZ):
        out[z : z + 1, :] = src[z + base, PAD * base + at : PAD * base + at + 1, :]


def column_layers(src, base, turn):
    group = lane_of((C, C)) // 4

    def plane(z, packed):
        return jnp.where(group == z, pltpu.roll(src[z + base, PAD * base : PAD * base + C, :], 4 * z + 2, 1), packed)

    packed = lax.fori_loop(0, CZ, plane, jnp.zeros((C, C), F32), unroll=CZ)
    turn[...] = packed.T


def layer_rows(i):
    return pl.ds(i, CZ, stride=4)


def pack_columns(turn, low, high):
    turn[...] = jnp.zeros((C, C), F32)
    turn[layer_rows(1), :] = high
    turn[layer_rows(2), :] = low
    return turn[...].T


def column_plane(packed, z):
    lanes = lane_of((C, C))
    edge = (lanes == 0) | (lanes == C - 1)
    return jnp.where(edge, pltpu.roll(packed, C - 2 - 4 * z, 1), 0.0)


def add_rows(dst, faces, sign):
    for z in range(CZ):
        dst[z, 0:1, :] = dst[z, 0:1, :] + sign * faces[0][z : z + 1, :]
        dst[z, C - 1 : C, :] = dst[z, C - 1 : C, :] + sign * faces[1][z : z + 1, :]
    dst[0] = dst[0] + sign * faces[4][...]
    dst[CZ - 1] = dst[CZ - 1] + sign * faces[5][...]


EDGES = (0, 1, C - 2, C - 1)


def rim(low, high, at):
    lanes = lane_of(low.shape)
    a = low if at == 0 else pltpu.roll(low, C - at, 1)
    b = high if at == C - 1 else pltpu.roll(high, C - 1 - at, 1)
    return jnp.where(lanes == 0, a, jnp.where(lanes == C - 1, b, 0.0))


def ends(low, high):
    rows = row_of((CZ, C))
    return jnp.where(rows == 0, low, jnp.where(rows == CZ - 1, high, 0.0))


def lift_layers(faces, turn, inner):
    bx, hx, by, hy, bz, hz = [f[...] for f in faces]
    lanes = lane_of((C, C))
    columns = jnp.where(lanes < 4, pltpu.roll(bz, 2, 1), pltpu.roll(hz, 6, 1)).T
    at = lambda i: columns[i : i + 1, :]
    column = {C - 2: (at(0), at(4)), C - 1: (at(1), at(5)), 0: (at(2), at(6)), 1: (at(3), at(7))}
    edges = EDGES if inner else (0, C - 1)
    on_x = {}
    on_y = {}
    for e in edges:
        on_x[e] = rim(by, hy, e) + ends(bz[e : e + 1, :], hz[e : e + 1, :])
        on_y[e] = rim(bx, hx, e) + ends(*column[e])
    on_x[0] = on_x[0] + bx
    on_x[C - 1] = on_x[C - 1] + hx
    on_y[0] = on_y[0] + by
    on_y[C - 1] = on_y[C - 1] + hy
    packed = pack_columns(turn, by, hy)
    rows = row_of((C, C))
    on_z = {}
    for z in (0, 1, CZ - 2, CZ - 1) if inner else (0, CZ - 1):
        p = column_plane(packed, z)
        p = p + jnp.where(rows == 0, bx[z : z + 1, :], jnp.where(rows == C - 1, hx[z : z + 1, :], 0.0))
        on_z[z] = p + bz if z == 0 else p + hz if z == CZ - 1 else p
    return on_x, on_y, on_z


def layer_weights(weight, wx, wy):
    return (
        {e: wx[i] for i, e in enumerate(EDGES)},
        {e: wy[i] for i, e in enumerate(EDGES)},
        {z: weight[z] for z in (0, 1, CZ - 2, CZ - 1)},
    )


def face_response(layers, weights):
    out = []
    for layer, w, last in zip(layers, weights, (C - 1, C - 1, CZ - 1)):
        for face, inside in ((0, 1), (last, last - 1)):
            once = w[face] * layer[face]
            near = in_plane(once) + w[inside] * layer[inside]
            out.append(KEPT * once + w[face] * (layer[face] + near))
    return out


def fold(t):
    return jnp.sum(t.reshape(t.shape[0] // 8, 8, C), axis=0)


def layer_energy(a, b, weights):
    rows = row_of((CZ, C))
    lanes = lane_of((CZ, C))
    inner = (rows > 0) & (rows < CZ - 1)
    both = inner & (lanes > 0) & (lanes < C - 1)
    acc = jnp.zeros((8, C), F32)
    for layers_a, layers_b, w, last, mask in zip(a, b, weights, (C - 1, C - 1, CZ - 1), (inner, both, None)):
        for e in (0, last):
            t = layers_a[e] * layers_b[e] * w[e]
            acc = acc + fold(t if mask is None else jnp.where(mask, t, 0.0))
    return acc * (1.0 / DAMPING_WEIGHT)


def places():
    x, y, z = (lax.axis_index(a) for a in AXES)
    more = [i < lax.axis_size(a) - 1 for a, i in zip(AXES, (x, y, z))]
    less = [i > 0 for i in (x, y, z)]
    return (x % 2 == 0, y % 2 == 0, z == 0), more, less


def pick(flag, a, b):
    return lax.select(jnp.broadcast_to(flag, a.shape), a, b)


def pack_sends(sends, faces, index):
    (xeven, yeven, zlow), _, _ = places()
    xa, xb, ya, yb, zz = sends
    for even, a, b, lo, hi in ((xeven, xa, xb, faces[0], faces[1]), (yeven, ya, yb, faces[2], faces[3])):
        s = slice(index * CZ, (index + 1) * CZ)
        a[s, :] = pick(even, hi, lo)
        b[s, :] = pick(even, lo, hi)
    zz[index * C : (index + 1) * C, :] = pick(zlow, faces[5], faces[4])


def own_faces(src, own, turn):
    row_layer(src, 1, 0, own[0])
    row_layer(src, 1, C - 1, own[1])
    column_layers(src, 1, turn)
    own[2][...] = turn[layer_rows(2), :]
    own[3][...] = turn[layer_rows(1), :]
    own[4][...] = src[1, INNER, :]
    own[5][...] = src[CZ, INNER, :]


def first_kernel(heat_in, cond_in, proj_in, segs_in, weight, state, parts, heat, wx, wy, *refs):
    own = refs[:6]
    sends = refs[6:11]
    cond, proj, segs, start, turn, pack, sems, small = refs[11:]
    tables = (pltpu.make_async_copy(proj_in, proj, small.at[0]), pltpu.make_async_copy(segs_in, segs, small.at[1]))

    def copies(i):
        s = pl.ds(i * DEPTH, DEPTH)
        return (
            pltpu.make_async_copy(cond_in.at[s], cond.at[s], sems.at[0, i]),
            pltpu.make_async_copy(heat_in.at[s], heat.at[s], sems.at[1, i]),
        )

    for c in tables:
        c.start()
    for i in range(PARTS):
        for c in copies(i):
            c.start()
    zero_ends(start)
    zero_ends(state)
    pack[...] = jnp.zeros((C, C), F32)
    group = lane_of((C, C)) // 4

    def part(i, carry):
        for c in copies(i):
            c.wait()
        packed = pack[...]
        for j in range(DEPTH):
            z = i * DEPTH + j
            w = DAMPING_WEIGHT / (6.0 + cond[z])
            weight[z] = w
            start[z + 1, INNER, :] = w * heat[z]
            packed = jnp.where(group == z, pltpu.roll(w, 4 * z + 2, 1), packed)
        pack[...] = packed

        @pl.when(i > 0)
        def _():
            sweep_planes(start, state, weight, heat, (i - 1) * DEPTH, DEPTH, 16)

        return carry

    lax.fori_loop(0, PARTS, part, 0)
    sweep_planes(start, state, weight, heat, CZ - DEPTH, DEPTH, 16)
    for c in tables:
        c.wait()
    for d in range(3):
        onehot = jnp.where(row_of((C, C)) == segs[d], 1.0, 0.0).astype(BF16)
        base = sum(lax.dot_general(onehot, p, (((1,), (1,)), ((), ())), preferred_element_type=F32) for p in reversed(parts_of(proj[d], 3)))
        store_parts(parts, d, base)
        for a in (sends[:2], sends[2:4])[d] if d < 2 else ():
            a[CZ : CZ + C, :] = base
        if d == 2:
            sends[4][C : 2 * C, :] = base
    own_faces(state, own, turn)
    pack_sends(sends, [f[...] for f in own], 0)
    for i, e in enumerate(EDGES):
        row_layer(weight, 0, e, wx.at[i])
    turn[...] = pack[...].T
    for i, e in enumerate((2, 3, 0, 1)):
        wy[i] = turn[layer_rows(e), :]


def free_kernel(state, weight, supply, out, *refs):
    own = refs[:6]
    mid, turn = refs[6:]
    zero_ends(mid)
    zero_ends(out)
    sweep(state, mid, weight, supply)
    sweep(mid, out, weight, supply)
    own_faces(out, own, turn)


def jumps(own, got, bases, prev_bases, back_bases, n, lifted):
    (xeven, yeven, zlow), more, less = places()
    xa, xb, ya, yb, zz = got
    for d, (even, a, b, rows) in enumerate(((xeven, xa, xb, n * CZ), (yeven, ya, yb, n * CZ), (zlow, zz, zz, n * C))):
        a = a[0:rows, :]
        b = b[0:rows, :]
        up = own[2 * d + 1][...] - dot(pick(even, a, b), bases, d)
        up = jnp.where(more[d], up, 0.0)
        down = pick(even, b, a) - dot(own[2 * d][...], prev_bases, d)
        back = jnp.where(less[d], -dot(down, back_bases, d), 0.0)
        size = rows // n
        for i in range(n):
            lifted[i][2 * d][...] = back[i * size : (i + 1) * size, :]
            lifted[i][2 * d + 1][...] = up[i * size : (i + 1) * size, :]


def square_sum(a, b):
    return sum(fold(a[i][...] * b[i][...]) for i in (1, 3, 5))


def row_of_sums(partials, base):
    rows = row_of((8, C))
    stacked = jnp.zeros((8, C), F32)
    for i, p in enumerate(partials):
        stacked = jnp.where(rows == base + i, jnp.sum(p, axis=0, keepdims=True), stacked)
    totals = jnp.sum(stacked, axis=1, keepdims=True)
    return jnp.sum(jnp.where(lane_of((8, C)) == rows, totals, 0.0), axis=0, keepdims=True)


def second_kernel(first, *refs):
    it = iter(refs)
    take = lambda n: [next(it) for _ in range(n)]
    own = take(6)
    got = take(5)
    (bases,) = take(1)
    prev, back = take(2) if not first else (None, None)
    weight, wx, wy = take(3)
    own_u = take(6)
    lifted = take(6)
    own_uv = take(6)
    sends = take(5)
    if first:
        prev, back = take(2)
    (turn,) = take(1)
    (xeven, yeven, _), _, _ = places()
    if first:
        xa, xb, ya, yb, zz = got
        for d, base in enumerate((pick(xeven, xb[CZ:, :], xa[CZ:, :]), pick(yeven, yb[CZ:, :], ya[CZ:, :]), zz[C:, :])):
            store_parts(prev, d, base)
            store_parts(back, d, base.T)
    jumps(own, got, bases, prev, back, 1, [lifted])
    response = face_response(lift_layers(lifted, turn, True), layer_weights(weight, wx, wy))
    free = [f[...] for f in own_u]
    for o, u, v in zip(own_uv, free, response):
        n = u.shape[0]
        o[0:n, :] = u
        o[n:, :] = v
    pack_sends(sends, free, 0)
    pack_sends(sends, response, 1)


def response_kernel(*refs):
    lifted = refs[:6]
    low_y, high_y, weight, wx, wy, resp, sums, lift, mid, turn, cols = refs[6:]
    layers = lift_layers(lifted, turn, False)
    sums[...] = row_of_sums([square_sum(lifted, lifted), layer_energy(layers, layers, layer_weights(weight, wx, wy))], 0)
    cols[...] = pack_columns(turn, lifted[2][...], lifted[3][...])
    turn[layer_rows(0), :] = wy[2] * (wy[3] * lifted[3][...])
    turn[layer_rows(1), :] = high_y[CZ:, :]
    turn[layer_rows(2), :] = low_y[CZ:, :]
    turn[layer_rows(3), :] = wy[1] * (wy[0] * lifted[2][...])
    turn[...] = turn[...].T
    zero_ends(mid)
    zero_ends(resp)
    lanes = lane_of((C, C))
    beside = (lanes < 2) | (lanes >= C - 2)

    def plane(z, carry):
        resp[z + 1, INNER, :] = jnp.where(beside, pltpu.roll(turn[...], C - 2 - 4 * z, 1), 0.0)
        return carry

    lax.fori_loop(0, CZ, plane, 0, unroll=WIDE)
    near_x = ((0, 16), (C - 16, C))
    near_z = (0, 1, 2, CZ - 3, CZ - 2, CZ - 1)
    edge = (lanes == 0) | (lanes == C - 1)
    for z in range(CZ):
        for a, b in ((0, C),) if z in near_z else near_x:
            lift[z, a:b, :] = jnp.where(edge[a:b], pltpu.roll(cols[a:b, :], C - 2 - 4 * z, 1), 0.0)
    add_rows(lift, lifted, 1.0)
    for z in range(CZ):
        for a, b in ((0, C),) if z in near_z else near_x:
            mid[z + 1, PAD + a : PAD + b, :] = weight[z, a:b, :] * lift[z, a:b, :]
    sweep_planes(mid, resp, weight, lift, 0, CZ, 8, (0, C - 8))
    for z in (0, CZ - 2):
        sweep_planes(mid, resp, weight, lift, z, 2, 8, range(8, C - 8, 8))


def merge_sides(low, high):
    return [f for pair in zip(low, high) for f in pair]


def third_kernel(*refs):
    it = iter(refs)
    take = lambda n: [next(it) for _ in range(n)]
    own_uv = take(6)
    got = take(5)
    bases, prev, back, weight, wx, wy, before = take(7)
    high_u, high_v = take(3), take(3)
    (rows,) = take(1)
    low_u, low_v = take(3), take(3)
    (turn,) = take(1)
    lift_u = merge_sides(low_u, high_u)
    lift_v = merge_sides(low_v, high_v)
    jumps(own_uv, got, bases, prev, back, 2, [lift_u, lift_v])
    weights = layer_weights(weight, wx, wy)
    u = lift_layers(lift_u, turn.at[0], False)
    v = lift_layers(lift_v, turn.at[1], False)
    sums = [square_sum(lift_u, lift_u), square_sum(lift_u, lift_v), square_sum(lift_v, lift_v)]
    sums += [layer_energy(u, u, weights), layer_energy(u, v, weights), layer_energy(v, v, weights)]
    rows[...] = jnp.broadcast_to(before[...] + row_of_sums(sums, 2), (C, C))


def steps(totals):
    row = jnp.sum(totals[...], axis=0, keepdims=True)
    lanes = lane_of((1, C))
    gg, gh, guu, guv, gvv, huu, huv, hvv = [jnp.sum(jnp.where(lanes == i, row, 0.0), axis=1, keepdims=True) for i in range(8)]
    one = gg / (gh + EPSILON)
    two = (guu - 2.0 * one * guv + one * one * gvv) / (huu - 2.0 * one * huv + one * one * hvv + EPSILON)
    return one, two


def fourth_kernel(*refs):
    it = iter(refs)
    take = lambda n: [next(it) for _ in range(n)]
    totals, heat, weight, free, resp = take(5)
    lift_1 = take(6)
    lift_u = take(6)
    lift_v = take(6)
    supply, state = take(2)
    high = take(3)
    own = take(6)
    sends = take(5)
    low = take(3)
    mid, turn, cols = take(3)
    held = merge_sides(low, high)
    one, two = steps(totals)
    for i in range(6):
        held[i][...] = one * lift_1[i][...] + two * (lift_u[i][...] - one * lift_v[i][...])
    cols[...] = pack_columns(turn, held[2][...], held[3][...])
    zero_ends(mid)
    zero_ends(state)

    def plane(z, carry):
        supply[z] = heat[z] - column_plane(cols[...], z)
        state[z + 1, INNER, :] = free[z + 1, INNER, :] - one * resp[z + 1, INNER, :]
        return carry

    lax.fori_loop(0, CZ, plane, 0, unroll=WIDE)
    add_rows(supply, held, -1.0)
    sweep(state, mid, weight, supply)
    sweep(mid, state, weight, supply)
    own_faces(state, own, turn)
    pack_sends(sends, [f[...] for f in own], 0)


def last_kernel(*refs):
    it = iter(refs)
    take = lambda n: [next(it) for _ in range(n)]
    totals, free, resp = take(3)
    held = take(3)
    lift_3 = take(3)
    lift_u = take(3)
    lift_v = take(3)
    (out,) = take(1)
    outs = take(3)
    state, sems = take(2)
    one, two = steps(totals)

    def plane(z, carry):
        state[z] = free[z + 1, INNER, :] - one * resp[z + 1, INNER, :]
        return carry

    copies = []
    for i in range(PARTS):
        lax.fori_loop(i * DEPTH, (i + 1) * DEPTH, plane, 0, unroll=UNROLL)
        s = pl.ds(i * DEPTH, DEPTH)
        copies.append(pltpu.make_async_copy(state.at[s], out.at[s], sems.at[i]))
        copies[-1].start()
    for i in range(3):
        outs[i][...] = held[i][...] + one * lift_3[i][...] + two * (lift_u[i][...] - one * lift_v[i][...])
    for c in copies:
        c.wait()


FIELD = jax.ShapeDtypeStruct((CZ, C, C), F32)
PADDED = jax.ShapeDtypeStruct((CZ + 2, C + 2 * PAD, C), F32)
FACE = jax.ShapeDtypeStruct((CZ, C), F32)
SQUARE = jax.ShapeDtypeStruct((C, C), F32)
FACES = [FACE] * 4 + [SQUARE] * 2
LAYERS = jax.ShapeDtypeStruct((4, CZ, C), F32)
ROW = jax.ShapeDtypeStruct((1, C), F32)
SIDE = [FACE, FACE, SQUARE]
S_SIDE = [pltpu.VMEM(f.shape, F32) for f in SIDE]
S_FIELD = pltpu.VMEM((CZ, C, C), F32)
S_PADDED = pltpu.VMEM((CZ + 2, C + 2 * PAD, C), F32)
PIECES = jax.ShapeDtypeStruct((3, C, 2 * C), BF16)
S_SQUARE = pltpu.VMEM((C, C), F32)


def sends_of(n, extra):
    small = jax.ShapeDtypeStruct((n * CZ + extra, C), F32)
    return [small] * 4 + [jax.ShapeDtypeStruct((n * C + extra, C), F32)]


def call(kernel, outs, scratch, args, us, in_specs=None, out_specs=None):
    return list(
        pl.pallas_call(
            kernel,
            out_shape=tuple(outs),
            in_specs=in_specs or [VM] * len(args),
            out_specs=tuple(out_specs or [VM] * len(outs)),
            scratch_shapes=scratch,
            compiler_params=pltpu.CompilerParams(vmem_limit_bytes=20 * 1024 * 1024),
            cost_estimate=pl.CostEstimate(flops=us * 10**7, transcendentals=0, bytes_accessed=2**20),
        )(*args)
    )


def swap_pairs(along, start):
    nx, ny = lax.axis_size("gx"), lax.axis_size("gy")
    place = lambda x, y: x * ny + y
    pairs = []
    for x in range(nx):
        for y in range(ny):
            i, n = (x, nx) if along == "x" else (y, ny)
            j = i + 1 if i % 2 == start else i - 1
            if 0 <= j < n:
                other = place(j, y) if along == "x" else place(x, j)
            else:
                other = place(x, y ^ 1) if along == "x" else place(x ^ 1, y)
            pairs.append((place(x, y), other))
    return pairs


def exchange(sends):
    xa, xb, ya, yb, zz = sends
    both = ("gx", "gy")
    xa = lax.ppermute(xa, both, swap_pairs("x", 0))
    yb = lax.ppermute(yb, both, swap_pairs("y", 1))
    zz = lax.ppermute(zz, "gz", [(0, 1), (1, 0)])
    xb = lax.ppermute(xb, both, swap_pairs("x", 1))
    ya = lax.ppermute(ya, both, swap_pairs("y", 0))
    return [xa, xb, ya, yb, zz]


def gather_rows(rows):
    rows = lax.all_to_all(rows.reshape(C, 1, C), AXES, 0, 0)
    return rows.reshape(C, C)


def body(heat, cond, projection, segment_map):
    proj = projection[0, 0, 0]
    segs = segment_map.reshape(3, 1, C)
    dma = pltpu.SemaphoreType.DMA
    scratch = [S_FIELD, pltpu.VMEM(proj.shape, F32), pltpu.VMEM(segs.shape, jnp.int32), S_PADDED, S_SQUARE, S_SQUARE, dma((2, PARTS)), dma((2,))]
    outs = [FIELD, PADDED, PIECES, FIELD, LAYERS, LAYERS] + FACES + sends_of(1, C)
    out = call(first_kernel, outs, scratch, [pltpu.with_memory_space_constraint(a, pltpu.MemorySpace.HBM) for a in (heat, cond, proj, segs)], 4, [AWAY] * 4)
    weight, state, bases, heat, wx, wy = out[:6]
    own, sends = out[6:12], out[12:]
    supply = heat
    prev = []
    held = None
    for pair in range(2):
        first = pair == 0
        got = exchange(sends)
        out = call(free_kernel, [PADDED] + FACES, [S_PADDED, S_SQUARE], (state, weight, supply), 3)
        free, own_u = out[0], out[1:]
        args = own + got + [bases] + prev + [weight, wx, wy] + own_u
        stacked = [jax.ShapeDtypeStruct((2 * f.shape[0], C), F32) for f in FACES]
        outs = FACES + stacked + sends_of(2, 0) + ([PIECES, PIECES] if first else [])
        out = call(functools.partial(second_kernel, first), outs, [S_SQUARE], args, 2)
        lift_1, own_uv, sends = out[:6], out[6:12], out[12:17]
        if first:
            prev = out[17:]
        got = exchange(sends)
        args = lift_1 + own_uv[2:4] + [weight, wx, wy]
        resp, sums = call(response_kernel, [PADDED, ROW], [S_FIELD, S_PADDED, S_SQUARE, S_SQUARE], args, 3)
        args = own_uv + got + [bases] + prev + [weight, wx, wy, sums]
        outs = SIDE + SIDE + [SQUARE] + (SIDE + SIDE if first else [])
        scratch = ([] if first else S_SIDE + S_SIDE) + [pltpu.VMEM((2, C, C), F32)]
        out = call(third_kernel, outs, scratch, args, 2)
        high_u, high_v, rows = out[:3], out[3:6], out[6]
        totals = gather_rows(rows)
        if first:
            args = [totals, heat, weight, free, resp] + lift_1 + merge_sides(out[7:10], high_u) + merge_sides(out[10:13], high_v)
            outs = [FIELD, PADDED] + SIDE + FACES + sends_of(1, 0)
            out = call(fourth_kernel, outs, S_SIDE + [S_PADDED, S_SQUARE, S_SQUARE], args, 5)
            supply, state, held, own, sends = out[0], out[1], out[2:5], out[5:11], out[11:]
    args = [totals, free, resp] + held + [lift_1[i] for i in (1, 3, 5)] + high_u + high_v
    state, mx, my, mz = call(last_kernel, [FIELD, FACE, FACE, SQUARE], [S_FIELD, dma((PARTS,))], args, 2, None, [AWAY, VM, VM, VM])
    return state, mx[None, None, None], my[None, None, None], mz[None, None, None]


def solution(mesh):
    field = P("gz", "gx", "gy")
    in_specs = (field, field, P("gz", "gx", "gy", None, None, None), P("gz", "gx", "gy", None, None))
    face = P("gz", "gx", "gy", None, None)
    return jax.shard_map(body, mesh=mesh, in_specs=in_specs, out_specs=(field, face, face, face), check_vma=False)
```
